32 devices in a mesh: dp: 8 (over z, x), mp: 4 (over y, core).
Axes of the slice: x: 2, y: 2, z: 4, core: 2. Of those that a mesh axis runs over, the one named last changes fastest.
Arguments:
- tokens: bfloat16 [16384, 1024], P('dp'), may hold values from -6 to 6
- cotangent: bfloat16 [16384, 1024], P('dp'), may hold values from -15 to 15
- item_lengths: int32 [8, 8], P('dp'), may hold values from 1 to 1024, 2048 in all within a row
- w_qkv: bfloat16 [3, 1024, 1024], P(None, None, 'mp'), may hold values from -0.1875 to 0.1875
- b_qv: float32 [2, 1024], P(None, 'mp'), may hold values from -3 to 3
- w_out: bfloat16 [1024, 1024], P('mp'), may hold values from -0.75 to 0.75
- b_out: float32 [1024], replicated, may hold values from -1.75 to 1.75
- w_fc1: bfloat16 [1024, 4096], P(None, 'mp'), may hold values from -0.1875 to 0.1875
- b_fc1: float32 [4096], P('mp'), may hold values from -3 to 3
- w_fc2: bfloat16 [4096, 1024], P('mp'), may hold values from -0.09375 to 0.09375
- b_fc2: float32 [1024], replicated, may hold values from -1.75 to 1.75
- ln1_gain: float32 [1024], replicated, may hold values from 0.5 to 1.5
- ln1_bias: float32 [1024], replicated, may hold values from -1.75 to 1.75
- ln2_gain: float32 [1024], replicated, may hold values from 0.5 to 1.5
- ln2_bias: float32 [1024], replicated, may hold values from -1.75 to 1.75
Outputs:
- output: bfloat16 [16384, 1024], P('dp')
- grad_tokens: float32 [16384, 1024], P('dp')
- grad_w_qkv: float32 [3, 1024, 1024], P(None, 'dp', 'mp')
- grad_b_qv: float32 [2, 1024], P(None, 'mp')
- grad_w_out: float32 [1024, 1024], P('mp', 'dp')
- grad_b_out: float32 [1024], replicated
- grad_w_fc1: float32 [1024, 4096], P('dp', 'mp')
- grad_b_fc1: float32 [4096], P('mp')
- grad_w_fc2: float32 [4096, 1024], P('mp', 'dp')
- grad_b_fc2: float32 [1024], replicated
- grad_ln1_gain: float32 [1024], replicated
- grad_ln1_bias: float32 [1024], replicated
- grad_ln2_gain: float32 [1024], replicated
- grad_ln2_bias: float32 [1024], replicated
The draws below stay inside these ranges and needn't reach their ends.
Inputs may be any that keep to these rules, and one draw needn't show every extreme that they name: `item_lengths`: each row sums to 2048, and each row's longest item has exactly 1024 patches.
All inputs are finite; a program needn't handle non-finite values.
Results may differ from the reference program's by a relative error of at most 0.019.
Values may be sent and summed in bfloat16 or wider, within the bound.
A program may use at most 192 MiB of HBM per device.

```python
import math
from functools import partial
import jax
import jax.numpy as jnp
import numpy as np
from jax import lax

D = 1024
HEADS = 16
FF = 4096
HEAD = 64
QBLOCK = 512
ITEMS = 8
TOK_DEV = 2048
LONGEST = 1024
GROUPS = 8
TOKENS = 16384
N_MP = 4


def draw_cotangent(key, part):
    groups = TOKENS // TOK_DEV
    block_of_row = (jnp.arange(TOKENS, dtype=jnp.int32) // TOK_DEV).astype(jnp.float32)
    ramp = 1.0 + 2.0 * block_of_row / max(groups - 1, 1)
    base = jnp.clip(jax.random.normal(key, (TOKENS, D), jnp.float32), -5.0, 5.0)
    return (base * ramp[:, None]).astype(jnp.bfloat16)


def block_scale(rng, dims, cuts, least, largest):
    factor_of = 1.0
    for axis_at, blocks in cuts:
        heights = jax.random.uniform(jax.random.fold_in(jax.random.fold_in(rng, 6), axis_at), (blocks,), jnp.float32, least / len(cuts), largest / len(cuts))
        factor_of = factor_of * jnp.repeat(jnp.exp(heights), dims[axis_at] // blocks).reshape((-1,) + (1,) * (len(dims) - 1 - axis_at))
    return factor_of


def split_up(amount, total, reach, slope):
    loads = [(1 << 20) // math.isqrt(grade ** slope) + 1 for grade in range(2, amount + 1)]
    rest, counts = total - reach - (amount - 1), [1] * (amount - 1)
    while rest > 0:
        movable = [i for i in range(amount - 1) if counts[i] < reach]
        pool, left = sum([loads[i] for i in movable]), rest
        for i in movable:
            more = min(reach - counts[i], max(1, left * loads[i] // pool), rest)
            counts[i] = counts[i] + more
            rest = rest - more
    return np.array([reach] + counts)


def ragged_sizes(stream_key, amount, total, limit, lean):
    if amount == 2:
        one = jax.random.randint(stream_key, (), max(1, total - limit), min(limit, total - 1) + 1)
        return jnp.stack([one, total - one])
    lengths = jnp.asarray(split_up(amount, total, limit, lean), jnp.int32)
    pairs = (amount - 1) // 2
    donor, receiver = lengths[1:1 + 2 * pairs:2], lengths[2:2 + 2 * pairs:2]
    margin = jnp.minimum(donor - 1, limit - receiver)
    shifted = jax.random.randint(jax.random.fold_in(stream_key, 1), (pairs,), 0, 1 << 20) % (margin + 1)
    lengths = lengths.at[1:1 + 2 * pairs:2].set(donor - shifted).at[2:2 + 2 * pairs:2].set(receiver + shifted)
    return lengths[jax.random.permutation(jax.random.fold_in(stream_key, 2), amount)]


def gaussian(own_key, extent, scale, bound, cuts=(), held_as=jnp.bfloat16):
    array = jax.random.normal(own_key, extent, jnp.float32) * scale
    if len(cuts) > 0:
        array = block_scale(own_key, extent, cuts, -0.22, 0.18) * array
    return jnp.clip(array, min=-bound, max=bound).astype(held_as)


def setup_inputs(seed: int = 0) -> dict:
    key_of = jax.random.split(jax.random.key(seed), 16)
    tokens = gaussian(key_of[0], (TOKENS, D), 1.0, 6.0, ((0, 8),))
    cotangent = draw_cotangent(jax.random.fold_in(key_of[15], 71), 0)
    item_lengths = jax.vmap(lambda own: ragged_sizes(own, ITEMS, TOK_DEV, LONGEST, 2))(jax.random.split(key_of[2], GROUPS)).reshape((GROUPS, ITEMS)).astype(jnp.int32)
    w_qkv = gaussian(key_of[3], (3, D, D), D ** -0.5, 0.1875, ((2, 4),))
    b_qv = gaussian(key_of[4], (2, D), 0.5, 3.0, ((1, 4),), jnp.float32)
    w_out = gaussian(key_of[5], (D, D), HEAD ** -0.5, 0.75, ((0, 4),))
    b_out = gaussian(key_of[6], (D,), 0.3, 1.75, (), jnp.float32)
    w_fc1 = gaussian(key_of[7], (D, FF), D ** -0.5, 0.1875, ((1, 4),))
    b_fc1 = gaussian(key_of[8], (FF,), 0.5, 3.0, ((0, 4),), jnp.float32)
    w_fc2 = gaussian(key_of[9], (FF, D), FF ** -0.5, 0.09375, ((0, 4),))
    b_fc2 = gaussian(key_of[10], (D,), 0.3, 1.75, (), jnp.float32)
    ln1_gain = jnp.clip(1.0 + 0.1 * jax.random.normal(key_of[11], (D,), jnp.float32), 0.5, 1.5)
    ln1_bias = gaussian(key_of[12], (D,), 0.3, 1.75, (), jnp.float32)
    ln2_gain = jnp.clip(1.0 + 0.1 * jax.random.normal(key_of[13], (D,), jnp.float32), 0.5, 1.5)
    ln2_bias = gaussian(key_of[14], (D,), 0.3, 1.75, (), jnp.float32)
    return {"tokens": tokens, "cotangent": cotangent, "item_lengths": item_lengths, "w_qkv": w_qkv, "b_qv": b_qv, "w_out": w_out, "b_out": b_out, "w_fc1": w_fc1, "b_fc1": b_fc1, "w_fc2": w_fc2, "b_fc2": b_fc2, "ln1_gain": ln1_gain, "ln1_bias": ln1_bias, "ln2_gain": ln2_gain, "ln2_bias": ln2_bias}


highest = lax.Precision.HIGHEST

@jax.custom_vjp
def low(v):
    return lax.optimization_barrier(v.astype(jnp.bfloat16)).astype(jnp.float32)

@jax.custom_vjp
def low_back(v):
    return v

def low_keep(v):
    return (low(v), None)

def low_pass(kept, grad):
    return (grad,)

def back_keep(v):
    return (v, None)

def back_low(kept, grad):
    return (low(grad),)
low.defvjp(low_keep, low_pass)
low_back.defvjp(back_keep, back_low)

def matmul_high(left, right):
    return jnp.dot(left, right, precision=highest)

def normalize(values, gain, shift):
    center = lax.optimization_barrier(jnp.mean(values, axis=-1, keepdims=True))
    centered = values - center
    spread = lax.optimization_barrier(jnp.mean(centered * centered, axis=-1, keepdims=True))
    return centered * lax.rsqrt(spread + 1e-06) * gain + shift

def exact_gelu(values):
    return jax.nn.gelu(values, approximate=False)

def segment_ids(lengths_row, row_count):
    ends = jnp.cumsum(lengths_row.astype(jnp.int32)).astype(jnp.int32)
    positions = jnp.arange(row_count, dtype=jnp.int32)
    return lax.optimization_barrier(jnp.sum((positions[:, None] >= ends[None, :]).astype(jnp.int32), axis=1)).astype(jnp.int32)

def attention(queries, key_rows, value_rows, segments):
    groups = segments.shape[0]
    row_count = segments.shape[1]
    blocks = row_count // QBLOCK
    score_scale = HEAD ** (-0.5)
    query_all = queries.reshape(groups, blocks, QBLOCK, HEADS, HEAD)
    keys_all = key_rows.reshape(groups, row_count, HEADS, HEAD)
    values_all = value_rows.reshape(groups, row_count, HEADS, HEAD)
    seg_blocks = segments.reshape(groups, blocks, QBLOCK)

    def one_group(inputs):
        query_group, keys_group, values_group, seg_group, seg_rows = inputs

        def one_block(pieces):
            query_block, seg_block = pieces
            scores = low_back(jnp.einsum('qhd,khd->hqk', query_block, keys_group, precision=highest) * score_scale)
            same = seg_block[:, None] == seg_group[None, :]
            scores = jnp.where(same[None], scores, -1e+30)
            row_max = lax.optimization_barrier(jnp.max(scores, axis=-1, keepdims=True))
            raised = jnp.exp(scores - row_max)
            probs = raised / lax.optimization_barrier(jnp.sum(raised, axis=-1, keepdims=True))
            return jnp.einsum('hqk,khd->qhd', low(probs), values_group, precision=highest)
        return lax.map(jax.checkpoint(one_block), (query_group, seg_rows))
    result = lax.map(jax.checkpoint(one_group), (query_all, keys_all, values_all, segments, seg_blocks))
    return result.reshape(groups * row_count, HEADS * HEAD)

def reference(tokens, cotangent, item_lengths, w_qkv, b_qv, w_out, b_out, w_fc1, b_fc1, w_fc2, b_fc2, ln1_gain, ln1_bias, ln2_gain, ln2_bias):
    segments = jax.vmap(partial(segment_ids, row_count=TOK_DEV))(item_lengths)
    cols = D // N_MP
    units = FF // N_MP

    def forward(inputs, qkv_w, qv_b, out_w, out_b, fc1_w, fc1_b, fc2_w, fc2_b, gain_one, shift_one, gain_two, shift_two):
        normed_one = low(normalize(inputs, gain_one, shift_one))
        query_parts = []
        key_parts = []
        value_parts = []
        for group_idx in range(N_MP):
            col_start = group_idx * cols
            col_stop = col_start + cols
            shared = low_back(normed_one)
            query_parts.append(low(low_back(matmul_high(shared, qkv_w[0][:, col_start:col_stop])) + qv_b[0, col_start:col_stop]))
            key_parts.append(low(low_back(matmul_high(shared, qkv_w[1][:, col_start:col_stop]))))
            value_parts.append(low(low_back(matmul_high(shared, qkv_w[2][:, col_start:col_stop])) + qv_b[1, col_start:col_stop]))
        attended = attention(jnp.concatenate(query_parts, axis=1), jnp.concatenate(key_parts, axis=1), jnp.concatenate(value_parts, axis=1), segments)
        attention_sum = jnp.zeros_like(inputs)
        for group_idx in range(N_MP):
            col_start = group_idx * cols
            col_stop = col_start + cols
            attended_part = low(low_back(attended[:, col_start:col_stop]))
            attention_sum = attention_sum + low(low_back(matmul_high(attended_part, out_w[col_start:col_stop, :])))
        middle = inputs + attention_sum + out_b
        normed_two = low(normalize(middle, gain_two, shift_two))
        mlp_sum = jnp.zeros_like(inputs)
        for group_idx in range(N_MP):
            unit_start = group_idx * units
            unit_stop = unit_start + units
            shared = low_back(normed_two)
            hidden_pre = low_back(matmul_high(shared, fc1_w[:, unit_start:unit_stop])) + fc1_b[unit_start:unit_stop]
            activated = low(exact_gelu(hidden_pre))
            mlp_sum = mlp_sum + low(low_back(matmul_high(activated, fc2_w[unit_start:unit_stop, :])))
        return middle + mlp_sum + fc2_b
    result, pullback = jax.vjp(forward, tokens.astype(jnp.float32), w_qkv.astype(jnp.float32), b_qv.astype(jnp.float32), w_out.astype(jnp.float32), b_out.astype(jnp.float32), w_fc1.astype(jnp.float32), b_fc1.astype(jnp.float32), w_fc2.astype(jnp.float32), b_fc2.astype(jnp.float32), ln1_gain.astype(jnp.float32), ln1_bias.astype(jnp.float32), ln2_gain.astype(jnp.float32), ln2_bias.astype(jnp.float32))
    grads = pullback(cotangent.astype(jnp.float32))
    return (result.astype(jnp.bfloat16), grads[0], grads[1], grads[2], grads[3], grads[4], grads[5], grads[6], grads[7], grads[8], grads[9], grads[10], grads[11], grads[12])
```

```python
from functools import partial

import jax
import jax.numpy as jnp
from jax import lax
from jax.sharding import PartitionSpec as P

HEAD = 64
QBLOCK = 512


def normalize(values, gain, shift):
    center = jnp.mean(values, axis=-1, keepdims=True)
    centered = values - center
    spread = jnp.mean(centered * centered, axis=-1, keepdims=True)
    return centered * lax.rsqrt(spread + 1e-06) * gain + shift


def exact_gelu(values):
    return jax.nn.gelu(values, approximate=False)


def segment_ids(lengths_row, row_count):
    ends = jnp.cumsum(lengths_row)
    positions = jnp.arange(row_count, dtype=jnp.int32)
    return jnp.sum((positions[:, None] >= ends[None, :]).astype(jnp.int32), axis=1)


def mp_allreduce(partial, n_mp):
    if n_mp != 4:
        return lax.psum(partial, "mp").astype(jnp.float32)
    idx = lax.axis_index("mp")
    low_bit = idx % 2
    half = partial.shape[0] // 2
    mine = lax.dynamic_slice_in_dim(partial, low_bit * half, half, 0)
    other = lax.dynamic_slice_in_dim(partial, (1 - low_bit) * half, half, 0)
    got = lax.ppermute(other, "mp", [(k, k ^ 1) for k in range(4)])
    first = (mine.astype(jnp.float32) + got.astype(jnp.float32)).astype(jnp.bfloat16)
    got_far = lax.ppermute(first, "mp", [(k, k ^ 2) for k in range(4)])
    second = (first.astype(jnp.float32) + got_far.astype(jnp.float32)).astype(jnp.bfloat16)
    got_back = lax.ppermute(second, "mp", [(k, k ^ 1) for k in range(4)])
    top = jnp.where(low_bit == 0, second, got_back)
    bottom = jnp.where(low_bit == 0, got_back, second)
    return jnp.concatenate([top, bottom], axis=0).astype(jnp.float32)


def per_device(n_mp,

    tokens,
    cotangent,
    item_lengths,
    w_qkv,
    b_qv,
    w_out,
    b_out,
    w_fc1,
    b_fc1,
    w_fc2,
    b_fc2,
    ln1_gain,
    ln1_bias,
    ln2_gain,
    ln2_bias,
):
    row_count = tokens.shape[0]
    local_cols = w_qkv.shape[2]
    heads_here = local_cols // HEAD
    blocks = row_count // QBLOCK
    score_scale = HEAD ** (-0.5)
    segments = segment_ids(item_lengths[0], row_count)
    seg_blocks = segments.reshape(blocks, QBLOCK)
    inputs = tokens.astype(jnp.float32)
    norm_one, norm_one_back = jax.vjp(normalize, inputs, ln1_gain, ln1_bias)
    normed_one = norm_one.astype(jnp.bfloat16)
    queries = (jnp.dot(normed_one, w_qkv[0], preferred_element_type=jnp.float32) + b_qv[0]).astype(
        jnp.bfloat16
    )
    key_rows = jnp.dot(normed_one, w_qkv[1], preferred_element_type=jnp.float32).astype(
        jnp.bfloat16
    )
    value_rows = (
        jnp.dot(normed_one, w_qkv[2], preferred_element_type=jnp.float32) + b_qv[1]
    ).astype(jnp.bfloat16)
    key_heads = key_rows.reshape(row_count, heads_here, HEAD)
    value_heads = value_rows.reshape(row_count, heads_here, HEAD)
    query_blocks = queries.reshape(blocks, QBLOCK, heads_here, HEAD)

    def block_scores(query_block, seg_block):
        scores = (
            jnp.einsum("qhd,khd->hqk", query_block, key_heads, preferred_element_type=jnp.float32)
            * score_scale
        )
        same = seg_block[:, None] == segments[None, :]
        return jnp.where(same[None], scores, -1e30)

    def forward_block(pieces):
        query_block, seg_block = pieces
        scores = block_scores(query_block, seg_block)
        row_max = jnp.max(scores, axis=-1, keepdims=True)
        raised = jnp.exp(scores - row_max)
        row_sum = jnp.sum(raised, axis=-1, keepdims=True)
        probs = raised / row_sum
        block_out = jnp.einsum(
            "hqk,khd->qhd",
            probs.astype(jnp.bfloat16),
            value_heads,
            preferred_element_type=jnp.float32,
        )
        return (block_out.astype(jnp.bfloat16), (row_max + jnp.log(row_sum))[..., 0])

    out_blocks, log_norms = lax.map(forward_block, (query_blocks, seg_blocks))
    attended = out_blocks.reshape(row_count, local_cols)
    attention_sum = mp_allreduce(
        jnp.dot(attended, w_out, preferred_element_type=jnp.float32).astype(jnp.bfloat16), n_mp
    )
    middle = inputs + attention_sum + b_out
    norm_two, norm_two_back = jax.vjp(normalize, middle, ln2_gain, ln2_bias)
    normed_two = norm_two.astype(jnp.bfloat16)
    hidden_pre = jnp.dot(normed_two, w_fc1, preferred_element_type=jnp.float32) + b_fc1
    activated_full, gelu_back = jax.vjp(exact_gelu, hidden_pre)
    activated = activated_full.astype(jnp.bfloat16)
    mlp_sum = mp_allreduce(
        jnp.dot(activated, w_fc2, preferred_element_type=jnp.float32).astype(jnp.bfloat16), n_mp
    )
    output = (middle + mlp_sum + b_fc2).astype(jnp.bfloat16)
    upstream = cotangent.astype(jnp.float32)
    grad_b_fc2 = jnp.sum(upstream, axis=0)
    grad_w_fc2 = jnp.einsum("tf,td->fd", activated, cotangent, preferred_element_type=jnp.float32)
    d_act = jnp.einsum("td,fd->tf", cotangent, w_fc2, preferred_element_type=jnp.float32)
    d_pre = gelu_back(d_act)[0]
    grad_b_fc1 = jnp.sum(d_pre, axis=0)
    d_pre_low = d_pre.astype(jnp.bfloat16)
    grad_w_fc1 = jnp.einsum("td,tf->df", normed_two, d_pre_low, preferred_element_type=jnp.float32)
    d_normed_two = mp_allreduce(
        jnp.einsum("tf,df->td", d_pre_low, w_fc1, preferred_element_type=jnp.float32).astype(
            jnp.bfloat16
        ),
        n_mp,
    )
    d_middle_norm, grad_ln2_gain, grad_ln2_bias = norm_two_back(d_normed_two)
    d_middle = upstream + d_middle_norm
    grad_b_out = jnp.sum(d_middle, axis=0)
    d_middle_low = d_middle.astype(jnp.bfloat16)
    grad_w_out = jnp.einsum("tc,td->cd", attended, d_middle_low, preferred_element_type=jnp.float32)
    d_attended = jnp.einsum(
        "td,cd->tc", d_middle_low, w_out, preferred_element_type=jnp.float32
    ).astype(jnp.bfloat16)
    d_att_blocks = d_attended.reshape(blocks, QBLOCK, heads_here, HEAD)

    def backward_block(running, pieces):
        d_keys_acc, d_values_acc = running
        query_block, seg_block, d_out_block, log_norm = pieces
        scores = block_scores(query_block, seg_block)
        probs = jnp.exp(scores - log_norm[..., None])
        d_probs = jnp.einsum(
            "qhd,khd->hqk", d_out_block, value_heads, preferred_element_type=jnp.float32
        )
        d_scores = probs * (d_probs - jnp.sum(probs * d_probs, axis=-1, keepdims=True))
        d_scores_low = d_scores.astype(jnp.bfloat16)
        d_query_block = (
            jnp.einsum("hqk,khd->qhd", d_scores_low, key_heads, preferred_element_type=jnp.float32)
            * score_scale
        )
        d_keys_acc = (
            d_keys_acc
            + jnp.einsum(
                "hqk,qhd->khd", d_scores_low, query_block, preferred_element_type=jnp.float32
            )
            * score_scale
        )
        d_values_acc = d_values_acc + jnp.einsum(
            "hqk,qhd->khd",
            probs.astype(jnp.bfloat16),
            d_out_block,
            preferred_element_type=jnp.float32,
        )
        return ((d_keys_acc, d_values_acc), d_query_block)

    zeros_acc = jnp.zeros((row_count, heads_here, HEAD), jnp.float32)
    (d_keys, d_values), d_query_blocks = lax.scan(
        backward_block, (zeros_acc, zeros_acc), (query_blocks, seg_blocks, d_att_blocks, log_norms)
    )
    d_queries = d_query_blocks.reshape(row_count, local_cols)
    d_keys = d_keys.reshape(row_count, local_cols)
    d_values = d_values.reshape(row_count, local_cols)
    grad_b_qv = jnp.stack([jnp.sum(d_queries, axis=0), jnp.sum(d_values, axis=0)])
    stacked = jnp.stack([d_queries, d_keys, d_values]).astype(jnp.bfloat16)
    grad_w_qkv = jnp.einsum("td,stc->sdc", normed_one, stacked, preferred_element_type=jnp.float32)
    d_normed_one = mp_allreduce(
        jnp.einsum("stc,sdc->td", stacked, w_qkv, preferred_element_type=jnp.float32).astype(
            jnp.bfloat16
        ),
        n_mp,
    )
    d_input_norm, grad_ln1_gain, grad_ln1_bias = norm_one_back(d_normed_one)
    grad_tokens = d_middle + d_input_norm
    def scatter(grad, dim):
        return lax.psum_scatter(
            grad.astype(jnp.bfloat16), "dp", scatter_dimension=dim, tiled=True
        ).astype(jnp.float32)

    summed_qkv = scatter(grad_w_qkv, 1)
    summed_out = scatter(grad_w_out, 1)
    summed_fc1 = scatter(grad_w_fc1, 0)
    summed_fc2 = scatter(grad_w_fc2, 1)
    packed = jnp.concatenate(
        [
            grad_ln1_gain,
            grad_ln1_bias,
            grad_ln2_gain,
            grad_ln2_bias,
            grad_b_out,
            grad_b_fc2,
            grad_b_qv.reshape(-1),
            grad_b_fc1,
        ]
    )
    packed = lax.psum(packed, "dp")
    width = grad_ln1_gain.shape[0]
    pieces = [packed[k * width : (k + 1) * width] for k in range(6)]
    qv_size = grad_b_qv.size
    summed_b_qv = packed[6 * width : 6 * width + qv_size].reshape(grad_b_qv.shape)
    summed_b_fc1 = packed[6 * width + qv_size :]
    return (
        output,
        grad_tokens,
        summed_qkv,
        summed_b_qv,
        summed_out,
        pieces[4],
        summed_fc1,
        summed_b_fc1,
        summed_fc2,
        pieces[5],
        pieces[0],
        pieces[1],
        pieces[2],
        pieces[3],
    )


def solution(mesh):
    in_specs = (
        P("dp", None),
        P("dp", None),
        P("dp", None),
        P(None, None, "mp"),
        P(None, "mp"),
        P("mp", None),
        P(),
        P(None, "mp"),
        P("mp"),
        P("mp", None),
        P(),
        P(),
        P(),
        P(),
        P(),
    )
    out_specs = (
        P("dp", None),
        P("dp", None),
        P(None, "dp", "mp"),
        P(None, "mp"),
        P("mp", "dp"),
        P(),
        P("dp", "mp"),
        P("mp"),
        P("mp", "dp"),
        P(),
        P(),
        P(),
        P(),
        P(),
    )
    return jax.shard_map(
        partial(per_device, mesh.shape["mp"]), mesh=mesh, in_specs=in_specs, out_specs=out_specs, check_vma=False
    )
```

```python
from functools import partial

import jax
import jax.numpy as jnp
from jax import lax
from jax.experimental import pallas as pl
from jax.experimental.pallas import tpu as pltpu
from jax.sharding import PartitionSpec as P

HEAD = 64
QBLOCK = 512
TQ = 256
TK = 256
NEG = -1e30


def _nt(a, b):
    return lax.dot_general(a, b, (((1,), (1,)), ((), ())), preferred_element_type=jnp.float32)


def _fwd_kernel(lo_ref, hi_ref, segc_ref, segr_ref, q_ref, k_ref, v_ref, o_ref, o32_ref, lse_ref):
    rows = q_ref.shape[1]
    scale = HEAD ** (-0.5)

    def q_body(i, carry):
        r0 = pl.multiple_of(i * TQ, TQ)
        q = q_ref[0, pl.ds(r0, TQ), :]
        sq = segc_ref[pl.ds(r0, TQ), :]
        lo = lo_ref[i]
        hi = hi_ref[i]

        def scores(j):
            c0 = pl.multiple_of(j * TK, TK)
            s = _nt(q, k_ref[0, pl.ds(c0, TK), :]) * scale
            same = sq == segr_ref[:, pl.ds(c0, TK)]
            return jnp.where(same, s, NEG), c0

        def stat_body(j, ml):
            m, l = ml
            s, _ = scores(j)
            m_new = jnp.maximum(m, jnp.max(s, axis=-1, keepdims=True))
            l = l * jnp.exp(m - m_new) + jnp.sum(jnp.exp(s - m_new), axis=-1, keepdims=True)
            return m_new, l

        m0 = jnp.full((TQ, 1), NEG, jnp.float32)
        l0 = jnp.zeros((TQ, 1), jnp.float32)
        m, l = lax.fori_loop(lo, hi, stat_body, (m0, l0))
        inv_l = 1.0 / l

        def acc_body(j, acc):
            s, c0 = scores(j)
            p = (jnp.exp(s - m) * inv_l).astype(jnp.bfloat16)
            return acc + jnp.dot(p, v_ref[0, pl.ds(c0, TK), :], preferred_element_type=jnp.float32)

        acc = lax.fori_loop(lo, hi, acc_body, jnp.zeros((TQ, HEAD), jnp.float32))
        o_ref[0, pl.ds(r0, TQ), :] = acc.astype(o_ref.dtype)
        o32_ref[0, pl.ds(r0, TQ), :] = acc
        lse_ref[0, pl.ds(r0, TQ), :] = m + jnp.log(l)
        return carry

    lax.fori_loop(0, rows // TQ, q_body, 0)


def _bwd_kernel(lo_ref, hi_ref, segc_ref, segr_ref, q_ref, k_ref, v_ref, do_ref, o32_ref, lse_ref,
                dq_ref, dk_ref, dv_ref):
    rows = q_ref.shape[1]
    scale = HEAD ** (-0.5)
    dk_ref[...] = jnp.zeros_like(dk_ref)
    dv_ref[...] = jnp.zeros_like(dv_ref)

    def q_body(i, carry):
        r0 = pl.multiple_of(i * TQ, TQ)
        q = q_ref[0, pl.ds(r0, TQ), :]
        do = do_ref[0, pl.ds(r0, TQ), :]
        sq = segc_ref[pl.ds(r0, TQ), :]
        lse = lse_ref[0, pl.ds(r0, TQ), :]
        dvec = jnp.sum(do.astype(jnp.float32) * o32_ref[0, pl.ds(r0, TQ), :], axis=-1, keepdims=True)

        def kv_body(j, dq):
            c0 = pl.multiple_of(j * TK, TK)
            k = k_ref[0, pl.ds(c0, TK), :]
            v = v_ref[0, pl.ds(c0, TK), :]
            s = _nt(q, k) * scale
            same = sq == segr_ref[:, pl.ds(c0, TK)]
            s = jnp.where(same, s, NEG)
            p = jnp.exp(s - lse)
            dp = _nt(do, v)
            ds = p * (dp - dvec)
            dq = dq + jnp.dot(ds.astype(jnp.bfloat16), k, preferred_element_type=jnp.float32)
            dk_ref[0, pl.ds(c0, TK), :] += jnp.dot(
                ds.T.astype(jnp.bfloat16), q, preferred_element_type=jnp.float32)
            dv_ref[0, pl.ds(c0, TK), :] += jnp.dot(
                p.T.astype(jnp.bfloat16), do, preferred_element_type=jnp.float32)
            return dq

        dq = lax.fori_loop(lo_ref[i], hi_ref[i], kv_body, jnp.zeros((TQ, HEAD), jnp.float32))
        dq_ref[0, pl.ds(r0, TQ), :] = dq * scale
        return carry

    lax.fori_loop(0, rows // TQ, q_body, 0)
    dk_ref[...] = dk_ref[...] * scale


def block_ranges(segments, item_lengths_row):
    rows = segments.shape[0]
    ends = jnp.cumsum(item_lengths_row.astype(jnp.int32))
    starts = ends - item_lengths_row.astype(jnp.int32)
    first = segments[0::TQ]
    last = segments[TQ - 1::TQ]
    n_items = item_lengths_row.shape[0]
    key_lo = jnp.take(starts, jnp.clip(first, 0, n_items - 1))
    key_hi = jnp.take(ends, jnp.clip(last, 0, n_items - 1))
    lo = jnp.clip(key_lo // TK, 0, rows // TK)
    hi = jnp.clip((key_hi + TK - 1) // TK, 0, rows // TK)
    return lo.astype(jnp.int32), hi.astype(jnp.int32)


def flash_forward(q, k, v, segments, lo, hi):
    heads, rows, _ = q.shape
    head_spec = pl.BlockSpec((1, rows, HEAD), lambda h, lo, hi: (h, 0, 0))
    lse_spec = pl.BlockSpec((1, rows, 1), lambda h, lo, hi: (h, 0, 0))
    col_spec = pl.BlockSpec((rows, 1), lambda h, lo, hi: (0, 0))
    row_spec = pl.BlockSpec((1, rows), lambda h, lo, hi: (0, 0))
    flops = int(heads * rows * rows * HEAD * 2 * 3 * 0.6)
    return pl.pallas_call(
        _fwd_kernel,
        out_shape=(
            jax.ShapeDtypeStruct((heads, rows, HEAD), jnp.bfloat16),
            jax.ShapeDtypeStruct((heads, rows, HEAD), jnp.float32),
            jax.ShapeDtypeStruct((heads, rows, 1), jnp.float32),
        ),
        grid_spec=pltpu.PrefetchScalarGridSpec(
            num_scalar_prefetch=2,
            grid=(heads,),
            in_specs=[col_spec, row_spec, head_spec, head_spec, head_spec],
            out_specs=[head_spec, head_spec, lse_spec],
        ),
        compiler_params=pltpu.CompilerParams(
            dimension_semantics=("arbitrary",), vmem_limit_bytes=48 * 1024 * 1024),
        cost_estimate=pl.CostEstimate(
            flops=flops, transcendentals=int(heads * rows * rows * 0.6 * 2),
            bytes_accessed=int(heads * rows * HEAD * (2 * 4 + 4) + heads * rows * 4)),
        name="segment_flash_fwd",
    )(lo, hi, segments.reshape(rows, 1), segments.reshape(1, rows), q, k, v)


def flash_backward(q, k, v, do, o32, lse, segments, lo, hi):
    heads, rows, _ = q.shape
    head_spec = pl.BlockSpec((1, rows, HEAD), lambda h, lo, hi: (h, 0, 0))
    lse_spec = pl.BlockSpec((1, rows, 1), lambda h, lo, hi: (h, 0, 0))
    col_spec = pl.BlockSpec((rows, 1), lambda h, lo, hi: (0, 0))
    row_spec = pl.BlockSpec((1, rows), lambda h, lo, hi: (0, 0))
    flops = int(heads * rows * rows * HEAD * 2 * 5 * 0.6)
    out = jax.ShapeDtypeStruct((heads, rows, HEAD), jnp.float32)
    return pl.pallas_call(
        _bwd_kernel,
        out_shape=(out, out, out),
        grid_spec=pltpu.PrefetchScalarGridSpec(
            num_scalar_prefetch=2,
            grid=(heads,),
            in_specs=[col_spec, row_spec, head_spec, head_spec, head_spec, head_spec, head_spec, lse_spec],
            out_specs=[head_spec, head_spec, head_spec],
        ),
        compiler_params=pltpu.CompilerParams(
            dimension_semantics=("arbitrary",), vmem_limit_bytes=48 * 1024 * 1024),
        cost_estimate=pl.CostEstimate(
            flops=flops, transcendentals=int(heads * rows * rows * 0.6),
            bytes_accessed=int(heads * rows * HEAD * (4 * 2 + 4 * 4) + heads * rows * 4)),
        name="segment_flash_bwd",
    )(lo, hi, segments.reshape(rows, 1), segments.reshape(1, rows), q, k, v, do, o32, lse)


def normalize(values, gain, shift):
    center = jnp.mean(values, axis=-1, keepdims=True)
    centered = values - center
    spread = jnp.mean(centered * centered, axis=-1, keepdims=True)
    return centered * lax.rsqrt(spread + 1e-06) * gain + shift


def exact_gelu(values):
    return jax.nn.gelu(values, approximate=False)


def segment_ids(lengths_row, row_count):
    ends = jnp.cumsum(lengths_row)
    positions = jnp.arange(row_count, dtype=jnp.int32)
    return jnp.sum((positions[:, None] >= ends[None, :]).astype(jnp.int32), axis=1)


def mp_allreduce(partial, n_mp):
    if n_mp != 4:
        return lax.psum(partial, "mp").astype(jnp.float32)
    idx = lax.axis_index("mp")
    low_bit = idx % 2
    half = partial.shape[0] // 2
    mine = lax.dynamic_slice_in_dim(partial, low_bit * half, half, 0)
    other = lax.dynamic_slice_in_dim(partial, (1 - low_bit) * half, half, 0)
    got = lax.ppermute(other, "mp", [(k, k ^ 1) for k in range(4)])
    first = (mine.astype(jnp.float32) + got.astype(jnp.float32)).astype(jnp.bfloat16)
    got_far = lax.ppermute(first, "mp", [(k, k ^ 2) for k in range(4)])
    second = (first.astype(jnp.float32) + got_far.astype(jnp.float32)).astype(jnp.bfloat16)
    got_back = lax.ppermute(second, "mp", [(k, k ^ 1) for k in range(4)])
    top = jnp.where(low_bit == 0, second, got_back)
    bottom = jnp.where(low_bit == 0, got_back, second)
    return jnp.concatenate([top, bottom], axis=0).astype(jnp.float32)


def per_device(n_mp,

    tokens,
    cotangent,
    item_lengths,
    w_qkv,
    b_qv,
    w_out,
    b_out,
    w_fc1,
    b_fc1,
    w_fc2,
    b_fc2,
    ln1_gain,
    ln1_bias,
    ln2_gain,
    ln2_bias,
):
    row_count = tokens.shape[0]
    local_cols = w_qkv.shape[2]
    heads_here = local_cols // HEAD
    segments = segment_ids(item_lengths[0], row_count)
    inputs = tokens.astype(jnp.float32)
    norm_one, norm_one_back = jax.vjp(normalize, inputs, ln1_gain, ln1_bias)
    normed_one = norm_one.astype(jnp.bfloat16)
    queries = (jnp.dot(normed_one, w_qkv[0], preferred_element_type=jnp.float32) + b_qv[0]).astype(
        jnp.bfloat16
    )
    key_rows = jnp.dot(normed_one, w_qkv[1], preferred_element_type=jnp.float32).astype(
        jnp.bfloat16
    )
    value_rows = (
        jnp.dot(normed_one, w_qkv[2], preferred_element_type=jnp.float32) + b_qv[1]
    ).astype(jnp.bfloat16)
    def to_heads(values):
        return values.reshape(row_count, heads_here, HEAD).transpose(1, 0, 2)

    def from_heads(values):
        return values.transpose(1, 0, 2).reshape(row_count, local_cols)

    lo_blocks, hi_blocks = block_ranges(segments, item_lengths[0])
    query_heads = to_heads(queries)
    key_heads = to_heads(key_rows)
    value_heads = to_heads(value_rows)
    out_heads, out_f32, log_norms = flash_forward(
        query_heads, key_heads, value_heads, segments, lo_blocks, hi_blocks
    )
    attended = from_heads(out_heads)
    attention_sum = mp_allreduce(
        jnp.dot(attended, w_out, preferred_element_type=jnp.float32).astype(jnp.bfloat16), n_mp
    )
    middle = inputs + attention_sum + b_out
    norm_two, norm_two_back = jax.vjp(normalize, middle, ln2_gain, ln2_bias)
    normed_two = norm_two.astype(jnp.bfloat16)
    hidden_pre = jnp.dot(normed_two, w_fc1, preferred_element_type=jnp.float32) + b_fc1
    activated_full, gelu_back = jax.vjp(exact_gelu, hidden_pre)
    activated = activated_full.astype(jnp.bfloat16)
    mlp_sum = mp_allreduce(
        jnp.dot(activated, w_fc2, preferred_element_type=jnp.float32).astype(jnp.bfloat16), n_mp
    )
    output = (middle + mlp_sum + b_fc2).astype(jnp.bfloat16)
    upstream = cotangent.astype(jnp.float32)
    grad_b_fc2 = jnp.sum(upstream, axis=0)
    grad_w_fc2 = jnp.einsum("tf,td->fd", activated, cotangent, preferred_element_type=jnp.float32)
    d_act = jnp.einsum("td,fd->tf", cotangent, w_fc2, preferred_element_type=jnp.float32)
    d_pre = gelu_back(d_act)[0]
    grad_b_fc1 = jnp.sum(d_pre, axis=0)
    d_pre_low = d_pre.astype(jnp.bfloat16)
    grad_w_fc1 = jnp.einsum("td,tf->df", normed_two, d_pre_low, preferred_element_type=jnp.float32)
    d_normed_two = mp_allreduce(
        jnp.einsum("tf,df->td", d_pre_low, w_fc1, preferred_element_type=jnp.float32).astype(
            jnp.bfloat16
        ),
        n_mp,
    )
    d_middle_norm, grad_ln2_gain, grad_ln2_bias = norm_two_back(d_normed_two)
    d_middle = upstream + d_middle_norm
    grad_b_out = jnp.sum(d_middle, axis=0)
    d_middle_low = d_middle.astype(jnp.bfloat16)
    grad_w_out = jnp.einsum("tc,td->cd", attended, d_middle_low, preferred_element_type=jnp.float32)
    d_attended = jnp.einsum(
        "td,cd->tc", d_middle_low, w_out, preferred_element_type=jnp.float32
    ).astype(jnp.bfloat16)
    d_q_heads, d_k_heads, d_v_heads = flash_backward(
        query_heads, key_heads, value_heads, to_heads(d_attended), out_f32, log_norms,
        segments, lo_blocks, hi_blocks,
    )
    d_queries = from_heads(d_q_heads)
    d_keys = from_heads(d_k_heads)
    d_values = from_heads(d_v_heads)
    grad_b_qv = jnp.stack([jnp.sum(d_queries, axis=0), jnp.sum(d_values, axis=0)])
    stacked = jnp.stack([d_queries, d_keys, d_values]).astype(jnp.bfloat16)
    grad_w_qkv = jnp.einsum("td,stc->sdc", normed_one, stacked, preferred_element_type=jnp.float32)
    d_normed_one = mp_allreduce(
        jnp.einsum("stc,sdc->td", stacked, w_qkv, preferred_element_type=jnp.float32).astype(
            jnp.bfloat16
        ),
        n_mp,
    )
    d_input_norm, grad_ln1_gain, grad_ln1_bias = norm_one_back(d_normed_one)
    grad_tokens = d_middle + d_input_norm
    def scatter(grad, dim):
        return lax.psum_scatter(
            grad.astype(jnp.bfloat16), "dp", scatter_dimension=dim, tiled=True
        ).astype(jnp.float32)

    summed_qkv = scatter(grad_w_qkv, 1)
    summed_out = scatter(grad_w_out, 1)
    summed_fc1 = scatter(grad_w_fc1, 0)
    summed_fc2 = scatter(grad_w_fc2, 1)
    packed = jnp.concatenate(
        [
            grad_ln1_gain,
            grad_ln1_bias,
            grad_ln2_gain,
            grad_ln2_bias,
            grad_b_out,
            grad_b_fc2,
            grad_b_qv.reshape(-1),
            grad_b_fc1,
        ]
    )
    packed = lax.psum(packed, "dp")
    width = grad_ln1_gain.shape[0]
    pieces = [packed[k * width : (k + 1) * width] for k in range(6)]
    qv_size = grad_b_qv.size
    summed_b_qv = packed[6 * width : 6 * width + qv_size].reshape(grad_b_qv.shape)
    summed_b_fc1 = packed[6 * width + qv_size :]
    return (
        output,
        grad_tokens,
        summed_qkv,
        summed_b_qv,
        summed_out,
        pieces[4],
        summed_fc1,
        summed_b_fc1,
        summed_fc2,
        pieces[5],
        pieces[0],
        pieces[1],
        pieces[2],
        pieces[3],
    )


def solution(mesh):
    in_specs = (
        P("dp", None),
        P("dp", None),
        P("dp", None),
        P(None, None, "mp"),
        P(None, "mp"),
        P("mp", None),
        P(),
        P(None, "mp"),
        P("mp"),
        P("mp", None),
        P(),
        P(),
        P(),
        P(),
        P(),
    )
    out_specs = (
        P("dp", None),
        P("dp", None),
        P(None, "dp", "mp"),
        P(None, "mp"),
        P("mp", "dp"),
        P(),
        P("dp", "mp"),
        P("mp"),
        P("mp", "dp"),
        P(),
        P(),
        P(),
        P(),
        P(),
    )
    return jax.shard_map(
        partial(per_device, mesh.shape["mp"]), mesh=mesh, in_specs=in_specs, out_specs=out_specs, check_vma=False
    )
```

```python
from functools import partial

import jax
import jax.numpy as jnp
from jax import lax
from jax.experimental import pallas as pl
from jax.experimental.pallas import tpu as pltpu
from jax.sharding import PartitionSpec as P

HEAD = 64
QBLOCK = 512
TQ = 256
TK = 256
NEG = -1e30


def _nt(a, b):
    return lax.dot_general(a, b, (((1,), (1,)), ((), ())), preferred_element_type=jnp.float32)


def _lanes(values, width):
    return jnp.tile(values, (1, width // 128))


def _fwd_kernel(lo_ref, hi_ref, segc_ref, segr_ref, q_ref, k_ref, v_ref, o_ref, o32_ref, lse_ref):
    rows = q_ref.shape[1]
    scale = HEAD ** (-0.5)

    def q_body(i, carry):
        r0 = pl.multiple_of(i * TQ, TQ)
        q = q_ref[0, pl.ds(r0, TQ), :]
        sq = segc_ref[pl.ds(r0, TQ), :]

        def kv_body(j, state):
            m, l, acc = state
            c0 = pl.multiple_of(j * TK, TK)
            s = _nt(q, k_ref[0, pl.ds(c0, TK), :]) * scale
            same = sq == segr_ref[:, pl.ds(c0, TK)]
            s = jnp.where(same, s, NEG)
            m_new = jnp.maximum(m, jnp.max(s, axis=-1, keepdims=True))
            p = jnp.exp(s - _lanes(m_new, TK))
            alpha = jnp.exp(m - m_new)
            l = alpha * l + jnp.sum(p, axis=-1, keepdims=True)
            pv = jnp.dot(p.astype(jnp.bfloat16), v_ref[0, pl.ds(c0, TK), :],
                         preferred_element_type=jnp.float32)
            acc = alpha[:, :HEAD] * acc + pv
            return m_new, l, acc

        m0 = jnp.full((TQ, 128), NEG, jnp.float32)
        l0 = jnp.zeros((TQ, 128), jnp.float32)
        acc0 = jnp.zeros((TQ, HEAD), jnp.float32)
        m, l, acc = lax.fori_loop(lo_ref[i], hi_ref[i], kv_body, (m0, l0, acc0))
        out = acc / l[:, :HEAD]
        o_ref[0, pl.ds(r0, TQ), :] = out.astype(o_ref.dtype)
        o32_ref[0, pl.ds(r0, TQ), :] = out
        lse_ref[0, pl.ds(r0, TQ), :] = (m + jnp.log(l))[:, :1]
        return carry

    lax.fori_loop(0, rows // TQ, q_body, 0)


def _bwd_kernel(lo_ref, hi_ref, segc_ref, segr_ref, q_ref, k_ref, v_ref, do_ref, o32_ref, lse_ref,
                dq_ref, dk_ref, dv_ref):
    rows = q_ref.shape[1]
    scale = HEAD ** (-0.5)
    dk_ref[...] = jnp.zeros_like(dk_ref)
    dv_ref[...] = jnp.zeros_like(dv_ref)

    def q_body(i, carry):
        r0 = pl.multiple_of(i * TQ, TQ)
        q = q_ref[0, pl.ds(r0, TQ), :]
        do = do_ref[0, pl.ds(r0, TQ), :]
        sq = segc_ref[pl.ds(r0, TQ), :]
        lse = _lanes(jnp.broadcast_to(lse_ref[0, pl.ds(r0, TQ), :], (TQ, 128)), TK)
        dvec = jnp.sum(do.astype(jnp.float32) * o32_ref[0, pl.ds(r0, TQ), :], axis=-1, keepdims=True)
        dvec = _lanes(jnp.broadcast_to(dvec, (TQ, 128)), TK)

        def kv_body(j, dq):
            c0 = pl.multiple_of(j * TK, TK)
            k = k_ref[0, pl.ds(c0, TK), :]
            v = v_ref[0, pl.ds(c0, TK), :]
            s = _nt(q, k) * scale
            same = sq == segr_ref[:, pl.ds(c0, TK)]
            s = jnp.where(same, s, NEG)
            p = jnp.exp(s - lse)
            dp = _nt(do, v)
            ds = p * (dp - dvec)
            dq = dq + jnp.dot(ds.astype(jnp.bfloat16), k, preferred_element_type=jnp.float32)
            dk_ref[0, pl.ds(c0, TK), :] += jnp.dot(
                ds.T.astype(jnp.bfloat16), q, preferred_element_type=jnp.float32)
            dv_ref[0, pl.ds(c0, TK), :] += jnp.dot(
                p.T.astype(jnp.bfloat16), do, preferred_element_type=jnp.float32)
            return dq

        dq = lax.fori_loop(lo_ref[i], hi_ref[i], kv_body, jnp.zeros((TQ, HEAD), jnp.float32))
        dq_ref[0, pl.ds(r0, TQ), :] = dq * scale
        return carry

    lax.fori_loop(0, rows // TQ, q_body, 0)
    dk_ref[...] = dk_ref[...] * scale


def block_ranges(segments, item_lengths_row):
    rows = segments.shape[0]
    ends = jnp.cumsum(item_lengths_row.astype(jnp.int32))
    starts = ends - item_lengths_row.astype(jnp.int32)
    first = segments[0::TQ]
    last = segments[TQ - 1::TQ]
    n_items = item_lengths_row.shape[0]
    key_lo = jnp.take(starts, jnp.clip(first, 0, n_items - 1))
    key_hi = jnp.take(ends, jnp.clip(last, 0, n_items - 1))
    lo = jnp.clip(key_lo // TK, 0, rows // TK)
    hi = jnp.clip((key_hi + TK - 1) // TK, 0, rows // TK)
    return lo.astype(jnp.int32), hi.astype(jnp.int32)


def flash_forward(q, k, v, segments, lo, hi):
    heads, rows, _ = q.shape
    head_spec = pl.BlockSpec((1, rows, HEAD), lambda h, lo, hi: (h, 0, 0))
    lse_spec = pl.BlockSpec((1, rows, 1), lambda h, lo, hi: (h, 0, 0))
    col_spec = pl.BlockSpec((rows, 1), lambda h, lo, hi: (0, 0))
    row_spec = pl.BlockSpec((1, rows), lambda h, lo, hi: (0, 0))
    flops = int(heads * rows * rows * HEAD * 2 * 3 * 0.6)
    return pl.pallas_call(
        _fwd_kernel,
        out_shape=(
            jax.ShapeDtypeStruct((heads, rows, HEAD), jnp.bfloat16),
            jax.ShapeDtypeStruct((heads, rows, HEAD), jnp.float32),
            jax.ShapeDtypeStruct((heads, rows, 1), jnp.float32),
        ),
        grid_spec=pltpu.PrefetchScalarGridSpec(
            num_scalar_prefetch=2,
            grid=(heads,),
            in_specs=[col_spec, row_spec, head_spec, head_spec, head_spec],
            out_specs=[head_spec, head_spec, lse_spec],
        ),
        compiler_params=pltpu.CompilerParams(
            dimension_semantics=("arbitrary",), vmem_limit_bytes=48 * 1024 * 1024),
        cost_estimate=pl.CostEstimate(
            flops=flops, transcendentals=int(heads * rows * rows * 0.6 * 2),
            bytes_accessed=int(heads * rows * HEAD * (2 * 4 + 4) + heads * rows * 4)),
        name="segment_flash_fwd",
    )(lo, hi, segments.reshape(rows, 1), segments.reshape(1, rows), q, k, v)


def flash_backward(q, k, v, do, o32, lse, segments, lo, hi):
    heads, rows, _ = q.shape
    head_spec = pl.BlockSpec((1, rows, HEAD), lambda h, lo, hi: (h, 0, 0))
    lse_spec = pl.BlockSpec((1, rows, 1), lambda h, lo, hi: (h, 0, 0))
    col_spec = pl.BlockSpec((rows, 1), lambda h, lo, hi: (0, 0))
    row_spec = pl.BlockSpec((1, rows), lambda h, lo, hi: (0, 0))
    flops = int(heads * rows * rows * HEAD * 2 * 5 * 0.6)
    out = jax.ShapeDtypeStruct((heads, rows, HEAD), jnp.float32)
    return pl.pallas_call(
        _bwd_kernel,
        out_shape=(out, out, out),
        grid_spec=pltpu.PrefetchScalarGridSpec(
            num_scalar_prefetch=2,
            grid=(heads,),
            in_specs=[col_spec, row_spec, head_spec, head_spec, head_spec, head_spec, head_spec, lse_spec],
            out_specs=[head_spec, head_spec, head_spec],
        ),
        compiler_params=pltpu.CompilerParams(
            dimension_semantics=("arbitrary",), vmem_limit_bytes=48 * 1024 * 1024),
        cost_estimate=pl.CostEstimate(
            flops=flops, transcendentals=int(heads * rows * rows * 0.6),
            bytes_accessed=int(heads * rows * HEAD * (4 * 2 + 4 * 4) + heads * rows * 4)),
        name="segment_flash_bwd",
    )(lo, hi, segments.reshape(rows, 1), segments.reshape(1, rows), q, k, v, do, o32, lse)


def normalize(values, gain, shift):
    center = jnp.mean(values, axis=-1, keepdims=True)
    centered = values - center
    spread = jnp.mean(centered * centered, axis=-1, keepdims=True)
    return centered * lax.rsqrt(spread + 1e-06) * gain + shift


def exact_gelu(values):
    return jax.nn.gelu(values, approximate=False)


def segment_ids(lengths_row, row_count):
    ends = jnp.cumsum(lengths_row)
    positions = jnp.arange(row_count, dtype=jnp.int32)
    return jnp.sum((positions[:, None] >= ends[None, :]).astype(jnp.int32), axis=1)


def mp_allreduce(partial, n_mp):
    if n_mp != 4:
        return lax.psum(partial, "mp").astype(jnp.float32)
    idx = lax.axis_index("mp")
    low_bit = idx % 2
    half = partial.shape[0] // 2
    mine = lax.dynamic_slice_in_dim(partial, low_bit * half, half, 0)
    other = lax.dynamic_slice_in_dim(partial, (1 - low_bit) * half, half, 0)
    got = lax.ppermute(other, "mp", [(k, k ^ 1) for k in range(4)])
    first = (mine.astype(jnp.float32) + got.astype(jnp.float32)).astype(jnp.bfloat16)
    got_far = lax.ppermute(first, "mp", [(k, k ^ 2) for k in range(4)])
    second = (first.astype(jnp.float32) + got_far.astype(jnp.float32)).astype(jnp.bfloat16)
    got_back = lax.ppermute(second, "mp", [(k, k ^ 1) for k in range(4)])
    top = jnp.where(low_bit == 0, second, got_back)
    bottom = jnp.where(low_bit == 0, got_back, second)
    return jnp.concatenate([top, bottom], axis=0).astype(jnp.float32)


def per_device(n_mp,

    tokens,
    cotangent,
    item_lengths,
    w_qkv,
    b_qv,
    w_out,
    b_out,
    w_fc1,
    b_fc1,
    w_fc2,
    b_fc2,
    ln1_gain,
    ln1_bias,
    ln2_gain,
    ln2_bias,
):
    row_count = tokens.shape[0]
    local_cols = w_qkv.shape[2]
    heads_here = local_cols // HEAD
    segments = segment_ids(item_lengths[0], row_count)
    inputs = tokens.astype(jnp.float32)
    norm_one, norm_one_back = jax.vjp(normalize, inputs, ln1_gain, ln1_bias)
    normed_one = norm_one.astype(jnp.bfloat16)
    queries = (jnp.dot(normed_one, w_qkv[0], preferred_element_type=jnp.float32) + b_qv[0]).astype(
        jnp.bfloat16
    )
    key_rows = jnp.dot(normed_one, w_qkv[1], preferred_element_type=jnp.float32).astype(
        jnp.bfloat16
    )
    value_rows = (
        jnp.dot(normed_one, w_qkv[2], preferred_element_type=jnp.float32) + b_qv[1]
    ).astype(jnp.bfloat16)
    def to_heads(values):
        return values.reshape(row_count, heads_here, HEAD).transpose(1, 0, 2)

    def from_heads(values):
        return values.transpose(1, 0, 2).reshape(row_count, local_cols)

    lo_blocks, hi_blocks = block_ranges(segments, item_lengths[0])
    query_heads = to_heads(queries)
    key_heads = to_heads(key_rows)
    value_heads = to_heads(value_rows)
    out_heads, out_f32, log_norms = flash_forward(
        query_heads, key_heads, value_heads, segments, lo_blocks, hi_blocks
    )
    attended = from_heads(out_heads)
    attention_sum = mp_allreduce(
        jnp.dot(attended, w_out, preferred_element_type=jnp.float32).astype(jnp.bfloat16), n_mp
    )
    middle = inputs + attention_sum + b_out
    norm_two, norm_two_back = jax.vjp(normalize, middle, ln2_gain, ln2_bias)
    normed_two = norm_two.astype(jnp.bfloat16)
    hidden_pre = jnp.dot(normed_two, w_fc1, preferred_element_type=jnp.float32) + b_fc1
    activated_full, gelu_back = jax.vjp(exact_gelu, hidden_pre)
    activated = activated_full.astype(jnp.bfloat16)
    mlp_sum = mp_allreduce(
        jnp.dot(activated, w_fc2, preferred_element_type=jnp.float32).astype(jnp.bfloat16), n_mp
    )
    output = (middle + mlp_sum + b_fc2).astype(jnp.bfloat16)
    upstream = cotangent.astype(jnp.float32)
    grad_b_fc2 = jnp.sum(upstream, axis=0)
    grad_w_fc2 = jnp.einsum("tf,td->fd", activated, cotangent, preferred_element_type=jnp.float32)
    d_act = jnp.einsum("td,fd->tf", cotangent, w_fc2, preferred_element_type=jnp.float32)
    d_pre = gelu_back(d_act)[0]
    grad_b_fc1 = jnp.sum(d_pre, axis=0)
    d_pre_low = d_pre.astype(jnp.bfloat16)
    grad_w_fc1 = jnp.einsum("td,tf->df", normed_two, d_pre_low, preferred_element_type=jnp.float32)
    d_normed_two = mp_allreduce(
        jnp.einsum("tf,df->td", d_pre_low, w_fc1, preferred_element_type=jnp.float32).astype(
            jnp.bfloat16
        ),
        n_mp,
    )
    d_middle_norm, grad_ln2_gain, grad_ln2_bias = norm_two_back(d_normed_two)
    d_middle = upstream + d_middle_norm
    grad_b_out = jnp.sum(d_middle, axis=0)
    d_middle_low = d_middle.astype(jnp.bfloat16)
    grad_w_out = jnp.einsum("tc,td->cd", attended, d_middle_low, preferred_element_type=jnp.float32)
    d_attended = jnp.einsum(
        "td,cd->tc", d_middle_low, w_out, preferred_element_type=jnp.float32
    ).astype(jnp.bfloat16)
    d_q_heads, d_k_heads, d_v_heads = flash_backward(
        query_heads, key_heads, value_heads, to_heads(d_attended), out_f32, log_norms,
        segments, lo_blocks, hi_blocks,
    )
    d_queries = from_heads(d_q_heads)
    d_keys = from_heads(d_k_heads)
    d_values = from_heads(d_v_heads)
    grad_b_qv = jnp.stack([jnp.sum(d_queries, axis=0), jnp.sum(d_values, axis=0)])
    stacked = jnp.stack([d_queries, d_keys, d_values]).astype(jnp.bfloat16)
    grad_w_qkv = jnp.einsum("td,stc->sdc", normed_one, stacked, preferred_element_type=jnp.float32)
    d_normed_one = mp_allreduce(
        jnp.einsum("stc,sdc->td", stacked, w_qkv, preferred_element_type=jnp.float32).astype(
            jnp.bfloat16
        ),
        n_mp,
    )
    d_input_norm, grad_ln1_gain, grad_ln1_bias = norm_one_back(d_normed_one)
    grad_tokens = d_middle + d_input_norm
    def scatter(grad, dim):
        return lax.psum_scatter(
            grad.astype(jnp.bfloat16), "dp", scatter_dimension=dim, tiled=True
        ).astype(jnp.float32)

    summed_qkv = scatter(grad_w_qkv, 1)
    summed_out = scatter(grad_w_out, 1)
    summed_fc1 = scatter(grad_w_fc1, 0)
    summed_fc2 = scatter(grad_w_fc2, 1)
    packed = jnp.concatenate(
        [
            grad_ln1_gain,
            grad_ln1_bias,
            grad_ln2_gain,
            grad_ln2_bias,
            grad_b_out,
            grad_b_fc2,
            grad_b_qv.reshape(-1),
            grad_b_fc1,
        ]
    )
    packed = lax.psum(packed, "dp")
    width = grad_ln1_gain.shape[0]
    pieces = [packed[k * width : (k + 1) * width] for k in range(6)]
    qv_size = grad_b_qv.size
    summed_b_qv = packed[6 * width : 6 * width + qv_size].reshape(grad_b_qv.shape)
    summed_b_fc1 = packed[6 * width + qv_size :]
    return (
        output,
        grad_tokens,
        summed_qkv,
        summed_b_qv,
        summed_out,
        pieces[4],
        summed_fc1,
        summed_b_fc1,
        summed_fc2,
        pieces[5],
        pieces[0],
        pieces[1],
        pieces[2],
        pieces[3],
    )


def solution(mesh):
    in_specs = (
        P("dp", None),
        P("dp", None),
        P("dp", None),
        P(None, None, "mp"),
        P(None, "mp"),
        P("mp", None),
        P(),
        P(None, "mp"),
        P("mp"),
        P("mp", None),
        P(),
        P(),
        P(),
        P(),
        P(),
    )
    out_specs = (
        P("dp", None),
        P("dp", None),
        P(None, "dp", "mp"),
        P(None, "mp"),
        P("mp", "dp"),
        P(),
        P("dp", "mp"),
        P("mp"),
        P("mp", "dp"),
        P(),
        P(),
        P(),
        P(),
        P(),
    )
    return jax.shard_map(
        partial(per_device, mesh.shape["mp"]), mesh=mesh, in_specs=in_specs, out_specs=out_specs, check_vma=False
    )
```

```python
from functools import partial

import jax
import jax.numpy as jnp
from jax import lax
from jax.experimental import pallas as pl
from jax.experimental.pallas import tpu as pltpu
from jax.sharding import PartitionSpec as P

HEAD = 64
QBLOCK = 512
TQ = 256
TK = 256
NEG = -1e30


def _fwd_kernel(lo_ref, hi_ref, segc_ref, segr_ref, qt_ref, k_ref, vt_ref, ot_ref, o32t_ref, lse_ref):
    rows = qt_ref.shape[2]
    scale = HEAD ** (-0.5)

    def q_body(i, carry):
        r0 = pl.multiple_of(i * TQ, TQ)
        qt = qt_ref[0, :, pl.ds(r0, TQ)]
        sq = segr_ref[:, pl.ds(r0, TQ)]

        def kv_body(j, state):
            m, l, acc = state
            c0 = pl.multiple_of(j * TK, TK)
            s = jnp.dot(k_ref[0, pl.ds(c0, TK), :], qt, preferred_element_type=jnp.float32) * scale
            same = segc_ref[pl.ds(c0, TK), :] == sq
            s = jnp.where(same, s, NEG)
            m_new = jnp.maximum(m, jnp.max(s, axis=0, keepdims=True))
            p = jnp.exp(s - m_new)
            alpha = jnp.exp(m - m_new)
            l = alpha * l + jnp.sum(p, axis=0, keepdims=True)
            pv = jnp.dot(vt_ref[0, :, pl.ds(c0, TK)], p.astype(jnp.bfloat16),
                         preferred_element_type=jnp.float32)
            return m_new, l, alpha * acc + pv

        m0 = jnp.full((1, TQ), NEG, jnp.float32)
        l0 = jnp.zeros((1, TQ), jnp.float32)
        acc0 = jnp.zeros((HEAD, TQ), jnp.float32)
        m, l, acc = lax.fori_loop(lo_ref[i], hi_ref[i], kv_body, (m0, l0, acc0))
        out = acc / l
        ot_ref[0, :, pl.ds(r0, TQ)] = out.astype(ot_ref.dtype)
        o32t_ref[0, :, pl.ds(r0, TQ)] = out
        lse_ref[0, :, pl.ds(r0, TQ)] = m + jnp.log(l)
        return carry

    lax.fori_loop(0, rows // TQ, q_body, 0)


def _bwd_kernel(lo_ref, hi_ref, segc_ref, segr_ref, q_ref, qt_ref, k_ref, kt_ref, v_ref, do_ref, dot_ref,
                o32t_ref, lse_ref, dqt_ref, dk_ref, dv_ref, dvec_ref):
    rows = q_ref.shape[1]
    scale = HEAD ** (-0.5)
    dqt_ref[...] = jnp.zeros_like(dqt_ref)

    def d_body(i, carry):
        r0 = pl.multiple_of(i * TQ, TQ)
        prod = dot_ref[0, :, pl.ds(r0, TQ)].astype(jnp.float32) * o32t_ref[0, :, pl.ds(r0, TQ)]
        dvec_ref[:, pl.ds(r0, TQ)] = jnp.sum(prod, axis=0, keepdims=True)
        return carry

    lax.fori_loop(0, rows // TQ, d_body, 0)

    def kv_body(j, carry):
        c0 = pl.multiple_of(j * TK, TK)
        k = k_ref[0, pl.ds(c0, TK), :]
        v = v_ref[0, pl.ds(c0, TK), :]
        kt = kt_ref[0, :, pl.ds(c0, TK)]
        sk = segc_ref[pl.ds(c0, TK), :]

        def q_body(i, grads):
            dk, dv = grads
            r0 = pl.multiple_of(i * TQ, TQ)
            s = jnp.dot(k, qt_ref[0, :, pl.ds(r0, TQ)], preferred_element_type=jnp.float32) * scale
            same = sk == segr_ref[:, pl.ds(r0, TQ)]
            s = jnp.where(same, s, NEG)
            p = jnp.exp(s - lse_ref[0, :, pl.ds(r0, TQ)])
            dp = jnp.dot(v, dot_ref[0, :, pl.ds(r0, TQ)], preferred_element_type=jnp.float32)
            ds = (p * (dp - dvec_ref[:, pl.ds(r0, TQ)])).astype(jnp.bfloat16)
            dv = dv + jnp.dot(p.astype(jnp.bfloat16), do_ref[0, pl.ds(r0, TQ), :],
                              preferred_element_type=jnp.float32)
            dk = dk + jnp.dot(ds, q_ref[0, pl.ds(r0, TQ), :], preferred_element_type=jnp.float32)
            dqt_ref[0, :, pl.ds(r0, TQ)] += jnp.dot(kt, ds, preferred_element_type=jnp.float32)
            return dk, dv

        zeros = jnp.zeros((TK, HEAD), jnp.float32)
        dk, dv = lax.fori_loop(lo_ref[j], hi_ref[j], q_body, (zeros, zeros))
        dk_ref[0, pl.ds(c0, TK), :] = dk * scale
        dv_ref[0, pl.ds(c0, TK), :] = dv
        return carry

    lax.fori_loop(0, rows // TK, kv_body, 0)
    dqt_ref[...] = dqt_ref[...] * scale


def block_ranges(segments, item_lengths_row):
    rows = segments.shape[0]
    ends = jnp.cumsum(item_lengths_row.astype(jnp.int32))
    starts = ends - item_lengths_row.astype(jnp.int32)
    first = segments[0::TQ]
    last = segments[TQ - 1::TQ]
    n_items = item_lengths_row.shape[0]
    key_lo = jnp.take(starts, jnp.clip(first, 0, n_items - 1))
    key_hi = jnp.take(ends, jnp.clip(last, 0, n_items - 1))
    lo = jnp.clip(key_lo // TK, 0, rows // TK)
    hi = jnp.clip((key_hi + TK - 1) // TK, 0, rows // TK)
    return lo.astype(jnp.int32), hi.astype(jnp.int32)


def _head_specs(rows):
    plain = pl.BlockSpec((1, rows, HEAD), lambda h, lo, hi: (h, 0, 0))
    flipped = pl.BlockSpec((1, HEAD, rows), lambda h, lo, hi: (h, 0, 0))
    stat = pl.BlockSpec((1, 1, rows), lambda h, lo, hi: (h, 0, 0))
    col = pl.BlockSpec((rows, 1), lambda h, lo, hi: (0, 0))
    row = pl.BlockSpec((1, rows), lambda h, lo, hi: (0, 0))
    return plain, flipped, stat, col, row


def flash_forward(q, k, v, segments, lo, hi):
    heads, rows, _ = q.shape
    plain, flipped, stat, col, row = _head_specs(rows)
    flops = int(heads * rows * rows * HEAD * 2 * 2 * 0.6)
    return pl.pallas_call(
        _fwd_kernel,
        out_shape=(
            jax.ShapeDtypeStruct((heads, HEAD, rows), jnp.bfloat16),
            jax.ShapeDtypeStruct((heads, HEAD, rows), jnp.float32),
            jax.ShapeDtypeStruct((heads, 1, rows), jnp.float32),
        ),
        grid_spec=pltpu.PrefetchScalarGridSpec(
            num_scalar_prefetch=2,
            grid=(heads,),
            in_specs=[col, row, flipped, plain, flipped],
            out_specs=[flipped, flipped, stat],
        ),
        compiler_params=pltpu.CompilerParams(
            dimension_semantics=("arbitrary",), vmem_limit_bytes=48 * 1024 * 1024),
        cost_estimate=pl.CostEstimate(
            flops=flops, transcendentals=int(heads * rows * rows * 0.6),
            bytes_accessed=int(heads * rows * HEAD * (2 * 4 + 4) + heads * rows * 4)),
        name="segment_flash_fwd",
    )(lo, hi, segments.reshape(rows, 1), segments.reshape(1, rows),
      q.transpose(0, 2, 1), k, v.transpose(0, 2, 1))


def flash_backward(q, k, v, do, o32t, lse, segments, lo, hi):
    heads, rows, _ = q.shape
    plain, flipped, stat, col, row = _head_specs(rows)
    flops = int(heads * rows * rows * HEAD * 2 * 4 * 0.6)
    return pl.pallas_call(
        _bwd_kernel,
        out_shape=(
            jax.ShapeDtypeStruct((heads, HEAD, rows), jnp.float32),
            jax.ShapeDtypeStruct((heads, rows, HEAD), jnp.float32),
            jax.ShapeDtypeStruct((heads, rows, HEAD), jnp.float32),
        ),
        grid_spec=pltpu.PrefetchScalarGridSpec(
            num_scalar_prefetch=2,
            grid=(heads,),
            in_specs=[col, row, plain, flipped, plain, flipped, plain, plain, flipped, flipped, stat],
            out_specs=[flipped, plain, plain],
            scratch_shapes=[pltpu.VMEM((1, rows), jnp.float32)],
        ),
        compiler_params=pltpu.CompilerParams(
            dimension_semantics=("arbitrary",), vmem_limit_bytes=48 * 1024 * 1024),
        cost_estimate=pl.CostEstimate(
            flops=flops, transcendentals=int(heads * rows * rows * 0.6),
            bytes_accessed=int(heads * rows * HEAD * (2 * 7 + 4 * 4) + heads * rows * 4)),
        name="segment_flash_bwd",
    )(lo, hi, segments.reshape(rows, 1), segments.reshape(1, rows),
      q, q.transpose(0, 2, 1), k, k.transpose(0, 2, 1), v, do, do.transpose(0, 2, 1), o32t, lse)

def normalize(values, gain, shift):
    center = jnp.mean(values, axis=-1, keepdims=True)
    centered = values - center
    spread = jnp.mean(centered * centered, axis=-1, keepdims=True)
    return centered * lax.rsqrt(spread + 1e-06) * gain + shift


def exact_gelu(values):
    return jax.nn.gelu(values, approximate=False)


def segment_ids(lengths_row, row_count):
    ends = jnp.cumsum(lengths_row)
    positions = jnp.arange(row_count, dtype=jnp.int32)
    return jnp.sum((positions[:, None] >= ends[None, :]).astype(jnp.int32), axis=1)


def mp_allreduce(partial, n_mp):
    if n_mp != 4:
        return lax.psum(partial, "mp").astype(jnp.float32)
    idx = lax.axis_index("mp")
    low_bit = idx % 2
    half = partial.shape[0] // 2
    mine = lax.dynamic_slice_in_dim(partial, low_bit * half, half, 0)
    other = lax.dynamic_slice_in_dim(partial, (1 - low_bit) * half, half, 0)
    got = lax.ppermute(other, "mp", [(k, k ^ 1) for k in range(4)])
    first = (mine.astype(jnp.float32) + got.astype(jnp.float32)).astype(jnp.bfloat16)
    got_far = lax.ppermute(first, "mp", [(k, k ^ 2) for k in range(4)])
    second = (first.astype(jnp.float32) + got_far.astype(jnp.float32)).astype(jnp.bfloat16)
    got_back = lax.ppermute(second, "mp", [(k, k ^ 1) for k in range(4)])
    top = jnp.where(low_bit == 0, second, got_back)
    bottom = jnp.where(low_bit == 0, got_back, second)
    return jnp.concatenate([top, bottom], axis=0).astype(jnp.float32)


def per_device(n_mp,

    tokens,
    cotangent,
    item_lengths,
    w_qkv,
    b_qv,
    w_out,
    b_out,
    w_fc1,
    b_fc1,
    w_fc2,
    b_fc2,
    ln1_gain,
    ln1_bias,
    ln2_gain,
    ln2_bias,
):
    row_count = tokens.shape[0]
    local_cols = w_qkv.shape[2]
    heads_here = local_cols // HEAD
    segments = segment_ids(item_lengths[0], row_count)
    inputs = tokens.astype(jnp.float32)
    norm_one, norm_one_back = jax.vjp(normalize, inputs, ln1_gain, ln1_bias)
    normed_one = norm_one.astype(jnp.bfloat16)
    queries = (jnp.dot(normed_one, w_qkv[0], preferred_element_type=jnp.float32) + b_qv[0]).astype(
        jnp.bfloat16
    )
    key_rows = jnp.dot(normed_one, w_qkv[1], preferred_element_type=jnp.float32).astype(
        jnp.bfloat16
    )
    value_rows = (
        jnp.dot(normed_one, w_qkv[2], preferred_element_type=jnp.float32) + b_qv[1]
    ).astype(jnp.bfloat16)
    def to_heads(values):
        return values.reshape(row_count, heads_here, HEAD).transpose(1, 0, 2)

    def from_heads(values):
        return values.transpose(1, 0, 2).reshape(row_count, local_cols)

    lo_blocks, hi_blocks = block_ranges(segments, item_lengths[0])
    query_heads = to_heads(queries)
    key_heads = to_heads(key_rows)
    value_heads = to_heads(value_rows)
    out_heads, out_f32, log_norms = flash_forward(
        query_heads, key_heads, value_heads, segments, lo_blocks, hi_blocks
    )
    attended = out_heads.transpose(2, 0, 1).reshape(row_count, local_cols)
    attention_sum = mp_allreduce(
        jnp.dot(attended, w_out, preferred_element_type=jnp.float32).astype(jnp.bfloat16), n_mp
    )
    middle = inputs + attention_sum + b_out
    norm_two, norm_two_back = jax.vjp(normalize, middle, ln2_gain, ln2_bias)
    normed_two = norm_two.astype(jnp.bfloat16)
    hidden_pre = jnp.dot(normed_two, w_fc1, preferred_element_type=jnp.float32) + b_fc1
    activated_full, gelu_back = jax.vjp(exact_gelu, hidden_pre)
    activated = activated_full.astype(jnp.bfloat16)
    mlp_sum = mp_allreduce(
        jnp.dot(activated, w_fc2, preferred_element_type=jnp.float32).astype(jnp.bfloat16), n_mp
    )
    output = (middle + mlp_sum + b_fc2).astype(jnp.bfloat16)
    upstream = cotangent.astype(jnp.float32)
    grad_b_fc2 = jnp.sum(upstream, axis=0)
    grad_w_fc2 = jnp.einsum("tf,td->fd", activated, cotangent, preferred_element_type=jnp.float32)
    d_act = jnp.einsum("td,fd->tf", cotangent, w_fc2, preferred_element_type=jnp.float32)
    d_pre = gelu_back(d_act)[0]
    grad_b_fc1 = jnp.sum(d_pre, axis=0)
    d_pre_low = d_pre.astype(jnp.bfloat16)
    grad_w_fc1 = jnp.einsum("td,tf->df", normed_two, d_pre_low, preferred_element_type=jnp.float32)
    d_normed_two = mp_allreduce(
        jnp.einsum("tf,df->td", d_pre_low, w_fc1, preferred_element_type=jnp.float32).astype(
            jnp.bfloat16
        ),
        n_mp,
    )
    d_middle_norm, grad_ln2_gain, grad_ln2_bias = norm_two_back(d_normed_two)
    d_middle = upstream + d_middle_norm
    grad_b_out = jnp.sum(d_middle, axis=0)
    d_middle_low = d_middle.astype(jnp.bfloat16)
    grad_w_out = jnp.einsum("tc,td->cd", attended, d_middle_low, preferred_element_type=jnp.float32)
    d_attended = jnp.einsum(
        "td,cd->tc", d_middle_low, w_out, preferred_element_type=jnp.float32
    ).astype(jnp.bfloat16)
    d_q_heads, d_k_heads, d_v_heads = flash_backward(
        query_heads, key_heads, value_heads, to_heads(d_attended), out_f32, log_norms,
        segments, lo_blocks, hi_blocks,
    )
    d_queries = d_q_heads.transpose(2, 0, 1).reshape(row_count, local_cols)
    d_keys = from_heads(d_k_heads)
    d_values = from_heads(d_v_heads)
    grad_b_qv = jnp.stack([jnp.sum(d_queries, axis=0), jnp.sum(d_values, axis=0)])
    stacked = jnp.stack([d_queries, d_keys, d_values]).astype(jnp.bfloat16)
    grad_w_qkv = jnp.einsum("td,stc->sdc", normed_one, stacked, preferred_element_type=jnp.float32)
    d_normed_one = mp_allreduce(
        jnp.einsum("stc,sdc->td", stacked, w_qkv, preferred_element_type=jnp.float32).astype(
            jnp.bfloat16
        ),
        n_mp,
    )
    d_input_norm, grad_ln1_gain, grad_ln1_bias = norm_one_back(d_normed_one)
    grad_tokens = d_middle + d_input_norm
    def scatter(grad, dim):
        return lax.psum_scatter(
            grad.astype(jnp.bfloat16), "dp", scatter_dimension=dim, tiled=True
        ).astype(jnp.float32)

    summed_qkv = scatter(grad_w_qkv, 1)
    summed_out = scatter(grad_w_out, 1)
    summed_fc1 = scatter(grad_w_fc1, 0)
    summed_fc2 = scatter(grad_w_fc2, 1)
    packed = jnp.concatenate(
        [
            grad_ln1_gain,
            grad_ln1_bias,
            grad_ln2_gain,
            grad_ln2_bias,
            grad_b_out,
            grad_b_fc2,
            grad_b_qv.reshape(-1),
            grad_b_fc1,
        ]
    )
    packed = lax.psum(packed, "dp")
    width = grad_ln1_gain.shape[0]
    pieces = [packed[k * width : (k + 1) * width] for k in range(6)]
    qv_size = grad_b_qv.size
    summed_b_qv = packed[6 * width : 6 * width + qv_size].reshape(grad_b_qv.shape)
    summed_b_fc1 = packed[6 * width + qv_size :]
    return (
        output,
        grad_tokens,
        summed_qkv,
        summed_b_qv,
        summed_out,
        pieces[4],
        summed_fc1,
        summed_b_fc1,
        summed_fc2,
        pieces[5],
        pieces[0],
        pieces[1],
        pieces[2],
        pieces[3],
    )


def solution(mesh):
    in_specs = (
        P("dp", None),
        P("dp", None),
        P("dp", None),
        P(None, None, "mp"),
        P(None, "mp"),
        P("mp", None),
        P(),
        P(None, "mp"),
        P("mp"),
        P("mp", None),
        P(),
        P(),
        P(),
        P(),
        P(),
    )
    out_specs = (
        P("dp", None),
        P("dp", None),
        P(None, "dp", "mp"),
        P(None, "mp"),
        P("mp", "dp"),
        P(),
        P("dp", "mp"),
        P("mp"),
        P("mp", "dp"),
        P(),
        P(),
        P(),
        P(),
        P(),
    )
    return jax.shard_map(
        partial(per_device, mesh.shape["mp"]), mesh=mesh, in_specs=in_specs, out_specs=out_specs, check_vma=False
    )
```

```python
from functools import partial

import jax
import jax.numpy as jnp
from jax import lax
from jax.experimental import pallas as pl
from jax.experimental.pallas import tpu as pltpu
from jax.sharding import PartitionSpec as P

HEAD = 64
QBLOCK = 512
TQ = 256
TK = 256
NEG = -1e30


def _fwd_kernel(lo_ref, hi_ref, segc_ref, segr_ref, qt_ref, k_ref, vt_ref, ot_ref, o32t_ref, lse_ref):
    rows = qt_ref.shape[2]
    scale = HEAD ** (-0.5)

    def q_body(i, carry):
        r0 = pl.multiple_of(i * TQ, TQ)
        qt = qt_ref[0, :, pl.ds(r0, TQ)]
        sq = segr_ref[:, pl.ds(r0, TQ)]

        def kv_body(j, state):
            m, l, acc = state
            c0 = pl.multiple_of(j * TK, TK)
            s = jnp.dot(k_ref[0, pl.ds(c0, TK), :], qt, preferred_element_type=jnp.float32) * scale
            same = segc_ref[pl.ds(c0, TK), :] == sq
            s = jnp.where(same, s, NEG)
            m_new = jnp.maximum(m, jnp.max(s, axis=0, keepdims=True))
            p = jnp.exp(s - m_new)
            alpha = jnp.exp(m - m_new)
            l = alpha * l + jnp.sum(p, axis=0, keepdims=True)
            pv = jnp.dot(vt_ref[0, :, pl.ds(c0, TK)], p.astype(jnp.bfloat16),
                         preferred_element_type=jnp.float32)
            return m_new, l, alpha * acc + pv

        m0 = jnp.full((1, TQ), NEG, jnp.float32)
        l0 = jnp.zeros((1, TQ), jnp.float32)
        acc0 = jnp.zeros((HEAD, TQ), jnp.float32)
        m, l, acc = lax.fori_loop(lo_ref[i], hi_ref[i], kv_body, (m0, l0, acc0))
        out = acc / l
        ot_ref[0, :, pl.ds(r0, TQ)] = out.astype(ot_ref.dtype)
        o32t_ref[0, :, pl.ds(r0, TQ)] = out
        lse_ref[0, :, pl.ds(r0, TQ)] = m + jnp.log(l)
        return carry

    lax.fori_loop(0, rows // TQ, q_body, 0)


def _bwd_kernel(lo_ref, hi_ref, segc_ref, segr_ref, q_ref, qt_ref, k_ref, kt_ref, v_ref, do_ref, dot_ref,
                o32t_ref, lse_ref, dqt_ref, dk_ref, dv_ref, dvec_ref):
    rows = q_ref.shape[1]
    scale = HEAD ** (-0.5)
    dqt_ref[...] = jnp.zeros_like(dqt_ref)

    def d_body(i, carry):
        r0 = pl.multiple_of(i * TQ, TQ)
        prod = dot_ref[0, :, pl.ds(r0, TQ)].astype(jnp.float32) * o32t_ref[0, :, pl.ds(r0, TQ)]
        dvec_ref[:, pl.ds(r0, TQ)] = jnp.sum(prod, axis=0, keepdims=True)
        return carry

    lax.fori_loop(0, rows // TQ, d_body, 0)

    def kv_body(j, carry):
        c0 = pl.multiple_of(j * TK, TK)
        k = k_ref[0, pl.ds(c0, TK), :]
        v = v_ref[0, pl.ds(c0, TK), :]
        kt = kt_ref[0, :, pl.ds(c0, TK)]
        sk = segc_ref[pl.ds(c0, TK), :]

        def q_body(i, grads):
            dk, dv = grads
            r0 = pl.multiple_of(i * TQ, TQ)
            s = jnp.dot(k, qt_ref[0, :, pl.ds(r0, TQ)], preferred_element_type=jnp.float32) * scale
            same = sk == segr_ref[:, pl.ds(r0, TQ)]
            s = jnp.where(same, s, NEG)
            p = jnp.exp(s - lse_ref[0, :, pl.ds(r0, TQ)])
            dp = jnp.dot(v, dot_ref[0, :, pl.ds(r0, TQ)], preferred_element_type=jnp.float32)
            ds = (p * (dp - dvec_ref[:, pl.ds(r0, TQ)])).astype(jnp.bfloat16)
            dv = dv + jnp.dot(p.astype(jnp.bfloat16), do_ref[0, pl.ds(r0, TQ), :],
                              preferred_element_type=jnp.float32)
            dk = dk + jnp.dot(ds, q_ref[0, pl.ds(r0, TQ), :], preferred_element_type=jnp.float32)
            dqt_ref[0, :, pl.ds(r0, TQ)] += jnp.dot(kt, ds, preferred_element_type=jnp.float32)
            return dk, dv

        zeros = jnp.zeros((TK, HEAD), jnp.float32)
        dk, dv = lax.fori_loop(lo_ref[j], hi_ref[j], q_body, (zeros, zeros))
        dk_ref[0, pl.ds(c0, TK), :] = dk * scale
        dv_ref[0, pl.ds(c0, TK), :] = dv
        return carry

    lax.fori_loop(0, rows // TK, kv_body, 0)
    dqt_ref[...] = dqt_ref[...] * scale


def block_ranges(segments, item_lengths_row):
    rows = segments.shape[0]
    ends = jnp.cumsum(item_lengths_row.astype(jnp.int32))
    starts = ends - item_lengths_row.astype(jnp.int32)
    first = segments[0::TQ]
    last = segments[TQ - 1::TQ]
    n_items = item_lengths_row.shape[0]
    key_lo = jnp.take(starts, jnp.clip(first, 0, n_items - 1))
    key_hi = jnp.take(ends, jnp.clip(last, 0, n_items - 1))
    lo = jnp.clip(key_lo // TK, 0, rows // TK)
    hi = jnp.clip((key_hi + TK - 1) // TK, 0, rows // TK)
    return lo.astype(jnp.int32), hi.astype(jnp.int32)


def _head_specs(rows):
    plain = pl.BlockSpec((1, rows, HEAD), lambda h, lo, hi: (h, 0, 0))
    flipped = pl.BlockSpec((1, HEAD, rows), lambda h, lo, hi: (h, 0, 0))
    stat = pl.BlockSpec((1, 1, rows), lambda h, lo, hi: (h, 0, 0))
    col = pl.BlockSpec((rows, 1), lambda h, lo, hi: (0, 0))
    row = pl.BlockSpec((1, rows), lambda h, lo, hi: (0, 0))
    return plain, flipped, stat, col, row


def flash_forward(q, k, v, segments, lo, hi):
    heads, rows, _ = q.shape
    plain, flipped, stat, col, row = _head_specs(rows)
    flops = int(heads * rows * rows * HEAD * 2 * 2 * 0.6)
    return pl.pallas_call(
        _fwd_kernel,
        out_shape=(
            jax.ShapeDtypeStruct((heads, HEAD, rows), jnp.bfloat16),
            jax.ShapeDtypeStruct((heads, HEAD, rows), jnp.float32),
            jax.ShapeDtypeStruct((heads, 1, rows), jnp.float32),
        ),
        grid_spec=pltpu.PrefetchScalarGridSpec(
            num_scalar_prefetch=2,
            grid=(heads,),
            in_specs=[col, row, flipped, plain, flipped],
            out_specs=[flipped, flipped, stat],
        ),
        compiler_params=pltpu.CompilerParams(
            dimension_semantics=("arbitrary",), vmem_limit_bytes=48 * 1024 * 1024),
        cost_estimate=pl.CostEstimate(
            flops=flops, transcendentals=int(heads * rows * rows * 0.6),
            bytes_accessed=int(heads * rows * HEAD * (2 * 4 + 4) + heads * rows * 4)),
        name="segment_flash_fwd",
    )(lo, hi, segments.reshape(rows, 1), segments.reshape(1, rows),
      q.transpose(0, 2, 1), k, v.transpose(0, 2, 1))


def flash_backward(q, k, v, do, o32t, lse, segments, lo, hi):
    heads, rows, _ = q.shape
    plain, flipped, stat, col, row = _head_specs(rows)
    flops = int(heads * rows * rows * HEAD * 2 * 4 * 0.6)
    return pl.pallas_call(
        _bwd_kernel,
        out_shape=(
            jax.ShapeDtypeStruct((heads, HEAD, rows), jnp.float32),
            jax.ShapeDtypeStruct((heads, rows, HEAD), jnp.float32),
            jax.ShapeDtypeStruct((heads, rows, HEAD), jnp.float32),
        ),
        grid_spec=pltpu.PrefetchScalarGridSpec(
            num_scalar_prefetch=2,
            grid=(heads,),
            in_specs=[col, row, plain, flipped, plain, flipped, plain, plain, flipped, flipped, stat],
            out_specs=[flipped, plain, plain],
            scratch_shapes=[pltpu.VMEM((1, rows), jnp.float32)],
        ),
        compiler_params=pltpu.CompilerParams(
            dimension_semantics=("arbitrary",), vmem_limit_bytes=48 * 1024 * 1024),
        cost_estimate=pl.CostEstimate(
            flops=flops, transcendentals=int(heads * rows * rows * 0.6),
            bytes_accessed=int(heads * rows * HEAD * (2 * 7 + 4 * 4) + heads * rows * 4)),
        name="segment_flash_bwd",
    )(lo, hi, segments.reshape(rows, 1), segments.reshape(1, rows),
      q, q.transpose(0, 2, 1), k, k.transpose(0, 2, 1), v, do, do.transpose(0, 2, 1), o32t, lse)

def normalize(values, gain, shift):
    center = jnp.mean(values, axis=-1, keepdims=True)
    centered = values - center
    spread = jnp.mean(centered * centered, axis=-1, keepdims=True)
    return centered * lax.rsqrt(spread + 1e-06) * gain + shift


def exact_gelu(values):
    return jax.nn.gelu(values, approximate=False)


def segment_ids(lengths_row, row_count):
    ends = jnp.cumsum(lengths_row)
    positions = jnp.arange(row_count, dtype=jnp.int32)
    return jnp.sum((positions[:, None] >= ends[None, :]).astype(jnp.int32), axis=1)


def mp_allreduce(partial, n_mp):
    if n_mp != 4:
        return lax.psum(partial, "mp").astype(jnp.float32)
    idx = lax.axis_index("mp")
    low_bit = idx % 2
    half = partial.shape[0] // 2
    mine = lax.dynamic_slice_in_dim(partial, low_bit * half, half, 0)
    other = lax.dynamic_slice_in_dim(partial, (1 - low_bit) * half, half, 0)
    got = lax.ppermute(other, "mp", [(k, k ^ 1) for k in range(4)])
    first = (mine.astype(jnp.float32) + got.astype(jnp.float32)).astype(jnp.bfloat16)
    got_far = lax.ppermute(first, "mp", [(k, k ^ 2) for k in range(4)])
    second = (first.astype(jnp.float32) + got_far.astype(jnp.float32)).astype(jnp.bfloat16)
    got_back = lax.ppermute(second, "mp", [(k, k ^ 1) for k in range(4)])
    top = jnp.where(low_bit == 0, second, got_back)
    bottom = jnp.where(low_bit == 0, got_back, second)
    return jnp.concatenate([top, bottom], axis=0).astype(jnp.float32)


def dp_allreduce(values, n_dp):
    if n_dp & (n_dp - 1):
        return lax.psum(values, "dp")
    total = values
    step = 1
    while step < n_dp:
        total = total + lax.ppermute(total, "dp", [(k, k ^ step) for k in range(n_dp)])
        step *= 2
    return total


def per_device(n_mp, n_dp,

    tokens,
    cotangent,
    item_lengths,
    w_qkv,
    b_qv,
    w_out,
    b_out,
    w_fc1,
    b_fc1,
    w_fc2,
    b_fc2,
    ln1_gain,
    ln1_bias,
    ln2_gain,
    ln2_bias,
):
    row_count = tokens.shape[0]
    local_cols = w_qkv.shape[2]
    heads_here = local_cols // HEAD
    segments = segment_ids(item_lengths[0], row_count)
    inputs = tokens.astype(jnp.float32)
    norm_one, norm_one_back = jax.vjp(normalize, inputs, ln1_gain, ln1_bias)
    normed_one = norm_one.astype(jnp.bfloat16)
    queries = (jnp.dot(normed_one, w_qkv[0], preferred_element_type=jnp.float32) + b_qv[0]).astype(
        jnp.bfloat16
    )
    key_rows = jnp.dot(normed_one, w_qkv[1], preferred_element_type=jnp.float32).astype(
        jnp.bfloat16
    )
    value_rows = (
        jnp.dot(normed_one, w_qkv[2], preferred_element_type=jnp.float32) + b_qv[1]
    ).astype(jnp.bfloat16)
    def to_heads(values):
        return values.reshape(row_count, heads_here, HEAD).transpose(1, 0, 2)

    def from_heads(values):
        return values.transpose(1, 0, 2).reshape(row_count, local_cols)

    lo_blocks, hi_blocks = block_ranges(segments, item_lengths[0])
    query_heads = to_heads(queries)
    key_heads = to_heads(key_rows)
    value_heads = to_heads(value_rows)
    out_heads, out_f32, log_norms = flash_forward(
        query_heads, key_heads, value_heads, segments, lo_blocks, hi_blocks
    )
    attended = out_heads.transpose(2, 0, 1).reshape(row_count, local_cols)
    attention_sum = mp_allreduce(
        jnp.dot(attended, w_out, preferred_element_type=jnp.float32).astype(jnp.bfloat16), n_mp
    )
    middle = inputs + attention_sum + b_out
    norm_two, norm_two_back = jax.vjp(normalize, middle, ln2_gain, ln2_bias)
    normed_two = norm_two.astype(jnp.bfloat16)
    hidden_pre = jnp.dot(normed_two, w_fc1, preferred_element_type=jnp.float32) + b_fc1
    activated_full, gelu_back = jax.vjp(exact_gelu, hidden_pre)
    activated = activated_full.astype(jnp.bfloat16)
    mlp_partial = jnp.dot(activated, w_fc2, preferred_element_type=jnp.float32).astype(jnp.bfloat16)
    upstream = cotangent.astype(jnp.float32)
    grad_b_fc2 = jnp.sum(upstream, axis=0)
    grad_w_fc2 = jnp.einsum("tf,td->fd", activated, cotangent, preferred_element_type=jnp.float32)
    d_act = jnp.einsum("td,fd->tf", cotangent, w_fc2, preferred_element_type=jnp.float32)
    d_pre = gelu_back(d_act)[0]
    grad_b_fc1 = jnp.sum(d_pre, axis=0)
    d_pre_low = d_pre.astype(jnp.bfloat16)
    grad_w_fc1 = jnp.einsum("td,tf->df", normed_two, d_pre_low, preferred_element_type=jnp.float32)
    d_normed_two = mp_allreduce(
        jnp.einsum("tf,df->td", d_pre_low, w_fc1, preferred_element_type=jnp.float32).astype(
            jnp.bfloat16
        ),
        n_mp,
    )
    d_middle_norm, grad_ln2_gain, grad_ln2_bias = norm_two_back(d_normed_two)
    d_middle = upstream + d_middle_norm
    mlp_partial, d_middle = lax.optimization_barrier((mlp_partial, d_middle))
    mlp_sum = mp_allreduce(mlp_partial, n_mp)
    output = (middle + mlp_sum + b_fc2).astype(jnp.bfloat16)
    grad_b_out = jnp.sum(d_middle, axis=0)
    d_middle_low = d_middle.astype(jnp.bfloat16)
    grad_w_out = jnp.einsum("tc,td->cd", attended, d_middle_low, preferred_element_type=jnp.float32)
    d_attended = jnp.einsum(
        "td,cd->tc", d_middle_low, w_out, preferred_element_type=jnp.float32
    ).astype(jnp.bfloat16)
    d_q_heads, d_k_heads, d_v_heads = flash_backward(
        query_heads, key_heads, value_heads, to_heads(d_attended), out_f32, log_norms,
        segments, lo_blocks, hi_blocks,
    )
    d_queries = d_q_heads.transpose(2, 0, 1).reshape(row_count, local_cols)
    d_keys = from_heads(d_k_heads)
    d_values = from_heads(d_v_heads)
    grad_b_qv = jnp.stack([jnp.sum(d_queries, axis=0), jnp.sum(d_values, axis=0)])
    stacked = jnp.stack([d_queries, d_keys, d_values]).astype(jnp.bfloat16)
    grad_w_qkv = jnp.einsum("td,stc->sdc", normed_one, stacked, preferred_element_type=jnp.float32)
    d_normed_one = mp_allreduce(
        jnp.einsum("stc,sdc->td", stacked, w_qkv, preferred_element_type=jnp.float32).astype(
            jnp.bfloat16
        ),
        n_mp,
    )
    d_input_norm, grad_ln1_gain, grad_ln1_bias = norm_one_back(d_normed_one)
    grad_tokens = d_middle + d_input_norm
    def scatter(grad, dim):
        return lax.psum_scatter(
            grad.astype(jnp.bfloat16), "dp", scatter_dimension=dim, tiled=True
        ).astype(jnp.float32)

    summed_qkv = scatter(grad_w_qkv, 1)
    summed_out = scatter(grad_w_out, 1)
    summed_fc1 = scatter(grad_w_fc1, 0)
    summed_fc2 = scatter(grad_w_fc2, 1)
    early = dp_allreduce(
        jnp.concatenate([grad_ln2_gain, grad_ln2_bias, grad_b_out, grad_b_fc2, grad_b_fc1]), n_dp
    )
    late = dp_allreduce(jnp.concatenate([grad_ln1_gain, grad_ln1_bias, grad_b_qv.reshape(-1)]), n_dp)
    width = grad_ln1_gain.shape[0]
    pieces = [late[0:width], late[width : 2 * width]] + [
        early[k * width : (k + 1) * width] for k in range(4)
    ]
    summed_b_qv = late[2 * width :].reshape(grad_b_qv.shape)
    summed_b_fc1 = early[4 * width :]
    return (
        output,
        grad_tokens,
        summed_qkv,
        summed_b_qv,
        summed_out,
        pieces[4],
        summed_fc1,
        summed_b_fc1,
        summed_fc2,
        pieces[5],
        pieces[0],
        pieces[1],
        pieces[2],
        pieces[3],
    )


def solution(mesh):
    in_specs = (
        P("dp", None),
        P("dp", None),
        P("dp", None),
        P(None, None, "mp"),
        P(None, "mp"),
        P("mp", None),
        P(),
        P(None, "mp"),
        P("mp"),
        P("mp", None),
        P(),
        P(),
        P(),
        P(),
        P(),
    )
    out_specs = (
        P("dp", None),
        P("dp", None),
        P(None, "dp", "mp"),
        P(None, "mp"),
        P("mp", "dp"),
        P(),
        P("dp", "mp"),
        P("mp"),
        P("mp", "dp"),
        P(),
        P(),
        P(),
        P(),
        P(),
    )
    return jax.shard_map(
        partial(per_device, mesh.shape["mp"], mesh.shape["dp"]), mesh=mesh, in_specs=in_specs, out_specs=out_specs, check_vma=False
    )
```

```python
import jax
import jax.numpy as jnp
from jax import lax
from jax.experimental import pallas as pl
from jax.experimental.pallas import tpu as pltpu
from jax.sharding import PartitionSpec as P


HEAD = 64
TQ = 256
TK = 256
NEG = -1e30


def _fwd_kernel(lo_ref, hi_ref, segc_ref, segr_ref, qt_ref, k_ref, vt_ref, ot_ref, o32t_ref, lse_ref):
    rows = qt_ref.shape[2]
    scale = HEAD ** (-0.5)

    def q_body(i, carry):
        r0 = pl.multiple_of(i * TQ, TQ)
        qt = qt_ref[0, :, pl.ds(r0, TQ)]
        sq = segr_ref[:, pl.ds(r0, TQ)]

        def kv_body(j, state):
            m, l, acc = state
            c0 = pl.multiple_of(j * TK, TK)
            s = jnp.dot(k_ref[0, pl.ds(c0, TK), :], qt, preferred_element_type=jnp.float32) * scale
            same = segc_ref[pl.ds(c0, TK), :] == sq
            s = jnp.where(same, s, NEG)
            m_new = jnp.maximum(m, jnp.max(s, axis=0, keepdims=True))
            p = jnp.exp(s - m_new)
            alpha = jnp.exp(m - m_new)
            l = alpha * l + jnp.sum(p, axis=0, keepdims=True)
            pv = jnp.dot(vt_ref[0, :, pl.ds(c0, TK)], p.astype(jnp.bfloat16),
                         preferred_element_type=jnp.float32)
            return m_new, l, alpha * acc + pv

        m0 = jnp.full((1, TQ), NEG, jnp.float32)
        l0 = jnp.zeros((1, TQ), jnp.float32)
        acc0 = jnp.zeros((HEAD, TQ), jnp.float32)
        m, l, acc = lax.fori_loop(lo_ref[i], hi_ref[i], kv_body, (m0, l0, acc0))
        out = acc / l
        ot_ref[0, :, pl.ds(r0, TQ)] = out.astype(ot_ref.dtype)
        o32t_ref[0, :, pl.ds(r0, TQ)] = out
        lse_ref[0, :, pl.ds(r0, TQ)] = m + jnp.log(l)
        return carry

    lax.fori_loop(0, rows // TQ, q_body, 0)


def _bwd_kernel(lo_ref, hi_ref, segc_ref, segr_ref, q_ref, qt_ref, k_ref, kt_ref, v_ref, do_ref, dot_ref,
                o32t_ref, lse_ref, dqt_ref, dk_ref, dv_ref, dvec_ref):
    rows = q_ref.shape[1]
    scale = HEAD ** (-0.5)
    dqt_ref[...] = jnp.zeros_like(dqt_ref)

    def d_body(i, carry):
        r0 = pl.multiple_of(i * TQ, TQ)
        prod = dot_ref[0, :, pl.ds(r0, TQ)].astype(jnp.float32) * o32t_ref[0, :, pl.ds(r0, TQ)]
        dvec_ref[:, pl.ds(r0, TQ)] = jnp.sum(prod, axis=0, keepdims=True)
        return carry

    lax.fori_loop(0, rows // TQ, d_body, 0)

    def kv_body(j, carry):
        c0 = pl.multiple_of(j * TK, TK)
        k = k_ref[0, pl.ds(c0, TK), :]
        v = v_ref[0, pl.ds(c0, TK), :]
        kt = kt_ref[0, :, pl.ds(c0, TK)]
        sk = segc_ref[pl.ds(c0, TK), :]

        def q_body(i, grads):
            dk, dv = grads
            r0 = pl.multiple_of(i * TQ, TQ)
            s = jnp.dot(k, qt_ref[0, :, pl.ds(r0, TQ)], preferred_element_type=jnp.float32) * scale
            same = sk == segr_ref[:, pl.ds(r0, TQ)]
            s = jnp.where(same, s, NEG)
            p = jnp.exp(s - lse_ref[0, :, pl.ds(r0, TQ)])
            dp = jnp.dot(v, dot_ref[0, :, pl.ds(r0, TQ)], preferred_element_type=jnp.float32)
            ds = (p * (dp - dvec_ref[:, pl.ds(r0, TQ)])).astype(jnp.bfloat16)
            dv = dv + jnp.dot(p.astype(jnp.bfloat16), do_ref[0, pl.ds(r0, TQ), :],
                              preferred_element_type=jnp.float32)
            dk = dk + jnp.dot(ds, q_ref[0, pl.ds(r0, TQ), :], preferred_element_type=jnp.float32)
            dqt_ref[0, :, pl.ds(r0, TQ)] += jnp.dot(kt, ds, preferred_element_type=jnp.float32)
            return dk, dv

        zeros = jnp.zeros((TK, HEAD), jnp.float32)
        dk, dv = lax.fori_loop(lo_ref[j], hi_ref[j], q_body, (zeros, zeros))
        dk_ref[0, pl.ds(c0, TK), :] = dk * scale
        dv_ref[0, pl.ds(c0, TK), :] = dv
        return carry

    lax.fori_loop(0, rows // TK, kv_body, 0)
    dqt_ref[...] = dqt_ref[...] * scale


def block_ranges(segments, item_lengths_row):
    rows = segments.shape[0]
    ends = jnp.cumsum(item_lengths_row.astype(jnp.int32))
    starts = ends - item_lengths_row.astype(jnp.int32)
    first = segments[0::TQ]
    last = segments[TQ - 1::TQ]
    n_items = item_lengths_row.shape[0]
    key_lo = jnp.take(starts, jnp.clip(first, 0, n_items - 1))
    key_hi = jnp.take(ends, jnp.clip(last, 0, n_items - 1))
    lo = jnp.clip(key_lo // TK, 0, rows // TK)
    hi = jnp.clip((key_hi + TK - 1) // TK, 0, rows // TK)
    return lo.astype(jnp.int32), hi.astype(jnp.int32)


def _head_specs(rows):
    plain = pl.BlockSpec((1, rows, HEAD), lambda h, lo, hi: (h, 0, 0))
    flipped = pl.BlockSpec((1, HEAD, rows), lambda h, lo, hi: (h, 0, 0))
    stat = pl.BlockSpec((1, 1, rows), lambda h, lo, hi: (h, 0, 0))
    col = pl.BlockSpec((rows, 1), lambda h, lo, hi: (0, 0))
    row = pl.BlockSpec((1, rows), lambda h, lo, hi: (0, 0))
    return plain, flipped, stat, col, row


def flash_forward(q, k, v, segments, lo, hi):
    heads, rows, _ = q.shape
    plain, flipped, stat, col, row = _head_specs(rows)
    flops = int(heads * rows * rows * HEAD * 2 * 2 * 0.6)
    return pl.pallas_call(
        _fwd_kernel,
        out_shape=(
            jax.ShapeDtypeStruct((heads, HEAD, rows), jnp.bfloat16),
            jax.ShapeDtypeStruct((heads, HEAD, rows), jnp.float32),
            jax.ShapeDtypeStruct((heads, 1, rows), jnp.float32),
        ),
        grid_spec=pltpu.PrefetchScalarGridSpec(
            num_scalar_prefetch=2,
            grid=(heads,),
            in_specs=[col, row, flipped, plain, flipped],
            out_specs=[flipped, flipped, stat],
        ),
        compiler_params=pltpu.CompilerParams(
            dimension_semantics=("arbitrary",), vmem_limit_bytes=48 * 1024 * 1024),
        cost_estimate=pl.CostEstimate(
            flops=flops, transcendentals=int(heads * rows * rows * 0.6),
            bytes_accessed=int(heads * rows * HEAD * (2 * 4 + 4) + heads * rows * 4)),
        name="segment_flash_fwd",
    )(lo, hi, segments.reshape(rows, 1), segments.reshape(1, rows),
      q.transpose(0, 2, 1), k, v.transpose(0, 2, 1))


def flash_backward(q, k, v, do, o32t, lse, segments, lo, hi):
    heads, rows, _ = q.shape
    plain, flipped, stat, col, row = _head_specs(rows)
    flops = int(heads * rows * rows * HEAD * 2 * 4 * 0.6)
    return pl.pallas_call(
        _bwd_kernel,
        out_shape=(
            jax.ShapeDtypeStruct((heads, HEAD, rows), jnp.float32),
            jax.ShapeDtypeStruct((heads, rows, HEAD), jnp.float32),
            jax.ShapeDtypeStruct((heads, rows, HEAD), jnp.float32),
        ),
        grid_spec=pltpu.PrefetchScalarGridSpec(
            num_scalar_prefetch=2,
            grid=(heads,),
            in_specs=[col, row, plain, flipped, plain, flipped, plain, plain, flipped, flipped, stat],
            out_specs=[flipped, plain, plain],
            scratch_shapes=[pltpu.VMEM((1, rows), jnp.float32)],
        ),
        compiler_params=pltpu.CompilerParams(
            dimension_semantics=("arbitrary",), vmem_limit_bytes=48 * 1024 * 1024),
        cost_estimate=pl.CostEstimate(
            flops=flops, transcendentals=int(heads * rows * rows * 0.6),
            bytes_accessed=int(heads * rows * HEAD * (2 * 7 + 4 * 4) + heads * rows * 4)),
        name="segment_flash_bwd",
    )(lo, hi, segments.reshape(rows, 1), segments.reshape(1, rows),
      q, q.transpose(0, 2, 1), k, k.transpose(0, 2, 1), v, do, do.transpose(0, 2, 1), o32t, lse)


def normalize(values, gain, shift):
    center = jnp.mean(values, axis=-1, keepdims=True)
    centered = values - center
    spread = jnp.mean(centered * centered, axis=-1, keepdims=True)
    return centered * lax.rsqrt(spread + 1e-06) * gain + shift


def exact_gelu(values):
    return jax.nn.gelu(values, approximate=False)


def segment_ids(lengths_row, row_count):
    ends = jnp.cumsum(lengths_row)
    positions = jnp.arange(row_count, dtype=jnp.int32)
    return jnp.sum((positions[:, None] >= ends[None, :]).astype(jnp.int32), axis=1)


def mp_allreduce(partial, n_mp):
    if n_mp != 4:
        return lax.psum(partial, "mp").astype(jnp.float32)
    idx = lax.axis_index("mp")
    low_bit = idx % 2
    half = partial.shape[0] // 2
    mine = lax.dynamic_slice_in_dim(partial, low_bit * half, half, 0)
    other = lax.dynamic_slice_in_dim(partial, (1 - low_bit) * half, half, 0)
    got = lax.ppermute(other, "mp", [(k, k ^ 1) for k in range(4)])
    first = (mine.astype(jnp.float32) + got.astype(jnp.float32)).astype(jnp.bfloat16)
    got_far = lax.ppermute(first, "mp", [(k, k ^ 2) for k in range(4)])
    second = (first.astype(jnp.float32) + got_far.astype(jnp.float32)).astype(jnp.bfloat16)
    got_back = lax.ppermute(second, "mp", [(k, k ^ 1) for k in range(4)])
    top = jnp.where(low_bit == 0, second, got_back)
    bottom = jnp.where(low_bit == 0, got_back, second)
    return jnp.concatenate([top, bottom], axis=0).astype(jnp.float32)


def dp_allreduce(values, n_dp):
    if n_dp & (n_dp - 1):
        return lax.psum(values, "dp")
    total = values
    step = 1
    while step < n_dp:
        total = total + lax.ppermute(total, "dp", [(k, k ^ step) for k in range(n_dp)])
        step *= 2
    return total


def per_device(n_mp, n_dp,
    tokens,
    cotangent,
    item_lengths,
    w_qkv,
    b_qv,
    w_out,
    b_out,
    w_fc1,
    b_fc1,
    w_fc2,
    b_fc2,
    ln1_gain,
    ln1_bias,
    ln2_gain,
    ln2_bias,
):
    row_count = tokens.shape[0]
    local_cols = w_qkv.shape[2]
    heads_here = local_cols // HEAD
    segments = segment_ids(item_lengths[0], row_count)
    inputs = tokens.astype(jnp.float32)
    norm_one, norm_one_back = jax.vjp(normalize, inputs, ln1_gain, ln1_bias)
    normed_one = norm_one.astype(jnp.bfloat16)
    queries = (jnp.dot(normed_one, w_qkv[0], preferred_element_type=jnp.float32) + b_qv[0]).astype(
        jnp.bfloat16
    )
    key_rows = jnp.dot(normed_one, w_qkv[1], preferred_element_type=jnp.float32).astype(
        jnp.bfloat16
    )
    value_rows = (
        jnp.dot(normed_one, w_qkv[2], preferred_element_type=jnp.float32) + b_qv[1]
    ).astype(jnp.bfloat16)

    def to_heads(values):
        return values.reshape(row_count, heads_here, HEAD).transpose(1, 0, 2)

    def from_heads(values):
        return values.transpose(1, 0, 2).reshape(row_count, local_cols)

    lo_blocks, hi_blocks = block_ranges(segments, item_lengths[0])
    query_heads = to_heads(queries)
    key_heads = to_heads(key_rows)
    value_heads = to_heads(value_rows)
    out_heads, out_f32, log_norms = flash_forward(
        query_heads, key_heads, value_heads, segments, lo_blocks, hi_blocks
    )
    attended = out_heads.transpose(2, 0, 1).reshape(row_count, local_cols)
    attention_sum = mp_allreduce(
        jnp.dot(attended, w_out, preferred_element_type=jnp.float32).astype(jnp.bfloat16), n_mp,
    )
    middle = inputs + attention_sum + b_out
    norm_two, norm_two_back = jax.vjp(normalize, middle, ln2_gain, ln2_bias)
    normed_two = norm_two.astype(jnp.bfloat16)
    hidden_pre = jnp.dot(normed_two, w_fc1, preferred_element_type=jnp.float32) + b_fc1
    activated_full, gelu_back = jax.vjp(exact_gelu, hidden_pre)
    activated = activated_full.astype(jnp.bfloat16)
    mlp_partial = jnp.dot(activated, w_fc2, preferred_element_type=jnp.float32).astype(jnp.bfloat16)
    upstream = cotangent.astype(jnp.float32)
    grad_b_fc2 = jnp.sum(upstream, axis=0)
    grad_w_fc2 = jnp.einsum("tf,td->fd", activated, cotangent, preferred_element_type=jnp.float32)
    d_act = jnp.einsum("td,fd->tf", cotangent, w_fc2, preferred_element_type=jnp.float32)
    d_pre = gelu_back(d_act)[0]
    grad_b_fc1 = jnp.sum(d_pre, axis=0)
    d_pre_low = d_pre.astype(jnp.bfloat16)
    grad_w_fc1 = jnp.einsum("td,tf->df", normed_two, d_pre_low, preferred_element_type=jnp.float32)
    d_normed_two = mp_allreduce(
        jnp.einsum("tf,df->td", d_pre_low, w_fc1, preferred_element_type=jnp.float32).astype(
            jnp.bfloat16
        ),
        n_mp,
    )
    d_middle_norm, grad_ln2_gain, grad_ln2_bias = norm_two_back(d_normed_two)
    d_middle = upstream + d_middle_norm
    mlp_partial, d_middle = lax.optimization_barrier((mlp_partial, d_middle))
    mlp_sum = mp_allreduce(mlp_partial, n_mp)
    output = (middle + mlp_sum + b_fc2).astype(jnp.bfloat16)
    grad_b_out = jnp.sum(d_middle, axis=0)
    d_middle_low = d_middle.astype(jnp.bfloat16)
    grad_w_out = jnp.einsum("tc,td->cd", attended, d_middle_low, preferred_element_type=jnp.float32)
    d_attended = jnp.einsum(
        "td,cd->tc", d_middle_low, w_out, preferred_element_type=jnp.float32
    ).astype(jnp.bfloat16)
    d_att_heads = to_heads(d_attended)
    d_q_heads, d_k_heads, d_v_heads = flash_backward(
        query_heads, key_heads, value_heads, d_att_heads, out_f32, log_norms,
        segments, lo_blocks, hi_blocks,
    )
    d_queries = d_q_heads.transpose(2, 0, 1).reshape(row_count, local_cols)
    d_keys = from_heads(d_k_heads)
    d_values = from_heads(d_v_heads)
    grad_b_qv = jnp.stack([jnp.sum(d_queries, axis=0), jnp.sum(d_values, axis=0)])
    stacked = jnp.stack([d_queries, d_keys, d_values]).astype(jnp.bfloat16)
    grad_w_qkv = jnp.einsum("td,stc->sdc", normed_one, stacked, preferred_element_type=jnp.float32)
    d_normed_one = mp_allreduce(
        jnp.einsum("stc,sdc->td", stacked, w_qkv, preferred_element_type=jnp.float32).astype(
            jnp.bfloat16
        ),
        n_mp,
    )
    d_input_norm, grad_ln1_gain, grad_ln1_bias = norm_one_back(d_normed_one)
    grad_tokens = d_middle + d_input_norm

    def scatter(grad, dim):
        return lax.psum_scatter(
            grad.astype(jnp.bfloat16), "dp", scatter_dimension=dim, tiled=True
        ).astype(jnp.float32)

    summed_qkv = scatter(grad_w_qkv, 1)
    summed_out = scatter(grad_w_out, 1)
    summed_fc1 = scatter(grad_w_fc1, 0)
    summed_fc2 = scatter(grad_w_fc2, 1)
    early = dp_allreduce(
        jnp.concatenate([grad_ln2_gain, grad_ln2_bias, grad_b_out, grad_b_fc2, grad_b_fc1]), n_dp
    )
    late = dp_allreduce(jnp.concatenate([grad_ln1_gain, grad_ln1_bias, grad_b_qv.reshape(-1)]), n_dp)
    width = grad_ln1_gain.shape[0]
    pieces = [late[0:width], late[width : 2 * width]] + [
        early[k * width : (k + 1) * width] for k in range(4)
    ]
    summed_b_qv = late[2 * width :].reshape(grad_b_qv.shape)
    summed_b_fc1 = early[4 * width :]
    return (
        output,
        grad_tokens,
        summed_qkv,
        summed_b_qv,
        summed_out,
        pieces[4],
        summed_fc1,
        summed_b_fc1,
        summed_fc2,
        pieces[5],
        pieces[0],
        pieces[1],
        pieces[2],
        pieces[3],
    )


def solution(mesh):
    in_specs = (
        P("dp", None),
        P("dp", None),
        P("dp", None),
        P(None, None, "mp"),
        P(None, "mp"),
        P("mp", None),
        P(),
        P(None, "mp"),
        P("mp"),
        P("mp", None),
        P(),
        P(),
        P(),
        P(),
        P(),
    )
    out_specs = (
        P("dp", None),
        P("dp", None),
        P(None, "dp", "mp"),
        P(None, "mp"),
        P("mp", "dp"),
        P(),
        P("dp", "mp"),
        P("mp"),
        P("mp", "dp"),
        P(),
        P(),
        P(),
        P(),
        P(),
    )

    def body(*args):
        return per_device(mesh.shape["mp"], mesh.shape["dp"], *args)

    return jax.shard_map(
        body, mesh=mesh, in_specs=in_specs, out_specs=out_specs, check_vma=False
    )
```

```python
import jax
import jax.numpy as jnp
from jax import lax
from jax.experimental import pallas as pl
from jax.experimental.pallas import tpu as pltpu
from jax.sharding import PartitionSpec as P


HEAD = 64
TQ = 256
TK = 256
NEG = -1e30


def _fwd_kernel(lo_ref, hi_ref, segc_ref, segr_ref, qt_ref, k_ref, vt_ref, ot_ref, o32t_ref, lse_ref):
    rows = qt_ref.shape[2]
    scale = HEAD ** (-0.5)

    def q_body(i, carry):
        r0 = pl.multiple_of(i * TQ, TQ)
        qt = qt_ref[0, :, pl.ds(r0, TQ)]
        sq = segr_ref[:, pl.ds(r0, TQ)]

        def kv_body(j, state):
            m, l, acc = state
            c0 = pl.multiple_of(j * TK, TK)
            s = jnp.dot(k_ref[0, pl.ds(c0, TK), :], qt, preferred_element_type=jnp.float32) * scale
            same = segc_ref[pl.ds(c0, TK), :] == sq
            s = jnp.where(same, s, NEG)
            m_new = jnp.maximum(m, jnp.max(s, axis=0, keepdims=True))
            p = jnp.exp(s - m_new)
            alpha = jnp.exp(m - m_new)
            l = alpha * l + jnp.sum(p, axis=0, keepdims=True)
            pv = jnp.dot(vt_ref[0, :, pl.ds(c0, TK)], p.astype(jnp.bfloat16),
                         preferred_element_type=jnp.float32)
            return m_new, l, alpha * acc + pv

        m0 = jnp.full((1, TQ), NEG, jnp.float32)
        l0 = jnp.zeros((1, TQ), jnp.float32)
        acc0 = jnp.zeros((HEAD, TQ), jnp.float32)
        m, l, acc = lax.fori_loop(lo_ref[i], hi_ref[i], kv_body, (m0, l0, acc0))
        out = acc / l
        ot_ref[0, :, pl.ds(r0, TQ)] = out.astype(ot_ref.dtype)
        o32t_ref[0, :, pl.ds(r0, TQ)] = out
        lse_ref[0, :, pl.ds(r0, TQ)] = m + jnp.log(l)
        return carry

    lax.fori_loop(0, rows // TQ, q_body, 0)


def _bwd_kernel(lo_ref, hi_ref, segc_ref, segr_ref, q_ref, qt_ref, k_ref, kt_ref, v_ref, do_ref, dot_ref,
                o32t_ref, lse_ref, dqt_ref, dk_ref, dv_ref, dvec_ref):
    rows = q_ref.shape[1]
    scale = HEAD ** (-0.5)
    dqt_ref[...] = jnp.zeros_like(dqt_ref)

    def d_body(i, carry):
        r0 = pl.multiple_of(i * TQ, TQ)
        prod = dot_ref[0, :, pl.ds(r0, TQ)].astype(jnp.float32) * o32t_ref[0, :, pl.ds(r0, TQ)]
        dvec_ref[:, pl.ds(r0, TQ)] = jnp.sum(prod, axis=0, keepdims=True)
        return carry

    lax.fori_loop(0, rows // TQ, d_body, 0)

    def kv_body(j, carry):
        c0 = pl.multiple_of(j * TK, TK)
        k = k_ref[0, pl.ds(c0, TK), :]
        v = v_ref[0, pl.ds(c0, TK), :]
        kt = kt_ref[0, :, pl.ds(c0, TK)]
        sk = segc_ref[pl.ds(c0, TK), :]

        def q_body(i, grads):
            dk, dv = grads
            r0 = pl.multiple_of(i * TQ, TQ)
            s = jnp.dot(k, qt_ref[0, :, pl.ds(r0, TQ)], preferred_element_type=jnp.float32) * scale
            same = sk == segr_ref[:, pl.ds(r0, TQ)]
            s = jnp.where(same, s, NEG)
            p = jnp.exp(s - lse_ref[0, :, pl.ds(r0, TQ)])
            dp = jnp.dot(v, dot_ref[0, :, pl.ds(r0, TQ)], preferred_element_type=jnp.float32)
            ds = (p * (dp - dvec_ref[:, pl.ds(r0, TQ)])).astype(jnp.bfloat16)
            dv = dv + jnp.dot(p.astype(jnp.bfloat16), do_ref[0, pl.ds(r0, TQ), :],
                              preferred_element_type=jnp.float32)
            dk = dk + jnp.dot(ds, q_ref[0, pl.ds(r0, TQ), :], preferred_element_type=jnp.float32)
            dqt_ref[0, :, pl.ds(r0, TQ)] += jnp.dot(kt, ds, preferred_element_type=jnp.float32)
            return dk, dv

        zeros = jnp.zeros((TK, HEAD), jnp.float32)
        dk, dv = lax.fori_loop(lo_ref[j], hi_ref[j], q_body, (zeros, zeros))
        dk_ref[0, pl.ds(c0, TK), :] = dk * scale
        dv_ref[0, pl.ds(c0, TK), :] = dv
        return carry

    lax.fori_loop(0, rows // TK, kv_body, 0)
    dqt_ref[...] = dqt_ref[...] * scale


def block_ranges(segments, item_lengths_row):
    rows = segments.shape[0]
    ends = jnp.cumsum(item_lengths_row.astype(jnp.int32))
    starts = ends - item_lengths_row.astype(jnp.int32)
    first = segments[0::TQ]
    last = segments[TQ - 1::TQ]
    n_items = item_lengths_row.shape[0]
    key_lo = jnp.take(starts, jnp.clip(first, 0, n_items - 1))
    key_hi = jnp.take(ends, jnp.clip(last, 0, n_items - 1))
    lo = jnp.clip(key_lo // TK, 0, rows // TK)
    hi = jnp.clip((key_hi + TK - 1) // TK, 0, rows // TK)
    return lo.astype(jnp.int32), hi.astype(jnp.int32)


def _head_specs(rows):
    plain = pl.BlockSpec((1, rows, HEAD), lambda h, lo, hi: (h, 0, 0))
    flipped = pl.BlockSpec((1, HEAD, rows), lambda h, lo, hi: (h, 0, 0))
    stat = pl.BlockSpec((1, 1, rows), lambda h, lo, hi: (h, 0, 0))
    col = pl.BlockSpec((rows, 1), lambda h, lo, hi: (0, 0))
    row = pl.BlockSpec((1, rows), lambda h, lo, hi: (0, 0))
    return plain, flipped, stat, col, row


def flash_forward(q, k, v, segments, lo, hi):
    heads, rows, _ = q.shape
    plain, flipped, stat, col, row = _head_specs(rows)
    flops = int(heads * rows * rows * HEAD * 2 * 2 * 0.6)
    return pl.pallas_call(
        _fwd_kernel,
        out_shape=(
            jax.ShapeDtypeStruct((heads, HEAD, rows), jnp.bfloat16),
            jax.ShapeDtypeStruct((heads, HEAD, rows), jnp.float32),
            jax.ShapeDtypeStruct((heads, 1, rows), jnp.float32),
        ),
        grid_spec=pltpu.PrefetchScalarGridSpec(
            num_scalar_prefetch=2,
            grid=(heads,),
            in_specs=[col, row, flipped, plain, flipped],
            out_specs=[flipped, flipped, stat],
        ),
        compiler_params=pltpu.CompilerParams(
            dimension_semantics=("arbitrary",), vmem_limit_bytes=48 * 1024 * 1024),
        cost_estimate=pl.CostEstimate(
            flops=flops, transcendentals=int(heads * rows * rows * 0.6),
            bytes_accessed=int(heads * rows * HEAD * (2 * 4 + 4) + heads * rows * 4)),
        name="segment_flash_fwd",
    )(lo, hi, segments.reshape(rows, 1), segments.reshape(1, rows),
      q.transpose(0, 2, 1), k, v.transpose(0, 2, 1))


def flash_backward(q, k, v, do, o32t, lse, segments, lo, hi):
    heads, rows, _ = q.shape
    plain, flipped, stat, col, row = _head_specs(rows)
    flops = int(heads * rows * rows * HEAD * 2 * 4 * 0.6)
    return pl.pallas_call(
        _bwd_kernel,
        out_shape=(
            jax.ShapeDtypeStruct((heads, HEAD, rows), jnp.float32),
            jax.ShapeDtypeStruct((heads, rows, HEAD), jnp.float32),
            jax.ShapeDtypeStruct((heads, rows, HEAD), jnp.float32),
        ),
        grid_spec=pltpu.PrefetchScalarGridSpec(
            num_scalar_prefetch=2,
            grid=(heads,),
            in_specs=[col, row, plain, flipped, plain, flipped, plain, plain, flipped, flipped, stat],
            out_specs=[flipped, plain, plain],
            scratch_shapes=[pltpu.VMEM((1, rows), jnp.float32)],
        ),
        compiler_params=pltpu.CompilerParams(
            dimension_semantics=("arbitrary",), vmem_limit_bytes=48 * 1024 * 1024),
        cost_estimate=pl.CostEstimate(
            flops=flops, transcendentals=int(heads * rows * rows * 0.6),
            bytes_accessed=int(heads * rows * HEAD * (2 * 7 + 4 * 4) + heads * rows * 4)),
        name="segment_flash_bwd",
    )(lo, hi, segments.reshape(rows, 1), segments.reshape(1, rows),
      q, q.transpose(0, 2, 1), k, k.transpose(0, 2, 1), v, do, do.transpose(0, 2, 1), o32t, lse)


def normalize(values, gain, shift):
    center = jnp.mean(values, axis=-1, keepdims=True)
    centered = values - center
    spread = jnp.mean(centered * centered, axis=-1, keepdims=True)
    return centered * lax.rsqrt(spread + 1e-06) * gain + shift


def exact_gelu(values):
    return jax.nn.gelu(values, approximate=False)


def segment_ids(lengths_row, row_count):
    ends = jnp.cumsum(lengths_row)
    positions = jnp.arange(row_count, dtype=jnp.int32)
    return jnp.sum((positions[:, None] >= ends[None, :]).astype(jnp.int32), axis=1)


def mp_allreduce(partial, n_mp):
    if n_mp != 4:
        return lax.psum(partial, "mp").astype(jnp.float32)
    idx = lax.axis_index("mp")
    low_bit = idx % 2
    half = partial.shape[0] // 2
    mine = lax.dynamic_slice_in_dim(partial, low_bit * half, half, 0)
    other = lax.dynamic_slice_in_dim(partial, (1 - low_bit) * half, half, 0)
    got = lax.ppermute(other, "mp", [(k, k ^ 1) for k in range(4)])
    first = (mine.astype(jnp.float32) + got.astype(jnp.float32)).astype(jnp.bfloat16)
    got_far = lax.ppermute(first, "mp", [(k, k ^ 2) for k in range(4)])
    second = (first.astype(jnp.float32) + got_far.astype(jnp.float32)).astype(jnp.bfloat16)
    got_back = lax.ppermute(second, "mp", [(k, k ^ 1) for k in range(4)])
    top = jnp.where(low_bit == 0, second, got_back)
    bottom = jnp.where(low_bit == 0, got_back, second)
    return jnp.concatenate([top, bottom], axis=0).astype(jnp.float32)


def dp_allreduce(values, n_dp):
    if n_dp & (n_dp - 1):
        return lax.psum(values, "dp")
    total = values
    step = 1
    while step < n_dp:
        total = total + lax.ppermute(total, "dp", [(k, k ^ step) for k in range(n_dp)])
        step *= 2
    return total


def per_device(n_mp, n_dp,
    tokens,
    cotangent,
    item_lengths,
    w_qkv,
    b_qv,
    w_out,
    b_out,
    w_fc1,
    b_fc1,
    w_fc2,
    b_fc2,
    ln1_gain,
    ln1_bias,
    ln2_gain,
    ln2_bias,
):
    row_count = tokens.shape[0]
    local_cols = w_qkv.shape[2]
    heads_here = local_cols // HEAD
    segments = segment_ids(item_lengths[0], row_count)
    inputs = tokens.astype(jnp.float32)
    norm_one, norm_one_back = jax.vjp(normalize, inputs, ln1_gain, ln1_bias)
    normed_one = norm_one.astype(jnp.bfloat16)
    queries = (jnp.dot(normed_one, w_qkv[0], preferred_element_type=jnp.float32) + b_qv[0]).astype(
        jnp.bfloat16
    )
    key_rows = jnp.dot(normed_one, w_qkv[1], preferred_element_type=jnp.float32).astype(
        jnp.bfloat16
    )
    value_rows = (
        jnp.dot(normed_one, w_qkv[2], preferred_element_type=jnp.float32) + b_qv[1]
    ).astype(jnp.bfloat16)

    def to_heads(values):
        return values.reshape(row_count, heads_here, HEAD).transpose(1, 0, 2)

    def from_heads(values):
        return values.transpose(1, 0, 2).reshape(row_count, local_cols)

    lo_blocks, hi_blocks = block_ranges(segments, item_lengths[0])
    query_heads = to_heads(queries)
    key_heads = to_heads(key_rows)
    value_heads = to_heads(value_rows)
    out_heads, out_f32, log_norms = flash_forward(
        query_heads, key_heads, value_heads, segments, lo_blocks, hi_blocks
    )
    attended = out_heads.transpose(2, 0, 1).reshape(row_count, local_cols)
    attention_sum = mp_allreduce(
        jnp.dot(attended, w_out, preferred_element_type=jnp.float32).astype(jnp.bfloat16), n_mp,
    )
    middle = inputs + attention_sum + b_out
    norm_two, norm_two_back = jax.vjp(normalize, middle, ln2_gain, ln2_bias)
    normed_two = norm_two.astype(jnp.bfloat16)
    hidden_pre = jnp.dot(normed_two, w_fc1, preferred_element_type=jnp.float32) + b_fc1
    activated_full, gelu_back = jax.vjp(exact_gelu, hidden_pre)
    activated = activated_full.astype(jnp.bfloat16)
    mlp_partial = jnp.dot(activated, w_fc2, preferred_element_type=jnp.float32).astype(jnp.bfloat16)
    upstream = cotangent.astype(jnp.float32)
    grad_b_fc2 = jnp.sum(upstream, axis=0)
    grad_w_fc2 = jnp.einsum("tf,td->fd", activated, cotangent, preferred_element_type=jnp.float32)
    d_act = jnp.einsum("td,fd->tf", cotangent, w_fc2, preferred_element_type=jnp.float32)
    d_pre = gelu_back(d_act)[0]
    grad_b_fc1 = jnp.sum(d_pre, axis=0)
    d_pre_low = d_pre.astype(jnp.bfloat16)
    grad_w_fc1_t = jnp.einsum("tf,td->fd", d_pre_low, normed_two, preferred_element_type=jnp.float32)
    dn_two_partial = jnp.einsum(
        "tf,df->td", d_pre_low, w_fc1, preferred_element_type=jnp.float32
    ).astype(jnp.bfloat16)
    mlp_weight_grads = jnp.concatenate([grad_w_fc2, grad_w_fc1_t], axis=0).astype(jnp.bfloat16)
    mlp_weight_grads, dn_two_partial = lax.optimization_barrier((mlp_weight_grads, dn_two_partial))
    summed_mlp = lax.psum_scatter(mlp_weight_grads, "dp", scatter_dimension=1, tiled=True)
    d_normed_two = mp_allreduce(dn_two_partial, n_mp)
    d_middle_norm, grad_ln2_gain, grad_ln2_bias = norm_two_back(d_normed_two)
    d_middle = upstream + d_middle_norm
    mlp_partial, d_middle = lax.optimization_barrier((mlp_partial, d_middle))
    mlp_sum = mp_allreduce(mlp_partial, n_mp)
    output = (middle + mlp_sum + b_fc2).astype(jnp.bfloat16)
    grad_b_out = jnp.sum(d_middle, axis=0)
    d_middle_low = d_middle.astype(jnp.bfloat16)
    grad_w_out = jnp.einsum("tc,td->cd", attended, d_middle_low, preferred_element_type=jnp.float32)
    d_attended = jnp.einsum(
        "td,cd->tc", d_middle_low, w_out, preferred_element_type=jnp.float32
    ).astype(jnp.bfloat16)
    d_att_heads = to_heads(d_attended)
    d_q_heads, d_k_heads, d_v_heads = flash_backward(
        query_heads, key_heads, value_heads, d_att_heads, out_f32, log_norms,
        segments, lo_blocks, hi_blocks,
    )
    summed_mlp, d_q_heads = lax.optimization_barrier((summed_mlp, d_q_heads))
    d_queries = d_q_heads.transpose(2, 0, 1).reshape(row_count, local_cols)
    d_keys = from_heads(d_k_heads)
    d_values = from_heads(d_v_heads)
    grad_b_qv = jnp.stack([jnp.sum(d_queries, axis=0), jnp.sum(d_values, axis=0)])
    stacked = jnp.stack([d_queries, d_keys, d_values]).astype(jnp.bfloat16)
    grad_w_qkv_t = jnp.einsum("stc,td->scd", stacked, normed_one, preferred_element_type=jnp.float32)
    d_normed_one = mp_allreduce(
        jnp.einsum("stc,sdc->td", stacked, w_qkv, preferred_element_type=jnp.float32).astype(
            jnp.bfloat16
        ),
        n_mp,
    )
    d_input_norm, grad_ln1_gain, grad_ln1_bias = norm_one_back(d_normed_one)
    grad_tokens = d_middle + d_input_norm

    def scatter(grad, dim):
        return lax.psum_scatter(grad.astype(jnp.bfloat16), "dp", scatter_dimension=dim, tiled=True).astype(jnp.float32)

    tail_grads = jnp.concatenate(
        [grad_w_qkv_t.reshape(3 * local_cols, -1), grad_w_out], axis=0
    )
    summed_tail = scatter(tail_grads, 1)
    share = summed_tail.shape[1]
    summed_qkv = summed_tail[: 3 * local_cols].reshape(3, local_cols, share).transpose(0, 2, 1)
    summed_out = summed_tail[3 * local_cols :]
    summed_mlp = summed_mlp.astype(jnp.float32)
    units = grad_w_fc2.shape[0]
    summed_fc2 = summed_mlp[:units]
    summed_fc1 = summed_mlp[units:].T
    early = dp_allreduce(
        jnp.concatenate([grad_ln2_gain, grad_ln2_bias, grad_b_out, grad_b_fc2, grad_b_fc1]), n_dp
    )
    late = dp_allreduce(jnp.concatenate([grad_ln1_gain, grad_ln1_bias, grad_b_qv.reshape(-1)]), n_dp)
    width = grad_ln1_gain.shape[0]
    pieces = [late[0:width], late[width : 2 * width]] + [
        early[k * width : (k + 1) * width] for k in range(4)
    ]
    summed_b_qv = late[2 * width :].reshape(grad_b_qv.shape)
    summed_b_fc1 = early[4 * width :]
    return (
        output,
        grad_tokens,
        summed_qkv,
        summed_b_qv,
        summed_out,
        pieces[4],
        summed_fc1,
        summed_b_fc1,
        summed_fc2,
        pieces[5],
        pieces[0],
        pieces[1],
        pieces[2],
        pieces[3],
    )


def solution(mesh):
    in_specs = (
        P("dp", None),
        P("dp", None),
        P("dp", None),
        P(None, None, "mp"),
        P(None, "mp"),
        P("mp", None),
        P(),
        P(None, "mp"),
        P("mp"),
        P("mp", None),
        P(),
        P(),
        P(),
        P(),
        P(),
    )
    out_specs = (
        P("dp", None),
        P("dp", None),
        P(None, "dp", "mp"),
        P(None, "mp"),
        P("mp", "dp"),
        P(),
        P("dp", "mp"),
        P("mp"),
        P("mp", "dp"),
        P(),
        P(),
        P(),
        P(),
        P(),
    )

    def body(*args):
        return per_device(mesh.shape["mp"], mesh.shape["dp"], *args)

    return jax.shard_map(
        body, mesh=mesh, in_specs=in_specs, out_specs=out_specs, check_vma=False
    )
```

```python
import jax
import jax.numpy as jnp
from jax import lax
from jax.experimental import pallas as pl
from jax.experimental.pallas import tpu as pltpu
from jax.sharding import PartitionSpec as P


HEAD = 64
TQ = 256
TK = 256
NEG = -1e30


def _fwd_kernel(lo_ref, hi_ref, segc_ref, segr_ref, qt_ref, k_ref, vt_ref, ot_ref, o32t_ref, lse_ref):
    rows = qt_ref.shape[2]
    scale = HEAD ** (-0.5)

    def q_body(i, carry):
        r0 = pl.multiple_of(i * TQ, TQ)
        qt = qt_ref[0, :, pl.ds(r0, TQ)]
        sq = segr_ref[:, pl.ds(r0, TQ)]

        def kv_body(j, state):
            m, l, acc = state
            c0 = pl.multiple_of(j * TK, TK)
            s = jnp.dot(k_ref[0, pl.ds(c0, TK), :], qt, preferred_element_type=jnp.float32) * scale
            same = segc_ref[pl.ds(c0, TK), :] == sq
            s = jnp.where(same, s, NEG)
            m_new = jnp.maximum(m, jnp.max(s, axis=0, keepdims=True))
            p = jnp.exp(s - m_new)
            alpha = jnp.exp(m - m_new)
            l = alpha * l + jnp.sum(p, axis=0, keepdims=True)
            pv = jnp.dot(vt_ref[0, :, pl.ds(c0, TK)], p.astype(jnp.bfloat16),
                         preferred_element_type=jnp.float32)
            return m_new, l, alpha * acc + pv

        m0 = jnp.full((1, TQ), NEG, jnp.float32)
        l0 = jnp.zeros((1, TQ), jnp.float32)
        acc0 = jnp.zeros((HEAD, TQ), jnp.float32)
        m, l, acc = lax.fori_loop(lo_ref[i], hi_ref[i], kv_body, (m0, l0, acc0))
        out = acc / l
        ot_ref[0, :, pl.ds(r0, TQ)] = out.astype(ot_ref.dtype)
        o32t_ref[0, :, pl.ds(r0, TQ)] = out
        lse_ref[0, :, pl.ds(r0, TQ)] = m + jnp.log(l)
        return carry

    lax.fori_loop(0, rows // TQ, q_body, 0)


def _bwd_kernel(lo_ref, hi_ref, segc_ref, segr_ref, q_ref, qt_ref, k_ref, kt_ref, v_ref, do_ref, dot_ref,
                o32t_ref, lse_ref, dqt_ref, dk_ref, dv_ref, dvec_ref):
    rows = q_ref.shape[1]
    scale = HEAD ** (-0.5)
    dqt_ref[...] = jnp.zeros_like(dqt_ref)

    def d_body(i, carry):
        r0 = pl.multiple_of(i * TQ, TQ)
        prod = dot_ref[0, :, pl.ds(r0, TQ)].astype(jnp.float32) * o32t_ref[0, :, pl.ds(r0, TQ)]
        dvec_ref[:, pl.ds(r0, TQ)] = jnp.sum(prod, axis=0, keepdims=True)
        return carry

    lax.fori_loop(0, rows // TQ, d_body, 0)

    def kv_body(j, carry):
        c0 = pl.multiple_of(j * TK, TK)
        k = k_ref[0, pl.ds(c0, TK), :]
        v = v_ref[0, pl.ds(c0, TK), :]
        kt = kt_ref[0, :, pl.ds(c0, TK)]
        sk = segc_ref[pl.ds(c0, TK), :]

        def q_body(i, grads):
            dk, dv = grads
            r0 = pl.multiple_of(i * TQ, TQ)
            s = jnp.dot(k, qt_ref[0, :, pl.ds(r0, TQ)], preferred_element_type=jnp.float32) * scale
            same = sk == segr_ref[:, pl.ds(r0, TQ)]
            s = jnp.where(same, s, NEG)
            p = jnp.exp(s - lse_ref[0, :, pl.ds(r0, TQ)])
            dp = jnp.dot(v, dot_ref[0, :, pl.ds(r0, TQ)], preferred_element_type=jnp.float32)
            ds = (p * (dp - dvec_ref[:, pl.ds(r0, TQ)])).astype(jnp.bfloat16)
            dv = dv + jnp.dot(p.astype(jnp.bfloat16), do_ref[0, pl.ds(r0, TQ), :],
                              preferred_element_type=jnp.float32)
            dk = dk + jnp.dot(ds, q_ref[0, pl.ds(r0, TQ), :], preferred_element_type=jnp.float32)
            dqt_ref[0, :, pl.ds(r0, TQ)] += jnp.dot(kt, ds, preferred_element_type=jnp.float32)
            return dk, dv

        zeros = jnp.zeros((TK, HEAD), jnp.float32)
        dk, dv = lax.fori_loop(lo_ref[j], hi_ref[j], q_body, (zeros, zeros))
        dk_ref[0, pl.ds(c0, TK), :] = dk * scale
        dv_ref[0, pl.ds(c0, TK), :] = dv
        return carry

    lax.fori_loop(0, rows // TK, kv_body, 0)
    dqt_ref[...] = dqt_ref[...] * scale


def block_ranges(segments, item_lengths_row):
    rows = segments.shape[0]
    ends = jnp.cumsum(item_lengths_row.astype(jnp.int32))
    starts = ends - item_lengths_row.astype(jnp.int32)
    first = segments[0::TQ]
    last = segments[TQ - 1::TQ]
    n_items = item_lengths_row.shape[0]
    key_lo = jnp.take(starts, jnp.clip(first, 0, n_items - 1))
    key_hi = jnp.take(ends, jnp.clip(last, 0, n_items - 1))
    lo = jnp.clip(key_lo // TK, 0, rows // TK)
    hi = jnp.clip((key_hi + TK - 1) // TK, 0, rows // TK)
    return lo.astype(jnp.int32), hi.astype(jnp.int32)


def _head_specs(rows):
    plain = pl.BlockSpec((1, rows, HEAD), lambda h, lo, hi: (h, 0, 0))
    flipped = pl.BlockSpec((1, HEAD, rows), lambda h, lo, hi: (h, 0, 0))
    stat = pl.BlockSpec((1, 1, rows), lambda h, lo, hi: (h, 0, 0))
    col = pl.BlockSpec((rows, 1), lambda h, lo, hi: (0, 0))
    row = pl.BlockSpec((1, rows), lambda h, lo, hi: (0, 0))
    return plain, flipped, stat, col, row


def flash_forward(qt, k, vt, seg_q, seg_k, lo, hi):
    heads, _, rows_q = qt.shape
    rows_k = k.shape[1]
    flipped_q = pl.BlockSpec((1, HEAD, rows_q), lambda h, lo, hi: (h, 0, 0))
    flipped_k = pl.BlockSpec((1, HEAD, rows_k), lambda h, lo, hi: (h, 0, 0))
    plain_k = pl.BlockSpec((1, rows_k, HEAD), lambda h, lo, hi: (h, 0, 0))
    stat = pl.BlockSpec((1, 1, rows_q), lambda h, lo, hi: (h, 0, 0))
    col = pl.BlockSpec((rows_k, 1), lambda h, lo, hi: (0, 0))
    row = pl.BlockSpec((1, rows_q), lambda h, lo, hi: (0, 0))
    flops = int(heads * rows_q * rows_k * HEAD * 2 * 2 * 0.6)
    return pl.pallas_call(
        _fwd_kernel,
        out_shape=(
            jax.ShapeDtypeStruct((heads, HEAD, rows_q), jnp.bfloat16),
            jax.ShapeDtypeStruct((heads, HEAD, rows_q), jnp.float32),
            jax.ShapeDtypeStruct((heads, 1, rows_q), jnp.float32),
        ),
        grid_spec=pltpu.PrefetchScalarGridSpec(
            num_scalar_prefetch=2,
            grid=(heads,),
            in_specs=[col, row, flipped_q, plain_k, flipped_k],
            out_specs=[flipped_q, flipped_q, stat],
        ),
        compiler_params=pltpu.CompilerParams(
            dimension_semantics=("arbitrary",), vmem_limit_bytes=48 * 1024 * 1024),
        cost_estimate=pl.CostEstimate(
            flops=flops, transcendentals=int(heads * rows_q * rows_k * 0.6),
            bytes_accessed=int(heads * HEAD * (rows_q * 8 + rows_k * 4))),
        name="segment_flash_fwd",
    )(lo, hi, seg_k.reshape(rows_k, 1), seg_q.reshape(1, rows_q), qt, k, vt)


def flash_backward(q, k, v, do, o32t, lse, segments, lo, hi):
    heads, rows, _ = q.shape
    plain, flipped, stat, col, row = _head_specs(rows)
    flops = int(heads * rows * rows * HEAD * 2 * 4 * 0.6)
    return pl.pallas_call(
        _bwd_kernel,
        out_shape=(
            jax.ShapeDtypeStruct((heads, HEAD, rows), jnp.float32),
            jax.ShapeDtypeStruct((heads, rows, HEAD), jnp.float32),
            jax.ShapeDtypeStruct((heads, rows, HEAD), jnp.float32),
        ),
        grid_spec=pltpu.PrefetchScalarGridSpec(
            num_scalar_prefetch=2,
            grid=(heads,),
            in_specs=[col, row, plain, flipped, plain, flipped, plain, plain, flipped, flipped, stat],
            out_specs=[flipped, plain, plain],
            scratch_shapes=[pltpu.VMEM((1, rows), jnp.float32)],
        ),
        compiler_params=pltpu.CompilerParams(
            dimension_semantics=("arbitrary",), vmem_limit_bytes=48 * 1024 * 1024),
        cost_estimate=pl.CostEstimate(
            flops=flops, transcendentals=int(heads * rows * rows * 0.6),
            bytes_accessed=int(heads * rows * HEAD * (2 * 7 + 4 * 4) + heads * rows * 4)),
        name="segment_flash_bwd",
    )(lo, hi, segments.reshape(rows, 1), segments.reshape(1, rows),
      q, q.transpose(0, 2, 1), k, k.transpose(0, 2, 1), v, do, do.transpose(0, 2, 1), o32t, lse)


def normalize(values, gain, shift):
    center = jnp.mean(values, axis=-1, keepdims=True)
    centered = values - center
    spread = jnp.mean(centered * centered, axis=-1, keepdims=True)
    return centered * lax.rsqrt(spread + 1e-06) * gain + shift


def exact_gelu(values):
    return jax.nn.gelu(values, approximate=False)


def segment_ids(lengths_row, row_count):
    ends = jnp.cumsum(lengths_row)
    positions = jnp.arange(row_count, dtype=jnp.int32)
    return jnp.sum((positions[:, None] >= ends[None, :]).astype(jnp.int32), axis=1)


def mp_allreduce(partial, n_mp):
    if n_mp != 4:
        return lax.psum(partial, "mp").astype(jnp.float32)
    idx = lax.axis_index("mp")
    low_bit = idx % 2
    half = partial.shape[0] // 2
    mine = lax.dynamic_slice_in_dim(partial, low_bit * half, half, 0)
    other = lax.dynamic_slice_in_dim(partial, (1 - low_bit) * half, half, 0)
    got = lax.ppermute(other, "mp", [(k, k ^ 1) for k in range(4)])
    first = (mine.astype(jnp.float32) + got.astype(jnp.float32)).astype(jnp.bfloat16)
    got_far = lax.ppermute(first, "mp", [(k, k ^ 2) for k in range(4)])
    second = (first.astype(jnp.float32) + got_far.astype(jnp.float32)).astype(jnp.bfloat16)
    got_back = lax.ppermute(second, "mp", [(k, k ^ 1) for k in range(4)])
    top = jnp.where(low_bit == 0, second, got_back)
    bottom = jnp.where(low_bit == 0, got_back, second)
    return jnp.concatenate([top, bottom], axis=0).astype(jnp.float32)


def dp_allreduce(values, n_dp):
    if n_dp & (n_dp - 1):
        return lax.psum(values, "dp")
    total = values
    step = 1
    while step < n_dp:
        total = total + lax.ppermute(total, "dp", [(k, k ^ step) for k in range(n_dp)])
        step *= 2
    return total


def per_device(n_mp, n_dp,
    tokens,
    cotangent,
    item_lengths,
    w_qkv,
    b_qv,
    w_out,
    b_out,
    w_fc1,
    b_fc1,
    w_fc2,
    b_fc2,
    ln1_gain,
    ln1_bias,
    ln2_gain,
    ln2_bias,
):
    row_count = tokens.shape[0]
    local_cols = w_qkv.shape[2]
    heads_here = local_cols // HEAD
    segments = segment_ids(item_lengths[0], row_count)
    inputs = tokens.astype(jnp.float32)
    norm_one, norm_one_back = jax.vjp(normalize, inputs, ln1_gain, ln1_bias)
    normed_one = norm_one.astype(jnp.bfloat16)
    queries = (jnp.dot(normed_one, w_qkv[0], preferred_element_type=jnp.float32) + b_qv[0]).astype(
        jnp.bfloat16
    )
    key_rows = jnp.dot(normed_one, w_qkv[1], preferred_element_type=jnp.float32).astype(
        jnp.bfloat16
    )
    value_rows = (
        jnp.dot(normed_one, w_qkv[2], preferred_element_type=jnp.float32) + b_qv[1]
    ).astype(jnp.bfloat16)

    def to_heads(values):
        return values.reshape(values.shape[0], heads_here, HEAD).transpose(1, 0, 2)

    def from_heads(values):
        return values.transpose(1, 0, 2).reshape(row_count, local_cols)

    lo_blocks, hi_blocks = block_ranges(segments, item_lengths[0])
    query_heads = to_heads(queries)
    key_heads = to_heads(key_rows)
    value_heads = to_heads(value_rows)
    query_t = queries.reshape(row_count, heads_here, HEAD).transpose(1, 2, 0)
    value_t = value_rows.reshape(row_count, heads_here, HEAD).transpose(1, 2, 0)
    upstream = cotangent.astype(jnp.float32)
    q_blocks = row_count // TQ
    first_blocks = (q_blocks * 3) // 8
    bounds = [(0, first_blocks), (first_blocks, q_blocks)]
    pieces_fwd = []
    for b0, b1 in bounds:
        rows = slice(b0 * TQ, b1 * TQ)
        out_t, out32_t, lse_h = flash_forward(
            query_t[:, :, rows], key_heads, value_t, segments[rows], segments,
            lo_blocks[b0:b1], hi_blocks[b0:b1],
        )
        attended_h = out_t.transpose(2, 0, 1).reshape((b1 - b0) * TQ, local_cols)
        att_sum_h = mp_allreduce(
            jnp.dot(attended_h, w_out, preferred_element_type=jnp.float32).astype(jnp.bfloat16),
            n_mp,
        )
        middle_h = inputs[rows] + att_sum_h + b_out
        norm_two_h, back_two_h = jax.vjp(normalize, middle_h, ln2_gain, ln2_bias)
        normed_two_h = norm_two_h.astype(jnp.bfloat16)
        hidden_pre_h = jnp.dot(normed_two_h, w_fc1, preferred_element_type=jnp.float32) + b_fc1
        act_h, gelu_back_h = jax.vjp(exact_gelu, hidden_pre_h)
        activated_h = act_h.astype(jnp.bfloat16)
        mlp_partial_h = jnp.dot(
            activated_h, w_fc2, preferred_element_type=jnp.float32
        ).astype(jnp.bfloat16)
        pieces_fwd.append(dict(
            rows=rows, out32_t=out32_t, lse=lse_h, attended=attended_h, middle=middle_h,
            back_two=back_two_h, normed_two=normed_two_h, gelu_back=gelu_back_h,
            activated=activated_h, mlp_partial=mlp_partial_h,
        ))
    grad_b_fc2 = jnp.sum(upstream, axis=0)
    for piece in pieces_fwd:
        d_act_h = jnp.einsum(
            "td,fd->tf", cotangent[piece["rows"]], w_fc2, preferred_element_type=jnp.float32
        )
        d_pre_h = piece["gelu_back"](d_act_h)[0]
        piece["b_fc1"] = jnp.sum(d_pre_h, axis=0)
        piece["d_pre_low"] = d_pre_h.astype(jnp.bfloat16)
        piece["dn_two_partial"] = jnp.einsum(
            "tf,df->td", piece["d_pre_low"], w_fc1, preferred_element_type=jnp.float32
        ).astype(jnp.bfloat16)
    activated = jnp.concatenate([p["activated"] for p in pieces_fwd], axis=0)
    normed_two = jnp.concatenate([p["normed_two"] for p in pieces_fwd], axis=0)
    d_pre_low = jnp.concatenate([p["d_pre_low"] for p in pieces_fwd], axis=0)
    grad_b_fc1 = sum(p["b_fc1"] for p in pieces_fwd)
    grad_w_fc2 = jnp.einsum("tf,td->fd", activated, cotangent, preferred_element_type=jnp.float32)
    grad_w_fc1_t = jnp.einsum("tf,td->fd", d_pre_low, normed_two, preferred_element_type=jnp.float32)
    mlp_weight_grads = jnp.concatenate([grad_w_fc2, grad_w_fc1_t], axis=0).astype(jnp.bfloat16)
    mlp_weight_grads, pieces_fwd[-1]["dn_two_partial"] = lax.optimization_barrier(
        (mlp_weight_grads, pieces_fwd[-1]["dn_two_partial"])
    )
    summed_mlp = lax.psum_scatter(mlp_weight_grads, "dp", scatter_dimension=1, tiled=True)
    for piece in pieces_fwd:
        d_normed_two_h = mp_allreduce(piece["dn_two_partial"], n_mp)
        d_mid_norm_h, gain_h, shift_h = piece["back_two"](d_normed_two_h)
        piece["ln2_gain"] = gain_h
        piece["ln2_bias"] = shift_h
        piece["d_middle"] = upstream[piece["rows"]] + d_mid_norm_h
        d_middle_low_h = piece["d_middle"].astype(jnp.bfloat16)
        piece["d_middle_low"] = d_middle_low_h
        piece["d_attended"] = jnp.einsum(
            "td,cd->tc", d_middle_low_h, w_out, preferred_element_type=jnp.float32
        ).astype(jnp.bfloat16)
    grad_ln2_gain = sum(p["ln2_gain"] for p in pieces_fwd)
    grad_ln2_bias = sum(p["ln2_bias"] for p in pieces_fwd)
    d_middle = jnp.concatenate([p["d_middle"] for p in pieces_fwd], axis=0)
    grad_b_out = jnp.sum(d_middle, axis=0)
    d_middle_low = jnp.concatenate([p["d_middle_low"] for p in pieces_fwd], axis=0)
    attended = jnp.concatenate([p["attended"] for p in pieces_fwd], axis=0)
    grad_w_out = jnp.einsum("tc,td->cd", attended, d_middle_low, preferred_element_type=jnp.float32)
    d_attended = jnp.concatenate([p["d_attended"] for p in pieces_fwd], axis=0)
    out_f32 = jnp.concatenate([p["out32_t"] for p in pieces_fwd], axis=2)
    log_norms = jnp.concatenate([p["lse"] for p in pieces_fwd], axis=2)
    d_att_heads = to_heads(d_attended)
    partials = lax.optimization_barrier(tuple(p["mlp_partial"] for p in pieces_fwd) + (d_att_heads,))
    d_att_heads = partials[-1]
    outputs = []
    for h, piece in enumerate(pieces_fwd):
        mlp_sum_h = mp_allreduce(partials[h], n_mp)
        outputs.append((piece["middle"] + mlp_sum_h + b_fc2).astype(jnp.bfloat16))
    output = jnp.concatenate(outputs, axis=0)
    d_q_heads, d_k_heads, d_v_heads = flash_backward(
        query_heads, key_heads, value_heads, d_att_heads, out_f32, log_norms,
        segments, lo_blocks, hi_blocks,
    )
    summed_mlp, d_q_heads = lax.optimization_barrier((summed_mlp, d_q_heads))
    d_queries = d_q_heads.transpose(2, 0, 1).reshape(row_count, local_cols)
    d_keys = from_heads(d_k_heads)
    d_values = from_heads(d_v_heads)
    grad_b_qv = jnp.stack([jnp.sum(d_queries, axis=0), jnp.sum(d_values, axis=0)])
    stacked = jnp.stack([d_queries, d_keys, d_values]).astype(jnp.bfloat16)
    grad_w_qkv_t = jnp.einsum("stc,td->scd", stacked, normed_one, preferred_element_type=jnp.float32)
    d_normed_one = mp_allreduce(
        jnp.einsum("stc,sdc->td", stacked, w_qkv, preferred_element_type=jnp.float32).astype(
            jnp.bfloat16
        ),
        n_mp,
    )
    d_input_norm, grad_ln1_gain, grad_ln1_bias = norm_one_back(d_normed_one)
    grad_tokens = d_middle + d_input_norm

    def scatter(grad, dim):
        return lax.psum_scatter(
            grad.astype(jnp.bfloat16), "dp", scatter_dimension=dim, tiled=True
        ).astype(jnp.float32)

    tail_grads = jnp.concatenate(
        [grad_w_qkv_t.reshape(3 * local_cols, -1), grad_w_out], axis=0
    )
    summed_tail = scatter(tail_grads, 1)
    share = summed_tail.shape[1]
    summed_qkv = summed_tail[: 3 * local_cols].reshape(3, local_cols, share).transpose(0, 2, 1)
    summed_out = summed_tail[3 * local_cols :]
    summed_mlp = summed_mlp.astype(jnp.float32)
    units = grad_w_fc2.shape[0]
    summed_fc2 = summed_mlp[:units]
    summed_fc1 = summed_mlp[units:].T
    early = dp_allreduce(
        jnp.concatenate([grad_ln2_gain, grad_ln2_bias, grad_b_out, grad_b_fc2, grad_b_fc1]), n_dp
    )
    late = dp_allreduce(jnp.concatenate([grad_ln1_gain, grad_ln1_bias, grad_b_qv.reshape(-1)]), n_dp)
    width = grad_ln1_gain.shape[0]
    pieces = [late[0:width], late[width : 2 * width]] + [
        early[k * width : (k + 1) * width] for k in range(4)
    ]
    summed_b_qv = late[2 * width :].reshape(grad_b_qv.shape)
    summed_b_fc1 = early[4 * width :]
    return (
        output,
        grad_tokens,
        summed_qkv,
        summed_b_qv,
        summed_out,
        pieces[4],
        summed_fc1,
        summed_b_fc1,
        summed_fc2,
        pieces[5],
        pieces[0],
        pieces[1],
        pieces[2],
        pieces[3],
    )


def solution(mesh):
    in_specs = (
        P("dp", None),
        P("dp", None),
        P("dp", None),
        P(None, None, "mp"),
        P(None, "mp"),
        P("mp", None),
        P(),
        P(None, "mp"),
        P("mp"),
        P("mp", None),
        P(),
        P(),
        P(),
        P(),
        P(),
    )
    out_specs = (
        P("dp", None),
        P("dp", None),
        P(None, "dp", "mp"),
        P(None, "mp"),
        P("mp", "dp"),
        P(),
        P("dp", "mp"),
        P("mp"),
        P("mp", "dp"),
        P(),
        P(),
        P(),
        P(),
        P(),
    )

    def body(*args):
        return per_device(mesh.shape["mp"], mesh.shape["dp"], *args)

    return jax.shard_map(
        body, mesh=mesh, in_specs=in_specs, out_specs=out_specs, check_vma=False
    )
```

```python
import jax
import jax.numpy as jnp
from jax import lax
from jax.experimental import pallas as pl
from jax.experimental.pallas import tpu as pltpu
from jax.sharding import PartitionSpec as P


HEAD = 64
TQ = 256
TK = 256
NEG = -1e30


HPS = 4


def _fwd_kernel(lo_ref, hi_ref, segc_ref, segr_ref, qt_ref, k_ref, vt_ref, ot_ref, o32t_ref, lse_ref):
    rows = qt_ref.shape[2]
    scale = HEAD ** (-0.5)

    def q_body(i, carry):
        r0 = pl.multiple_of(i * TQ, TQ)
        qts = [qt_ref[hh, :, pl.ds(r0, TQ)] for hh in range(HPS)]
        sq = segr_ref[:, pl.ds(r0, TQ)]

        def kv_body(j, state):
            c0 = pl.multiple_of(j * TK, TK)
            same = segc_ref[pl.ds(c0, TK), :] == sq
            new_state = []
            for hh in range(HPS):
                m, l, acc = state[hh]
                s = jnp.dot(k_ref[hh, pl.ds(c0, TK), :], qts[hh], preferred_element_type=jnp.float32) * scale
                s = jnp.where(same, s, NEG)
                m_new = jnp.maximum(m, jnp.max(s, axis=0, keepdims=True))
                p = jnp.exp(s - m_new)
                alpha = jnp.exp(m - m_new)
                l = alpha * l + jnp.sum(p, axis=0, keepdims=True)
                pv = jnp.dot(vt_ref[hh, :, pl.ds(c0, TK)], p.astype(jnp.bfloat16),
                             preferred_element_type=jnp.float32)
                new_state.append((m_new, l, alpha * acc + pv))
            return tuple(new_state)

        init = tuple(
            (jnp.full((1, TQ), NEG, jnp.float32), jnp.zeros((1, TQ), jnp.float32),
             jnp.zeros((HEAD, TQ), jnp.float32))
            for _ in range(HPS)
        )
        final = lax.fori_loop(lo_ref[i], hi_ref[i], kv_body, init)
        for hh in range(HPS):
            m, l, acc = final[hh]
            out = acc / l
            ot_ref[hh, :, pl.ds(r0, TQ)] = out.astype(ot_ref.dtype)
            o32t_ref[hh, :, pl.ds(r0, TQ)] = out
            lse_ref[hh, :, pl.ds(r0, TQ)] = m + jnp.log(l)
        return carry

    lax.fori_loop(0, rows // TQ, q_body, 0)


def _bwd_kernel(lo_ref, hi_ref, segc_ref, segr_ref, q_ref, qt_ref, k_ref, kt_ref, v_ref, do_ref, dot_ref,
                o32t_ref, lse_ref, dqt_ref, dk_ref, dv_ref, dvec_ref):
    rows = q_ref.shape[1]
    scale = HEAD ** (-0.5)
    dqt_ref[...] = jnp.zeros_like(dqt_ref)

    def d_body(i, carry):
        r0 = pl.multiple_of(i * TQ, TQ)
        for hh in range(HPS):
            prod = dot_ref[hh, :, pl.ds(r0, TQ)].astype(jnp.float32) * o32t_ref[hh, :, pl.ds(r0, TQ)]
            dvec_ref[hh, :, pl.ds(r0, TQ)] = jnp.sum(prod, axis=0, keepdims=True)
        return carry

    lax.fori_loop(0, rows // TQ, d_body, 0)

    def kv_body(j, carry):
        c0 = pl.multiple_of(j * TK, TK)
        ks = [k_ref[hh, pl.ds(c0, TK), :] for hh in range(HPS)]
        vs = [v_ref[hh, pl.ds(c0, TK), :] for hh in range(HPS)]
        kts = [kt_ref[hh, :, pl.ds(c0, TK)] for hh in range(HPS)]
        sk = segc_ref[pl.ds(c0, TK), :]

        def q_body(i, grads):
            r0 = pl.multiple_of(i * TQ, TQ)
            same = sk == segr_ref[:, pl.ds(r0, TQ)]
            new_grads = []
            for hh in range(HPS):
                dk, dv = grads[hh]
                s = jnp.dot(ks[hh], qt_ref[hh, :, pl.ds(r0, TQ)], preferred_element_type=jnp.float32) * scale
                s = jnp.where(same, s, NEG)
                p = jnp.exp(s - lse_ref[hh, :, pl.ds(r0, TQ)])
                dp = jnp.dot(vs[hh], dot_ref[hh, :, pl.ds(r0, TQ)], preferred_element_type=jnp.float32)
                ds = (p * (dp - dvec_ref[hh, :, pl.ds(r0, TQ)])).astype(jnp.bfloat16)
                dv = dv + jnp.dot(p.astype(jnp.bfloat16), do_ref[hh, pl.ds(r0, TQ), :],
                                  preferred_element_type=jnp.float32)
                dk = dk + jnp.dot(ds, q_ref[hh, pl.ds(r0, TQ), :], preferred_element_type=jnp.float32)
                dqt_ref[hh, :, pl.ds(r0, TQ)] += jnp.dot(kts[hh], ds, preferred_element_type=jnp.float32)
                new_grads.append((dk, dv))
            return tuple(new_grads)

        zeros = jnp.zeros((TK, HEAD), jnp.float32)
        final = lax.fori_loop(lo_ref[j], hi_ref[j], q_body, tuple((zeros, zeros) for _ in range(HPS)))
        for hh in range(HPS):
            dk, dv = final[hh]
            dk_ref[hh, pl.ds(c0, TK), :] = dk * scale
            dv_ref[hh, pl.ds(c0, TK), :] = dv
        return carry

    lax.fori_loop(0, rows // TK, kv_body, 0)
    dqt_ref[...] = dqt_ref[...] * scale


def block_ranges(segments, item_lengths_row):
    rows = segments.shape[0]
    ends = jnp.cumsum(item_lengths_row.astype(jnp.int32))
    starts = ends - item_lengths_row.astype(jnp.int32)
    first = segments[0::TQ]
    last = segments[TQ - 1::TQ]
    n_items = item_lengths_row.shape[0]
    key_lo = jnp.take(starts, jnp.clip(first, 0, n_items - 1))
    key_hi = jnp.take(ends, jnp.clip(last, 0, n_items - 1))
    lo = jnp.clip(key_lo // TK, 0, rows // TK)
    hi = jnp.clip((key_hi + TK - 1) // TK, 0, rows // TK)
    return lo.astype(jnp.int32), hi.astype(jnp.int32)


def _head_specs(rows):
    plain = pl.BlockSpec((HPS, rows, HEAD), lambda h, lo, hi: (h, 0, 0))
    flipped = pl.BlockSpec((HPS, HEAD, rows), lambda h, lo, hi: (h, 0, 0))
    stat = pl.BlockSpec((HPS, 1, rows), lambda h, lo, hi: (h, 0, 0))
    col = pl.BlockSpec((rows, 1), lambda h, lo, hi: (0, 0))
    row = pl.BlockSpec((1, rows), lambda h, lo, hi: (0, 0))
    return plain, flipped, stat, col, row


def flash_forward(qt, k, vt, seg_q, seg_k, lo, hi):
    heads, _, rows_q = qt.shape
    rows_k = k.shape[1]
    flipped_q = pl.BlockSpec((HPS, HEAD, rows_q), lambda h, lo, hi: (h, 0, 0))
    flipped_k = pl.BlockSpec((HPS, HEAD, rows_k), lambda h, lo, hi: (h, 0, 0))
    plain_k = pl.BlockSpec((HPS, rows_k, HEAD), lambda h, lo, hi: (h, 0, 0))
    stat = pl.BlockSpec((HPS, 1, rows_q), lambda h, lo, hi: (h, 0, 0))
    col = pl.BlockSpec((rows_k, 1), lambda h, lo, hi: (0, 0))
    row = pl.BlockSpec((1, rows_q), lambda h, lo, hi: (0, 0))
    flops = int(heads * rows_q * rows_k * HEAD * 2 * 2 * 0.6)
    return pl.pallas_call(
        _fwd_kernel,
        out_shape=(
            jax.ShapeDtypeStruct((heads, HEAD, rows_q), jnp.bfloat16),
            jax.ShapeDtypeStruct((heads, HEAD, rows_q), jnp.float32),
            jax.ShapeDtypeStruct((heads, 1, rows_q), jnp.float32),
        ),
        grid_spec=pltpu.PrefetchScalarGridSpec(
            num_scalar_prefetch=2,
            grid=(heads // HPS,),
            in_specs=[col, row, flipped_q, plain_k, flipped_k],
            out_specs=[flipped_q, flipped_q, stat],
        ),
        compiler_params=pltpu.CompilerParams(
            dimension_semantics=("arbitrary",), vmem_limit_bytes=48 * 1024 * 1024),
        cost_estimate=pl.CostEstimate(
            flops=flops, transcendentals=int(heads * rows_q * rows_k * 0.6),
            bytes_accessed=int(heads * HEAD * (rows_q * 8 + rows_k * 4))),
        name="segment_flash_fwd",
    )(lo, hi, seg_k.reshape(rows_k, 1), seg_q.reshape(1, rows_q), qt, k, vt)


def flash_backward(q, k, v, do, o32t, lse, segments, lo, hi):
    heads, rows, _ = q.shape
    plain, flipped, stat, col, row = _head_specs(rows)
    flops = int(heads * rows * rows * HEAD * 2 * 4 * 0.6)
    return pl.pallas_call(
        _bwd_kernel,
        out_shape=(
            jax.ShapeDtypeStruct((heads, HEAD, rows), jnp.float32),
            jax.ShapeDtypeStruct((heads, rows, HEAD), jnp.float32),
            jax.ShapeDtypeStruct((heads, rows, HEAD), jnp.float32),
        ),
        grid_spec=pltpu.PrefetchScalarGridSpec(
            num_scalar_prefetch=2,
            grid=(heads // HPS,),
            in_specs=[col, row, plain, flipped, plain, flipped, plain, plain, flipped, flipped, stat],
            out_specs=[flipped, plain, plain],
            scratch_shapes=[pltpu.VMEM((HPS, 1, rows), jnp.float32)],
        ),
        compiler_params=pltpu.CompilerParams(
            dimension_semantics=("arbitrary",), vmem_limit_bytes=48 * 1024 * 1024),
        cost_estimate=pl.CostEstimate(
            flops=flops, transcendentals=int(heads * rows * rows * 0.6),
            bytes_accessed=int(heads * rows * HEAD * (2 * 7 + 4 * 4) + heads * rows * 4)),
        name="segment_flash_bwd",
    )(lo, hi, segments.reshape(rows, 1), segments.reshape(1, rows),
      q, q.transpose(0, 2, 1), k, k.transpose(0, 2, 1), v, do, do.transpose(0, 2, 1), o32t, lse)


def normalize(values, gain, shift):
    center = jnp.mean(values, axis=-1, keepdims=True)
    centered = values - center
    spread = jnp.mean(centered * centered, axis=-1, keepdims=True)
    return centered * lax.rsqrt(spread + 1e-06) * gain + shift


def exact_gelu(values):
    return jax.nn.gelu(values, approximate=False)


def segment_ids(lengths_row, row_count):
    ends = jnp.cumsum(lengths_row)
    positions = jnp.arange(row_count, dtype=jnp.int32)
    return jnp.sum((positions[:, None] >= ends[None, :]).astype(jnp.int32), axis=1)


def mp_allreduce(partial, n_mp):
    if n_mp != 4:
        return lax.psum(partial, "mp").astype(jnp.float32)
    idx = lax.axis_index("mp")
    low_bit = idx % 2
    half = partial.shape[0] // 2
    mine = lax.dynamic_slice_in_dim(partial, low_bit * half, half, 0)
    other = lax.dynamic_slice_in_dim(partial, (1 - low_bit) * half, half, 0)
    got = lax.ppermute(other, "mp", [(k, k ^ 1) for k in range(4)])
    first = (mine.astype(jnp.float32) + got.astype(jnp.float32)).astype(jnp.bfloat16)
    got_far = lax.ppermute(first, "mp", [(k, k ^ 2) for k in range(4)])
    second = (first.astype(jnp.float32) + got_far.astype(jnp.float32)).astype(jnp.bfloat16)
    got_back = lax.ppermute(second, "mp", [(k, k ^ 1) for k in range(4)])
    top = jnp.where(low_bit == 0, second, got_back)
    bottom = jnp.where(low_bit == 0, got_back, second)
    return jnp.concatenate([top, bottom], axis=0).astype(jnp.float32)


def dp_allreduce(values, n_dp):
    if n_dp & (n_dp - 1):
        return lax.psum(values, "dp")
    total = values
    step = 1
    while step < n_dp:
        total = total + lax.ppermute(total, "dp", [(k, k ^ step) for k in range(n_dp)])
        step *= 2
    return total


def per_device(n_mp, n_dp,
    tokens,
    cotangent,
    item_lengths,
    w_qkv,
    b_qv,
    w_out,
    b_out,
    w_fc1,
    b_fc1,
    w_fc2,
    b_fc2,
    ln1_gain,
    ln1_bias,
    ln2_gain,
    ln2_bias,
):
    row_count = tokens.shape[0]
    local_cols = w_qkv.shape[2]
    heads_here = local_cols // HEAD
    segments = segment_ids(item_lengths[0], row_count)
    inputs = tokens.astype(jnp.float32)
    norm_one, norm_one_back = jax.vjp(normalize, inputs, ln1_gain, ln1_bias)
    normed_one = norm_one.astype(jnp.bfloat16)
    queries = (jnp.dot(normed_one, w_qkv[0], preferred_element_type=jnp.float32) + b_qv[0]).astype(
        jnp.bfloat16
    )
    key_rows = jnp.dot(normed_one, w_qkv[1], preferred_element_type=jnp.float32).astype(
        jnp.bfloat16
    )
    value_rows = (
        jnp.dot(normed_one, w_qkv[2], preferred_element_type=jnp.float32) + b_qv[1]
    ).astype(jnp.bfloat16)

    def to_heads(values):
        return values.reshape(values.shape[0], heads_here, HEAD).transpose(1, 0, 2)

    def from_heads(values):
        return values.transpose(1, 0, 2).reshape(row_count, local_cols)

    lo_blocks, hi_blocks = block_ranges(segments, item_lengths[0])
    query_heads = to_heads(queries)
    key_heads = to_heads(key_rows)
    value_heads = to_heads(value_rows)
    query_t = queries.reshape(row_count, heads_here, HEAD).transpose(1, 2, 0)
    value_t = value_rows.reshape(row_count, heads_here, HEAD).transpose(1, 2, 0)
    upstream = cotangent.astype(jnp.float32)
    q_blocks = row_count // TQ
    first_blocks = (q_blocks * 3) // 8
    bounds = [(0, first_blocks), (first_blocks, q_blocks)]
    pieces_fwd = []
    for b0, b1 in bounds:
        rows = slice(b0 * TQ, b1 * TQ)
        out_t, out32_t, lse_h = flash_forward(
            query_t[:, :, rows], key_heads, value_t, segments[rows], segments,
            lo_blocks[b0:b1], hi_blocks[b0:b1],
        )
        attended_h = out_t.transpose(2, 0, 1).reshape((b1 - b0) * TQ, local_cols)
        att_sum_h = mp_allreduce(
            jnp.dot(attended_h, w_out, preferred_element_type=jnp.float32).astype(jnp.bfloat16), n_mp
        )
        middle_h = inputs[rows] + att_sum_h + b_out
        norm_two_h, back_two_h = jax.vjp(normalize, middle_h, ln2_gain, ln2_bias)
        normed_two_h = norm_two_h.astype(jnp.bfloat16)
        hidden_pre_h = jnp.dot(normed_two_h, w_fc1, preferred_element_type=jnp.float32) + b_fc1
        act_h, gelu_back_h = jax.vjp(exact_gelu, hidden_pre_h)
        activated_h = act_h.astype(jnp.bfloat16)
        mlp_partial_h = jnp.dot(
            activated_h, w_fc2, preferred_element_type=jnp.float32
        ).astype(jnp.bfloat16)
        pieces_fwd.append(dict(
            rows=rows, out32_t=out32_t, lse=lse_h, attended=attended_h, middle=middle_h,
            back_two=back_two_h, normed_two=normed_two_h, gelu_back=gelu_back_h,
            activated=activated_h, mlp_partial=mlp_partial_h,
        ))
    grad_b_fc2 = jnp.sum(upstream, axis=0)
    for piece in pieces_fwd:
        d_act_h = jnp.einsum(
            "td,fd->tf", cotangent[piece["rows"]], w_fc2, preferred_element_type=jnp.float32
        )
        d_pre_h = piece["gelu_back"](d_act_h)[0]
        piece["b_fc1"] = jnp.sum(d_pre_h, axis=0)
        piece["d_pre_low"] = d_pre_h.astype(jnp.bfloat16)
        piece["dn_two_partial"] = jnp.einsum(
            "tf,df->td", piece["d_pre_low"], w_fc1, preferred_element_type=jnp.float32
        ).astype(jnp.bfloat16)
    activated = jnp.concatenate([p["activated"] for p in pieces_fwd], axis=0)
    normed_two = jnp.concatenate([p["normed_two"] for p in pieces_fwd], axis=0)
    d_pre_low = jnp.concatenate([p["d_pre_low"] for p in pieces_fwd], axis=0)
    grad_b_fc1 = sum(p["b_fc1"] for p in pieces_fwd)
    grad_w_fc2 = jnp.einsum("tf,td->fd", activated, cotangent, preferred_element_type=jnp.float32)
    grad_w_fc1_t = jnp.einsum("tf,td->fd", d_pre_low, normed_two, preferred_element_type=jnp.float32)
    mlp_weight_grads = jnp.concatenate([grad_w_fc2, grad_w_fc1_t], axis=0).astype(jnp.bfloat16)
    mlp_weight_grads, pieces_fwd[-1]["dn_two_partial"] = lax.optimization_barrier(
        (mlp_weight_grads, pieces_fwd[-1]["dn_two_partial"])
    )
    summed_mlp = lax.psum_scatter(mlp_weight_grads, "dp", scatter_dimension=1, tiled=True)
    for piece in pieces_fwd:
        d_normed_two_h = mp_allreduce(piece["dn_two_partial"], n_mp)
        d_mid_norm_h, gain_h, shift_h = piece["back_two"](d_normed_two_h)
        piece["ln2_gain"] = gain_h
        piece["ln2_bias"] = shift_h
        piece["d_middle"] = upstream[piece["rows"]] + d_mid_norm_h
        d_middle_low_h = piece["d_middle"].astype(jnp.bfloat16)
        piece["d_middle_low"] = d_middle_low_h
        piece["d_attended"] = jnp.einsum(
            "td,cd->tc", d_middle_low_h, w_out, preferred_element_type=jnp.float32
        ).astype(jnp.bfloat16)
    grad_ln2_gain = sum(p["ln2_gain"] for p in pieces_fwd)
    grad_ln2_bias = sum(p["ln2_bias"] for p in pieces_fwd)
    d_middle = jnp.concatenate([p["d_middle"] for p in pieces_fwd], axis=0)
    grad_b_out = jnp.sum(d_middle, axis=0)
    d_middle_low = jnp.concatenate([p["d_middle_low"] for p in pieces_fwd], axis=0)
    attended = jnp.concatenate([p["attended"] for p in pieces_fwd], axis=0)
    grad_w_out = jnp.einsum("tc,td->cd", attended, d_middle_low, preferred_element_type=jnp.float32)
    d_attended = jnp.concatenate([p["d_attended"] for p in pieces_fwd], axis=0)
    out_f32 = jnp.concatenate([p["out32_t"] for p in pieces_fwd], axis=2)
    log_norms = jnp.concatenate([p["lse"] for p in pieces_fwd], axis=2)
    d_att_heads = to_heads(d_attended)
    partials = lax.optimization_barrier(tuple(p["mlp_partial"] for p in pieces_fwd) + (d_att_heads,))
    d_att_heads = partials[-1]
    outputs = []
    for h, piece in enumerate(pieces_fwd):
        mlp_sum_h = mp_allreduce(partials[h], n_mp)
        outputs.append((piece["middle"] + mlp_sum_h + b_fc2).astype(jnp.bfloat16))
    output = jnp.concatenate(outputs, axis=0)
    d_q_heads, d_k_heads, d_v_heads = flash_backward(
        query_heads, key_heads, value_heads, d_att_heads, out_f32, log_norms,
        segments, lo_blocks, hi_blocks,
    )
    summed_mlp, d_q_heads = lax.optimization_barrier((summed_mlp, d_q_heads))
    d_queries = d_q_heads.transpose(2, 0, 1).reshape(row_count, local_cols)
    d_keys = from_heads(d_k_heads)
    d_values = from_heads(d_v_heads)
    grad_b_qv = jnp.stack([jnp.sum(d_queries, axis=0), jnp.sum(d_values, axis=0)])
    stacked = jnp.stack([d_queries, d_keys, d_values]).astype(jnp.bfloat16)
    grad_w_qkv_t = jnp.einsum("stc,td->scd", stacked, normed_one, preferred_element_type=jnp.float32)
    d_normed_one = mp_allreduce(
        jnp.einsum("stc,sdc->td", stacked, w_qkv, preferred_element_type=jnp.float32).astype(
            jnp.bfloat16
        ),
        n_mp,
    )
    d_input_norm, grad_ln1_gain, grad_ln1_bias = norm_one_back(d_normed_one)
    grad_tokens = d_middle + d_input_norm

    def scatter(grad, dim):
        return lax.psum_scatter(grad.astype(jnp.bfloat16), "dp", scatter_dimension=dim, tiled=True).astype(jnp.float32)

    tail_grads = jnp.concatenate(
        [grad_w_qkv_t.reshape(3 * local_cols, -1), grad_w_out], axis=0
    )
    summed_tail = scatter(tail_grads, 1)
    share = summed_tail.shape[1]
    summed_qkv = summed_tail[: 3 * local_cols].reshape(3, local_cols, share).transpose(0, 2, 1)
    summed_out = summed_tail[3 * local_cols :]
    summed_mlp = summed_mlp.astype(jnp.float32)
    units = grad_w_fc2.shape[0]
    summed_fc2 = summed_mlp[:units]
    summed_fc1 = summed_mlp[units:].T
    early = dp_allreduce(
        jnp.concatenate([grad_ln2_gain, grad_ln2_bias, grad_b_out, grad_b_fc2, grad_b_fc1]), n_dp
    )
    late = dp_allreduce(jnp.concatenate([grad_ln1_gain, grad_ln1_bias, grad_b_qv.reshape(-1)]), n_dp)
    width = grad_ln1_gain.shape[0]
    pieces = [late[0:width], late[width : 2 * width]] + [
        early[k * width : (k + 1) * width] for k in range(4)
    ]
    summed_b_qv = late[2 * width :].reshape(grad_b_qv.shape)
    summed_b_fc1 = early[4 * width :]
    return (
        output,
        grad_tokens,
        summed_qkv,
        summed_b_qv,
        summed_out,
        pieces[4],
        summed_fc1,
        summed_b_fc1,
        summed_fc2,
        pieces[5],
        pieces[0],
        pieces[1],
        pieces[2],
        pieces[3],
    )


def solution(mesh):
    in_specs = (
        P("dp", None),
        P("dp", None),
        P("dp", None),
        P(None, None, "mp"),
        P(None, "mp"),
        P("mp", None),
        P(),
        P(None, "mp"),
        P("mp"),
        P("mp", None),
        P(),
        P(),
        P(),
        P(),
        P(),
    )
    out_specs = (
        P("dp", None),
        P("dp", None),
        P(None, "dp", "mp"),
        P(None, "mp"),
        P("mp", "dp"),
        P(),
        P("dp", "mp"),
        P("mp"),
        P("mp", "dp"),
        P(),
        P(),
        P(),
        P(),
        P(),
    )

    def body(*args):
        return per_device(mesh.shape["mp"], mesh.shape["dp"], *args)

    return jax.shard_map(
        body, mesh=mesh, in_specs=in_specs, out_specs=out_specs, check_vma=False
    )
```

```python
import jax
import jax.numpy as jnp
from jax import lax
from jax.experimental import pallas as pl
from jax.experimental.pallas import tpu as pltpu
from jax.sharding import PartitionSpec as P


HEAD = 64
TQ = 256
TK = 256
NEG = -1e30


HPS = 4


def _fwd_kernel(lo_ref, hi_ref, segc_ref, segr_ref, qt_ref, k_ref, vt_ref, ot_ref, o32t_ref, lse_ref):
    rows = qt_ref.shape[2]
    scale = HEAD ** (-0.5)

    def q_body(i, carry):
        r0 = pl.multiple_of(i * TQ, TQ)
        qts = [qt_ref[hh, :, pl.ds(r0, TQ)] for hh in range(HPS)]
        sq = segr_ref[:, pl.ds(r0, TQ)]

        def kv_body(j, state):
            c0 = pl.multiple_of(j * TK, TK)
            same = segc_ref[pl.ds(c0, TK), :] == sq
            new_state = []
            for hh in range(HPS):
                m, l, acc = state[hh]
                s = jnp.dot(k_ref[hh, pl.ds(c0, TK), :], qts[hh], preferred_element_type=jnp.float32) * scale
                s = jnp.where(same, s, NEG)
                m_new = jnp.maximum(m, jnp.max(s, axis=0, keepdims=True))
                p = jnp.exp(s - m_new)
                alpha = jnp.exp(m - m_new)
                l = alpha * l + jnp.sum(p, axis=0, keepdims=True)
                pv = jnp.dot(vt_ref[hh, :, pl.ds(c0, TK)], p.astype(jnp.bfloat16),
                             preferred_element_type=jnp.float32)
                new_state.append((m_new, l, alpha * acc + pv))
            return tuple(new_state)

        init = tuple(
            (jnp.full((1, TQ), NEG, jnp.float32), jnp.zeros((1, TQ), jnp.float32),
             jnp.zeros((HEAD, TQ), jnp.float32))
            for _ in range(HPS)
        )
        final = lax.fori_loop(lo_ref[i], hi_ref[i], kv_body, init)
        for hh in range(HPS):
            m, l, acc = final[hh]
            out = acc / l
            ot_ref[hh, :, pl.ds(r0, TQ)] = out.astype(ot_ref.dtype)
            o32t_ref[hh, :, pl.ds(r0, TQ)] = out
            lse_ref[hh, :, pl.ds(r0, TQ)] = m + jnp.log(l)
        return carry

    lax.fori_loop(0, rows // TQ, q_body, 0)


def _bwd_kernel(lo_ref, hi_ref, segc_ref, segr_ref, q_ref, qt_ref, k_ref, kt_ref, v_ref, do_ref, dot_ref,
                o32t_ref, lse_ref, dqt_ref, dk_ref, dv_ref, dvec_ref):
    rows = q_ref.shape[1]
    scale = HEAD ** (-0.5)
    dqt_ref[...] = jnp.zeros_like(dqt_ref)

    def d_body(i, carry):
        r0 = pl.multiple_of(i * TQ, TQ)
        for hh in range(HPS):
            prod = dot_ref[hh, :, pl.ds(r0, TQ)].astype(jnp.float32) * o32t_ref[hh, :, pl.ds(r0, TQ)]
            dvec_ref[hh, :, pl.ds(r0, TQ)] = jnp.sum(prod, axis=0, keepdims=True)
        return carry

    lax.fori_loop(0, rows // TQ, d_body, 0)

    def kv_body(j, carry):
        c0 = pl.multiple_of(j * TK, TK)
        ks = [k_ref[hh, pl.ds(c0, TK), :] for hh in range(HPS)]
        vs = [v_ref[hh, pl.ds(c0, TK), :] for hh in range(HPS)]
        kts = [kt_ref[hh, :, pl.ds(c0, TK)] for hh in range(HPS)]
        sk = segc_ref[pl.ds(c0, TK), :]

        def q_body(i, grads):
            r0 = pl.multiple_of(i * TQ, TQ)
            same = sk == segr_ref[:, pl.ds(r0, TQ)]
            new_grads = []
            for hh in range(HPS):
                dk, dv = grads[hh]
                s = jnp.dot(ks[hh], qt_ref[hh, :, pl.ds(r0, TQ)], preferred_element_type=jnp.float32) * scale
                s = jnp.where(same, s, NEG)
                p = jnp.exp(s - lse_ref[hh, :, pl.ds(r0, TQ)])
                dp = jnp.dot(vs[hh], dot_ref[hh, :, pl.ds(r0, TQ)], preferred_element_type=jnp.float32)
                ds = (p * (dp - dvec_ref[hh, :, pl.ds(r0, TQ)])).astype(jnp.bfloat16)
                dv = dv + jnp.dot(p.astype(jnp.bfloat16), do_ref[hh, pl.ds(r0, TQ), :],
                                  preferred_element_type=jnp.float32)
                dk = dk + jnp.dot(ds, q_ref[hh, pl.ds(r0, TQ), :], preferred_element_type=jnp.float32)
                dqt_ref[hh, :, pl.ds(r0, TQ)] += jnp.dot(kts[hh], ds, preferred_element_type=jnp.float32)
                new_grads.append((dk, dv))
            return tuple(new_grads)

        zeros = jnp.zeros((TK, HEAD), jnp.float32)
        final = lax.fori_loop(lo_ref[j], hi_ref[j], q_body, tuple((zeros, zeros) for _ in range(HPS)))
        for hh in range(HPS):
            dk, dv = final[hh]
            dk_ref[hh, pl.ds(c0, TK), :] = dk * scale
            dv_ref[hh, pl.ds(c0, TK), :] = dv
        return carry

    lax.fori_loop(0, rows // TK, kv_body, 0)
    dqt_ref[...] = dqt_ref[...] * scale


def block_ranges(segments, item_lengths_row):
    rows = segments.shape[0]
    ends = jnp.cumsum(item_lengths_row.astype(jnp.int32))
    starts = ends - item_lengths_row.astype(jnp.int32)
    first = segments[0::TQ]
    last = segments[TQ - 1::TQ]
    n_items = item_lengths_row.shape[0]
    key_lo = jnp.take(starts, jnp.clip(first, 0, n_items - 1))
    key_hi = jnp.take(ends, jnp.clip(last, 0, n_items - 1))
    lo = jnp.clip(key_lo // TK, 0, rows // TK)
    hi = jnp.clip((key_hi + TK - 1) // TK, 0, rows // TK)
    return lo.astype(jnp.int32), hi.astype(jnp.int32)


def _head_specs(rows):
    plain = pl.BlockSpec((HPS, rows, HEAD), lambda h, lo, hi: (h, 0, 0))
    flipped = pl.BlockSpec((HPS, HEAD, rows), lambda h, lo, hi: (h, 0, 0))
    stat = pl.BlockSpec((HPS, 1, rows), lambda h, lo, hi: (h, 0, 0))
    col = pl.BlockSpec((rows, 1), lambda h, lo, hi: (0, 0))
    row = pl.BlockSpec((1, rows), lambda h, lo, hi: (0, 0))
    return plain, flipped, stat, col, row


def flash_forward(qt, k, vt, seg_q, seg_k, lo, hi):
    heads, _, rows_q = qt.shape
    rows_k = k.shape[1]
    flipped_q = pl.BlockSpec((HPS, HEAD, rows_q), lambda h, lo, hi: (h, 0, 0))
    flipped_k = pl.BlockSpec((HPS, HEAD, rows_k), lambda h, lo, hi: (h, 0, 0))
    plain_k = pl.BlockSpec((HPS, rows_k, HEAD), lambda h, lo, hi: (h, 0, 0))
    stat = pl.BlockSpec((HPS, 1, rows_q), lambda h, lo, hi: (h, 0, 0))
    col = pl.BlockSpec((rows_k, 1), lambda h, lo, hi: (0, 0))
    row = pl.BlockSpec((1, rows_q), lambda h, lo, hi: (0, 0))
    flops = int(heads * rows_q * rows_k * HEAD * 2 * 2 * 0.6)
    return pl.pallas_call(
        _fwd_kernel,
        out_shape=(
            jax.ShapeDtypeStruct((heads, HEAD, rows_q), jnp.bfloat16),
            jax.ShapeDtypeStruct((heads, HEAD, rows_q), jnp.float32),
            jax.ShapeDtypeStruct((heads, 1, rows_q), jnp.float32),
        ),
        grid_spec=pltpu.PrefetchScalarGridSpec(
            num_scalar_prefetch=2,
            grid=(heads // HPS,),
            in_specs=[col, row, flipped_q, plain_k, flipped_k],
            out_specs=[flipped_q, flipped_q, stat],
        ),
        compiler_params=pltpu.CompilerParams(
            dimension_semantics=("arbitrary",), vmem_limit_bytes=48 * 1024 * 1024),
        cost_estimate=pl.CostEstimate(
            flops=flops, transcendentals=int(heads * rows_q * rows_k * 0.6),
            bytes_accessed=int(heads * HEAD * (rows_q * 8 + rows_k * 4))),
        name="segment_flash_fwd",
    )(lo, hi, seg_k.reshape(rows_k, 1), seg_q.reshape(1, rows_q), qt, k, vt)


def flash_backward(q, k, v, do, o32t, lse, segments, lo, hi):
    heads, rows, _ = q.shape
    plain, flipped, stat, col, row = _head_specs(rows)
    flops = int(heads * rows * rows * HEAD * 2 * 4 * 0.6)
    return pl.pallas_call(
        _bwd_kernel,
        out_shape=(
            jax.ShapeDtypeStruct((heads, HEAD, rows), jnp.float32),
            jax.ShapeDtypeStruct((heads, rows, HEAD), jnp.float32),
            jax.ShapeDtypeStruct((heads, rows, HEAD), jnp.float32),
        ),
        grid_spec=pltpu.PrefetchScalarGridSpec(
            num_scalar_prefetch=2,
            grid=(heads // HPS,),
            in_specs=[col, row, plain, flipped, plain, flipped, plain, plain, flipped, flipped, stat],
            out_specs=[flipped, plain, plain],
            scratch_shapes=[pltpu.VMEM((HPS, 1, rows), jnp.float32)],
        ),
        compiler_params=pltpu.CompilerParams(
            dimension_semantics=("arbitrary",), vmem_limit_bytes=48 * 1024 * 1024),
        cost_estimate=pl.CostEstimate(
            flops=flops, transcendentals=int(heads * rows * rows * 0.6),
            bytes_accessed=int(heads * rows * HEAD * (2 * 7 + 4 * 4) + heads * rows * 4)),
        name="segment_flash_bwd",
    )(lo, hi, segments.reshape(rows, 1), segments.reshape(1, rows),
      q, q.transpose(0, 2, 1), k, k.transpose(0, 2, 1), v, do, do.transpose(0, 2, 1), o32t, lse)


def normalize(values, gain, shift):
    center = jnp.mean(values, axis=-1, keepdims=True)
    centered = values - center
    spread = jnp.mean(centered * centered, axis=-1, keepdims=True)
    return centered * lax.rsqrt(spread + 1e-06) * gain + shift


def exact_gelu(values):
    return jax.nn.gelu(values, approximate=False)


def segment_ids(lengths_row, row_count):
    ends = jnp.cumsum(lengths_row)
    positions = jnp.arange(row_count, dtype=jnp.int32)
    return jnp.sum((positions[:, None] >= ends[None, :]).astype(jnp.int32), axis=1)


def mp_allreduce(partial, n_mp):
    if n_mp != 4:
        return lax.psum(partial, "mp").astype(jnp.float32)
    idx = lax.axis_index("mp")
    low_bit = idx % 2
    half = partial.shape[0] // 2
    mine = lax.dynamic_slice_in_dim(partial, low_bit * half, half, 0)
    other = lax.dynamic_slice_in_dim(partial, (1 - low_bit) * half, half, 0)
    got = lax.ppermute(other, "mp", [(k, k ^ 1) for k in range(4)])
    first = (mine.astype(jnp.float32) + got.astype(jnp.float32)).astype(jnp.bfloat16)
    got_far = lax.ppermute(first, "mp", [(k, k ^ 2) for k in range(4)])
    second = (first.astype(jnp.float32) + got_far.astype(jnp.float32)).astype(jnp.bfloat16)
    got_back = lax.ppermute(second, "mp", [(k, k ^ 1) for k in range(4)])
    top = jnp.where(low_bit == 0, second, got_back)
    bottom = jnp.where(low_bit == 0, got_back, second)
    return jnp.concatenate([top, bottom], axis=0).astype(jnp.float32)


def dp_allreduce(values, n_dp):
    if n_dp & (n_dp - 1):
        return lax.psum(values, "dp")
    total = values
    step = 1
    while step < n_dp:
        total = total + lax.ppermute(total, "dp", [(k, k ^ step) for k in range(n_dp)])
        step *= 2
    return total


def per_device(n_mp, n_dp,
    tokens,
    cotangent,
    item_lengths,
    w_qkv,
    b_qv,
    w_out,
    b_out,
    w_fc1,
    b_fc1,
    w_fc2,
    b_fc2,
    ln1_gain,
    ln1_bias,
    ln2_gain,
    ln2_bias,
):
    row_count = tokens.shape[0]
    local_cols = w_qkv.shape[2]
    heads_here = local_cols // HEAD
    segments = segment_ids(item_lengths[0], row_count)
    inputs = tokens.astype(jnp.float32)
    norm_one = normalize(inputs, ln1_gain, ln1_bias)
    normed_one = norm_one.astype(jnp.bfloat16)
    queries = (jnp.dot(normed_one, w_qkv[0], preferred_element_type=jnp.float32) + b_qv[0]).astype(
        jnp.bfloat16
    )
    key_rows = jnp.dot(normed_one, w_qkv[1], preferred_element_type=jnp.float32).astype(
        jnp.bfloat16
    )
    value_rows = (
        jnp.dot(normed_one, w_qkv[2], preferred_element_type=jnp.float32) + b_qv[1]
    ).astype(jnp.bfloat16)

    def to_heads(values):
        return values.reshape(values.shape[0], heads_here, HEAD).transpose(1, 0, 2)

    def from_heads(values):
        return values.transpose(1, 0, 2).reshape(row_count, local_cols)

    lo_blocks, hi_blocks = block_ranges(segments, item_lengths[0])
    query_heads = to_heads(queries)
    key_heads = to_heads(key_rows)
    value_heads = to_heads(value_rows)
    query_t = queries.reshape(row_count, heads_here, HEAD).transpose(1, 2, 0)
    value_t = value_rows.reshape(row_count, heads_here, HEAD).transpose(1, 2, 0)
    upstream = cotangent.astype(jnp.float32)
    q_blocks = row_count // TQ
    first_blocks = (q_blocks * 3) // 8
    bounds = [(0, first_blocks), (first_blocks, q_blocks)]
    pieces_fwd = []
    for b0, b1 in bounds:
        rows = slice(b0 * TQ, b1 * TQ)
        out_t, out32_t, lse_h = flash_forward(
            query_t[:, :, rows], key_heads, value_t, segments[rows], segments,
            lo_blocks[b0:b1], hi_blocks[b0:b1],
        )
        attended_h = out_t.transpose(2, 0, 1).reshape((b1 - b0) * TQ, local_cols)
        att_sum_h = mp_allreduce(
            jnp.dot(attended_h, w_out, preferred_element_type=jnp.float32).astype(jnp.bfloat16), n_mp
        )
        middle_h = inputs[rows] + att_sum_h + b_out
        norm_two_h, back_two_h = jax.vjp(normalize, middle_h, ln2_gain, ln2_bias)
        normed_two_h = norm_two_h.astype(jnp.bfloat16)
        hidden_pre_h = jnp.dot(normed_two_h, w_fc1, preferred_element_type=jnp.float32) + b_fc1
        act_h, gelu_back_h = jax.vjp(exact_gelu, hidden_pre_h)
        activated_h = act_h.astype(jnp.bfloat16)
        mlp_partial_h = jnp.dot(
            activated_h, w_fc2, preferred_element_type=jnp.float32
        ).astype(jnp.bfloat16)
        pieces_fwd.append(dict(
            rows=rows, out32_t=out32_t, lse=lse_h, attended=attended_h, middle=middle_h,
            back_two=back_two_h, normed_two=normed_two_h, gelu_back=gelu_back_h,
            activated=activated_h, mlp_partial=mlp_partial_h,
        ))
    grad_b_fc2 = jnp.sum(upstream, axis=0)
    for piece in pieces_fwd:
        d_act_h = jnp.einsum(
            "td,fd->tf", cotangent[piece["rows"]], w_fc2, preferred_element_type=jnp.float32
        )
        d_pre_h = piece["gelu_back"](d_act_h)[0]
        piece["b_fc1"] = jnp.sum(d_pre_h, axis=0)
        piece["d_pre_low"] = d_pre_h.astype(jnp.bfloat16)
        piece["dn_two_partial"] = jnp.einsum(
            "tf,df->td", piece["d_pre_low"], w_fc1, preferred_element_type=jnp.float32
        ).astype(jnp.bfloat16)
    activated = jnp.concatenate([p["activated"] for p in pieces_fwd], axis=0)
    normed_two = jnp.concatenate([p["normed_two"] for p in pieces_fwd], axis=0)
    d_pre_low = jnp.concatenate([p["d_pre_low"] for p in pieces_fwd], axis=0)
    grad_b_fc1 = sum(p["b_fc1"] for p in pieces_fwd)
    grad_w_fc2 = jnp.einsum("tf,td->fd", activated, cotangent, preferred_element_type=jnp.float32)
    grad_w_fc1_t = jnp.einsum(
        "tf,td->fd", d_pre_low, normed_two, preferred_element_type=jnp.float32
    )
    mlp_weight_grads = jnp.concatenate([grad_w_fc2, grad_w_fc1_t], axis=0).astype(jnp.bfloat16)
    summed_mlp = lax.psum_scatter(mlp_weight_grads, "dp", scatter_dimension=1, tiled=True)
    for piece in pieces_fwd:
        d_normed_two_h = mp_allreduce(piece["dn_two_partial"], n_mp)
        d_mid_norm_h, gain_h, shift_h = piece["back_two"](d_normed_two_h)
        piece["ln2_gain"] = gain_h
        piece["ln2_bias"] = shift_h
        piece["d_middle"] = upstream[piece["rows"]] + d_mid_norm_h
        d_middle_low_h = piece["d_middle"].astype(jnp.bfloat16)
        piece["d_middle_low"] = d_middle_low_h
        piece["d_attended"] = jnp.einsum(
            "td,cd->tc", d_middle_low_h, w_out, preferred_element_type=jnp.float32
        ).astype(jnp.bfloat16)
    grad_ln2_gain = sum(p["ln2_gain"] for p in pieces_fwd)
    grad_ln2_bias = sum(p["ln2_bias"] for p in pieces_fwd)
    d_middle = jnp.concatenate([p["d_middle"] for p in pieces_fwd], axis=0)
    grad_b_out = jnp.sum(d_middle, axis=0)
    d_middle_low = jnp.concatenate([p["d_middle_low"] for p in pieces_fwd], axis=0)
    attended = jnp.concatenate([p["attended"] for p in pieces_fwd], axis=0)
    grad_w_out = jnp.einsum("tc,td->cd", attended, d_middle_low, preferred_element_type=jnp.float32)
    d_attended = jnp.concatenate([p["d_attended"] for p in pieces_fwd], axis=0)
    out_f32 = jnp.concatenate([p["out32_t"] for p in pieces_fwd], axis=2)
    log_norms = jnp.concatenate([p["lse"] for p in pieces_fwd], axis=2)
    d_att_heads = to_heads(d_attended)
    partials = lax.optimization_barrier(tuple(p["mlp_partial"] for p in pieces_fwd) + (d_att_heads,))
    d_att_heads = partials[-1]
    outputs = []
    for h, piece in enumerate(pieces_fwd):
        mlp_sum_h = mp_allreduce(partials[h], n_mp)
        outputs.append((piece["middle"] + mlp_sum_h + b_fc2).astype(jnp.bfloat16))
    output = jnp.concatenate(outputs, axis=0)
    d_q_heads, d_k_heads, d_v_heads = flash_backward(
        query_heads, key_heads, value_heads, d_att_heads, out_f32, log_norms,
        segments, lo_blocks, hi_blocks,
    )
    summed_mlp, d_q_heads = lax.optimization_barrier((summed_mlp, d_q_heads))
    d_queries = d_q_heads.transpose(2, 0, 1).reshape(row_count, local_cols)
    d_keys = from_heads(d_k_heads)
    d_values = from_heads(d_v_heads)
    grad_b_qv = jnp.stack([jnp.sum(d_queries, axis=0), jnp.sum(d_values, axis=0)])
    stacked = jnp.stack([d_queries, d_keys, d_values]).astype(jnp.bfloat16)
    tail_parts = []
    for b0, b1 in bounds:
        rows = slice(b0 * TQ, b1 * TQ)
        dn_one_partial_h = jnp.einsum(
            "stc,sdc->td", stacked[:, rows], w_qkv, preferred_element_type=jnp.float32
        ).astype(jnp.bfloat16)
        tail_parts.append((rows, dn_one_partial_h))
    grad_w_qkv_t = jnp.einsum(
        "stc,td->scd", stacked, normed_one, preferred_element_type=jnp.float32
    )
    grad_pieces = []
    grad_ln1_gain = 0.0
    grad_ln1_bias = 0.0
    for rows, dn_one_partial_h in tail_parts:
        d_normed_one_h = mp_allreduce(dn_one_partial_h, n_mp)
        _, back_one_h = jax.vjp(normalize, inputs[rows], ln1_gain, ln1_bias)
        d_input_h, gain_h, shift_h = back_one_h(d_normed_one_h)
        grad_ln1_gain = grad_ln1_gain + gain_h
        grad_ln1_bias = grad_ln1_bias + shift_h
        grad_pieces.append(d_middle[rows] + d_input_h)
    grad_tokens = jnp.concatenate(grad_pieces, axis=0)

    def scatter(grad, dim):
        return lax.psum_scatter(grad.astype(jnp.bfloat16), "dp", scatter_dimension=dim, tiled=True).astype(jnp.float32)

    tail_grads = jnp.concatenate(
        [grad_w_qkv_t.reshape(3 * local_cols, -1), grad_w_out], axis=0
    )
    summed_tail = scatter(tail_grads, 1)
    share = summed_tail.shape[1]
    summed_qkv = summed_tail[: 3 * local_cols].reshape(3, local_cols, share).transpose(0, 2, 1)
    summed_out = summed_tail[3 * local_cols :]
    summed_mlp = summed_mlp.astype(jnp.float32)
    units = grad_w_fc2.shape[0]
    summed_fc2 = summed_mlp[:units]
    summed_fc1 = summed_mlp[units:].T
    early = dp_allreduce(
        jnp.concatenate([grad_ln2_gain, grad_ln2_bias, grad_b_out, grad_b_fc2, grad_b_fc1]), n_dp
    )
    late = dp_allreduce(jnp.concatenate([grad_ln1_gain, grad_ln1_bias, grad_b_qv.reshape(-1)]), n_dp)
    width = grad_ln1_gain.shape[0]
    pieces = [late[0:width], late[width : 2 * width]] + [
        early[k * width : (k + 1) * width] for k in range(4)
    ]
    summed_b_qv = late[2 * width :].reshape(grad_b_qv.shape)
    summed_b_fc1 = early[4 * width :]
    return (
        output,
        grad_tokens,
        summed_qkv,
        summed_b_qv,
        summed_out,
        pieces[4],
        summed_fc1,
        summed_b_fc1,
        summed_fc2,
        pieces[5],
        pieces[0],
        pieces[1],
        pieces[2],
        pieces[3],
    )


def solution(mesh):
    in_specs = (
        P("dp", None),
        P("dp", None),
        P("dp", None),
        P(None, None, "mp"),
        P(None, "mp"),
        P("mp", None),
        P(),
        P(None, "mp"),
        P("mp"),
        P("mp", None),
        P(),
        P(),
        P(),
        P(),
        P(),
    )
    out_specs = (
        P("dp", None),
        P("dp", None),
        P(None, "dp", "mp"),
        P(None, "mp"),
        P("mp", "dp"),
        P(),
        P("dp", "mp"),
        P("mp"),
        P("mp", "dp"),
        P(),
        P(),
        P(),
        P(),
        P(),
    )

    def body(*args):
        return per_device(mesh.shape["mp"], mesh.shape["dp"], *args)

    return jax.shard_map(
        body, mesh=mesh, in_specs=in_specs, out_specs=out_specs, check_vma=False
    )
```

```python
import jax
import jax.numpy as jnp
from jax import lax
from jax.experimental import pallas as pl
from jax.experimental.pallas import tpu as pltpu
from jax.sharding import PartitionSpec as P


HEAD = 64
TQ = 256
TK = 256
NEG = -1e30


HPS = 4


def _fwd_kernel(lo_ref, hi_ref, segc_ref, segr_ref, qt_ref, k_ref, vt_ref, ot_ref, o32t_ref, lse_ref):
    rows = qt_ref.shape[2]
    scale = HEAD ** (-0.5)

    def q_body(i, carry):
        r0 = pl.multiple_of(i * TQ, TQ)
        qts = [qt_ref[hh, :, pl.ds(r0, TQ)] for hh in range(HPS)]
        sq = segr_ref[:, pl.ds(r0, TQ)]

        def kv_body(j, state):
            c0 = pl.multiple_of(j * TK, TK)
            same = segc_ref[pl.ds(c0, TK), :] == sq
            new_state = []
            for hh in range(HPS):
                m, l, acc = state[hh]
                s = jnp.dot(k_ref[hh, pl.ds(c0, TK), :], qts[hh], preferred_element_type=jnp.float32) * scale
                s = jnp.where(same, s, NEG)
                m_new = jnp.maximum(m, jnp.max(s, axis=0, keepdims=True))
                p = jnp.exp(s - m_new)
                alpha = jnp.exp(m - m_new)
                l = alpha * l + jnp.sum(p, axis=0, keepdims=True)
                pv = jnp.dot(vt_ref[hh, :, pl.ds(c0, TK)], p.astype(jnp.bfloat16),
                             preferred_element_type=jnp.float32)
                new_state.append((m_new, l, alpha * acc + pv))
            return tuple(new_state)

        init = tuple(
            (jnp.full((1, TQ), NEG, jnp.float32), jnp.zeros((1, TQ), jnp.float32),
             jnp.zeros((HEAD, TQ), jnp.float32))
            for _ in range(HPS)
        )
        final = lax.fori_loop(lo_ref[i], hi_ref[i], kv_body, init)
        for hh in range(HPS):
            m, l, acc = final[hh]
            out = acc / l
            ot_ref[hh, :, pl.ds(r0, TQ)] = out.astype(ot_ref.dtype)
            o32t_ref[hh, :, pl.ds(r0, TQ)] = out
            lse_ref[hh, :, pl.ds(r0, TQ)] = m + jnp.log(l)
        return carry

    lax.fori_loop(0, rows // TQ, q_body, 0)


def _bwd_kernel(lo_ref, hi_ref, segc_ref, segr_ref, q_ref, qt_ref, k_ref, kt_ref, v_ref, do_ref, dot_ref,
                o32t_ref, lse_ref, dqt_ref, dk_ref, dv_ref, dvec_ref):
    rows = q_ref.shape[1]
    scale = HEAD ** (-0.5)
    dqt_ref[...] = jnp.zeros_like(dqt_ref)

    def d_body(i, carry):
        r0 = pl.multiple_of(i * TQ, TQ)
        for hh in range(HPS):
            prod = dot_ref[hh, :, pl.ds(r0, TQ)].astype(jnp.float32) * o32t_ref[hh, :, pl.ds(r0, TQ)]
            dvec_ref[hh, :, pl.ds(r0, TQ)] = jnp.sum(prod, axis=0, keepdims=True)
        return carry

    lax.fori_loop(0, rows // TQ, d_body, 0)

    def kv_body(j, carry):
        c0 = pl.multiple_of(j * TK, TK)
        ks = [k_ref[hh, pl.ds(c0, TK), :] for hh in range(HPS)]
        vs = [v_ref[hh, pl.ds(c0, TK), :] for hh in range(HPS)]
        kts = [kt_ref[hh, :, pl.ds(c0, TK)] for hh in range(HPS)]
        sk = segc_ref[pl.ds(c0, TK), :]

        def q_body(i, grads):
            r0 = pl.multiple_of(i * TQ, TQ)
            same = sk == segr_ref[:, pl.ds(r0, TQ)]
            new_grads = []
            for hh in range(HPS):
                dk, dv = grads[hh]
                s = jnp.dot(ks[hh], qt_ref[hh, :, pl.ds(r0, TQ)], preferred_element_type=jnp.float32) * scale
                s = jnp.where(same, s, NEG)
                p = jnp.exp(s - lse_ref[hh, :, pl.ds(r0, TQ)])
                dp = jnp.dot(vs[hh], dot_ref[hh, :, pl.ds(r0, TQ)], preferred_element_type=jnp.float32)
                ds = (p * (dp - dvec_ref[hh, :, pl.ds(r0, TQ)])).astype(jnp.bfloat16)
                dv = dv + jnp.dot(p.astype(jnp.bfloat16), do_ref[hh, pl.ds(r0, TQ), :],
                                  preferred_element_type=jnp.float32)
                dk = dk + jnp.dot(ds, q_ref[hh, pl.ds(r0, TQ), :], preferred_element_type=jnp.float32)
                dqt_ref[hh, :, pl.ds(r0, TQ)] += jnp.dot(kts[hh], ds, preferred_element_type=jnp.float32)
                new_grads.append((dk, dv))
            return tuple(new_grads)

        zeros = jnp.zeros((TK, HEAD), jnp.float32)
        final = lax.fori_loop(lo_ref[j], hi_ref[j], q_body, tuple((zeros, zeros) for _ in range(HPS)))
        for hh in range(HPS):
            dk, dv = final[hh]
            dk_ref[hh, pl.ds(c0, TK), :] = dk * scale
            dv_ref[hh, pl.ds(c0, TK), :] = dv
        return carry

    lax.fori_loop(0, rows // TK, kv_body, 0)
    dqt_ref[...] = dqt_ref[...] * scale


def block_ranges(segments, item_lengths_row):
    rows = segments.shape[0]
    ends = jnp.cumsum(item_lengths_row.astype(jnp.int32))
    starts = ends - item_lengths_row.astype(jnp.int32)
    first = segments[0::TQ]
    last = segments[TQ - 1::TQ]
    n_items = item_lengths_row.shape[0]
    key_lo = jnp.take(starts, jnp.clip(first, 0, n_items - 1))
    key_hi = jnp.take(ends, jnp.clip(last, 0, n_items - 1))
    lo = jnp.clip(key_lo // TK, 0, rows // TK)
    hi = jnp.clip((key_hi + TK - 1) // TK, 0, rows // TK)
    return lo.astype(jnp.int32), hi.astype(jnp.int32)


def _head_specs(rows):
    plain = pl.BlockSpec((HPS, rows, HEAD), lambda h, lo, hi: (h, 0, 0))
    flipped = pl.BlockSpec((HPS, HEAD, rows), lambda h, lo, hi: (h, 0, 0))
    stat = pl.BlockSpec((HPS, 1, rows), lambda h, lo, hi: (h, 0, 0))
    col = pl.BlockSpec((rows, 1), lambda h, lo, hi: (0, 0))
    row = pl.BlockSpec((1, rows), lambda h, lo, hi: (0, 0))
    return plain, flipped, stat, col, row


def flash_forward(qt, k, vt, seg_q, seg_k, lo, hi):
    heads, _, rows_q = qt.shape
    rows_k = k.shape[1]
    flipped_q = pl.BlockSpec((HPS, HEAD, rows_q), lambda h, lo, hi: (h, 0, 0))
    flipped_k = pl.BlockSpec((HPS, HEAD, rows_k), lambda h, lo, hi: (h, 0, 0))
    plain_k = pl.BlockSpec((HPS, rows_k, HEAD), lambda h, lo, hi: (h, 0, 0))
    stat = pl.BlockSpec((HPS, 1, rows_q), lambda h, lo, hi: (h, 0, 0))
    col = pl.BlockSpec((rows_k, 1), lambda h, lo, hi: (0, 0))
    row = pl.BlockSpec((1, rows_q), lambda h, lo, hi: (0, 0))
    flops = int(heads * rows_q * rows_k * HEAD * 2 * 2 * 0.6)
    return pl.pallas_call(
        _fwd_kernel,
        out_shape=(
            jax.ShapeDtypeStruct((heads, HEAD, rows_q), jnp.bfloat16),
            jax.ShapeDtypeStruct((heads, HEAD, rows_q), jnp.float32),
            jax.ShapeDtypeStruct((heads, 1, rows_q), jnp.float32),
        ),
        grid_spec=pltpu.PrefetchScalarGridSpec(
            num_scalar_prefetch=2,
            grid=(heads // HPS,),
            in_specs=[col, row, flipped_q, plain_k, flipped_k],
            out_specs=[flipped_q, flipped_q, stat],
        ),
        compiler_params=pltpu.CompilerParams(
            dimension_semantics=("arbitrary",), vmem_limit_bytes=48 * 1024 * 1024),
        cost_estimate=pl.CostEstimate(
            flops=flops, transcendentals=int(heads * rows_q * rows_k * 0.6),
            bytes_accessed=int(heads * HEAD * (rows_q * 8 + rows_k * 4))),
        name="segment_flash_fwd",
    )(lo, hi, seg_k.reshape(rows_k, 1), seg_q.reshape(1, rows_q), qt, k, vt)


def flash_backward(q, k, v, do, o32t, lse, segments, lo, hi):
    heads, rows, _ = q.shape
    plain, flipped, stat, col, row = _head_specs(rows)
    flops = int(heads * rows * rows * HEAD * 2 * 4 * 0.6)
    return pl.pallas_call(
        _bwd_kernel,
        out_shape=(
            jax.ShapeDtypeStruct((heads, HEAD, rows), jnp.float32),
            jax.ShapeDtypeStruct((heads, rows, HEAD), jnp.float32),
            jax.ShapeDtypeStruct((heads, rows, HEAD), jnp.float32),
        ),
        grid_spec=pltpu.PrefetchScalarGridSpec(
            num_scalar_prefetch=2,
            grid=(heads // HPS,),
            in_specs=[col, row, plain, flipped, plain, flipped, plain, plain, flipped, flipped, stat],
            out_specs=[flipped, plain, plain],
            scratch_shapes=[pltpu.VMEM((HPS, 1, rows), jnp.float32)],
        ),
        compiler_params=pltpu.CompilerParams(
            dimension_semantics=("arbitrary",), vmem_limit_bytes=48 * 1024 * 1024),
        cost_estimate=pl.CostEstimate(
            flops=flops, transcendentals=int(heads * rows * rows * 0.6),
            bytes_accessed=int(heads * rows * HEAD * (2 * 7 + 4 * 4) + heads * rows * 4)),
        name="segment_flash_bwd",
    )(lo, hi, segments.reshape(rows, 1), segments.reshape(1, rows),
      q, q.transpose(0, 2, 1), k, k.transpose(0, 2, 1), v, do, do.transpose(0, 2, 1), o32t, lse)


def normalize(values, gain, shift):
    center = jnp.mean(values, axis=-1, keepdims=True)
    centered = values - center
    spread = jnp.mean(centered * centered, axis=-1, keepdims=True)
    return centered * lax.rsqrt(spread + 1e-06) * gain + shift


def exact_gelu(values):
    return jax.nn.gelu(values, approximate=False)


def segment_ids(lengths_row, row_count):
    ends = jnp.cumsum(lengths_row)
    positions = jnp.arange(row_count, dtype=jnp.int32)
    return jnp.sum((positions[:, None] >= ends[None, :]).astype(jnp.int32), axis=1)


def mp_allreduce(partial, n_mp):
    if n_mp != 4:
        return lax.psum(partial, "mp").astype(jnp.float32)
    idx = lax.axis_index("mp")
    low_bit = idx % 2
    half = partial.shape[0] // 2
    mine = lax.dynamic_slice_in_dim(partial, low_bit * half, half, 0)
    other = lax.dynamic_slice_in_dim(partial, (1 - low_bit) * half, half, 0)
    got = lax.ppermute(other, "mp", [(k, k ^ 1) for k in range(4)])
    first = (mine.astype(jnp.float32) + got.astype(jnp.float32)).astype(jnp.bfloat16)
    got_far = lax.ppermute(first, "mp", [(k, k ^ 2) for k in range(4)])
    second = (first.astype(jnp.float32) + got_far.astype(jnp.float32)).astype(jnp.bfloat16)
    got_back = lax.ppermute(second, "mp", [(k, k ^ 1) for k in range(4)])
    top = jnp.where(low_bit == 0, second, got_back)
    bottom = jnp.where(low_bit == 0, got_back, second)
    return jnp.concatenate([top, bottom], axis=0).astype(jnp.float32)


def dp_allreduce(values, n_dp):
    if n_dp & (n_dp - 1):
        return lax.psum(values, "dp")
    total = values
    step = 1
    while step < n_dp:
        total = total + lax.ppermute(total, "dp", [(k, k ^ step) for k in range(n_dp)])
        step *= 2
    return total


def per_device(n_mp, n_dp,
    tokens,
    cotangent,
    item_lengths,
    w_qkv,
    b_qv,
    w_out,
    b_out,
    w_fc1,
    b_fc1,
    w_fc2,
    b_fc2,
    ln1_gain,
    ln1_bias,
    ln2_gain,
    ln2_bias,
):
    row_count = tokens.shape[0]
    local_cols = w_qkv.shape[2]
    heads_here = local_cols // HEAD
    segments = segment_ids(item_lengths[0], row_count)
    inputs = tokens.astype(jnp.float32)
    norm_one, norm_one_back = jax.vjp(normalize, inputs, ln1_gain, ln1_bias)
    normed_one = norm_one.astype(jnp.bfloat16)
    queries = (jnp.dot(normed_one, w_qkv[0], preferred_element_type=jnp.float32) + b_qv[0]).astype(
        jnp.bfloat16
    )
    key_rows = jnp.dot(normed_one, w_qkv[1], preferred_element_type=jnp.float32).astype(
        jnp.bfloat16
    )
    value_rows = (
        jnp.dot(normed_one, w_qkv[2], preferred_element_type=jnp.float32) + b_qv[1]
    ).astype(jnp.bfloat16)

    def to_heads(values):
        return values.reshape(values.shape[0], heads_here, HEAD).transpose(1, 0, 2)

    def from_heads(values):
        return values.transpose(1, 0, 2).reshape(row_count, local_cols)

    lo_blocks, hi_blocks = block_ranges(segments, item_lengths[0])
    query_heads = to_heads(queries)
    key_heads = to_heads(key_rows)
    value_heads = to_heads(value_rows)
    query_t = queries.reshape(row_count, heads_here, HEAD).transpose(1, 2, 0)
    value_t = value_rows.reshape(row_count, heads_here, HEAD).transpose(1, 2, 0)
    upstream = cotangent.astype(jnp.float32)
    q_blocks = row_count // TQ
    first_blocks = (q_blocks * 3) // 8
    bounds = [(0, first_blocks), (first_blocks, q_blocks)]
    pieces_fwd = []
    for b0, b1 in bounds:
        rows = slice(b0 * TQ, b1 * TQ)
        out_t, out32_t, lse_h = flash_forward(
            query_t[:, :, rows], key_heads, value_t, segments[rows], segments,
            lo_blocks[b0:b1], hi_blocks[b0:b1],
        )
        attended_h = out_t.transpose(2, 0, 1).reshape((b1 - b0) * TQ, local_cols)
        att_sum_h = mp_allreduce(
            jnp.dot(attended_h, w_out, preferred_element_type=jnp.float32).astype(jnp.bfloat16), n_mp
        )
        middle_h = inputs[rows] + att_sum_h + b_out
        norm_two_h, back_two_h = jax.vjp(normalize, middle_h, ln2_gain, ln2_bias)
        normed_two_h = norm_two_h.astype(jnp.bfloat16)
        hidden_pre_h = jnp.dot(normed_two_h, w_fc1, preferred_element_type=jnp.float32) + b_fc1
        act_h, gelu_back_h = jax.vjp(exact_gelu, hidden_pre_h)
        activated_h = act_h.astype(jnp.bfloat16)
        mlp_partial_h = jnp.dot(
            activated_h, w_fc2, preferred_element_type=jnp.float32
        ).astype(jnp.bfloat16)
        pieces_fwd.append(dict(
            rows=rows, out32_t=out32_t, lse=lse_h, attended=attended_h, middle=middle_h,
            back_two=back_two_h, normed_two=normed_two_h, gelu_back=gelu_back_h,
            activated=activated_h, mlp_partial=mlp_partial_h,
        ))
    grad_b_fc2 = jnp.sum(upstream, axis=0)
    for piece in pieces_fwd:
        d_act_h = jnp.einsum(
            "td,fd->tf", cotangent[piece["rows"]], w_fc2, preferred_element_type=jnp.float32
        )
        d_pre_h = piece["gelu_back"](d_act_h)[0]
        piece["b_fc1"] = jnp.sum(d_pre_h, axis=0)
        piece["d_pre_low"] = d_pre_h.astype(jnp.bfloat16)
        piece["dn_two_partial"] = jnp.einsum(
            "tf,df->td", piece["d_pre_low"], w_fc1, preferred_element_type=jnp.float32
        ).astype(jnp.bfloat16)
    activated = jnp.concatenate([p["activated"] for p in pieces_fwd], axis=0)
    normed_two = jnp.concatenate([p["normed_two"] for p in pieces_fwd], axis=0)
    d_pre_low = jnp.concatenate([p["d_pre_low"] for p in pieces_fwd], axis=0)
    grad_b_fc1 = sum(p["b_fc1"] for p in pieces_fwd)
    grad_w_fc2 = jnp.einsum("tf,td->fd", activated, cotangent, preferred_element_type=jnp.float32)
    grad_w_fc1_t = jnp.einsum(
        "tf,td->fd", d_pre_low, normed_two, preferred_element_type=jnp.float32
    )
    mlp_weight_grads = jnp.concatenate([grad_w_fc2, grad_w_fc1_t], axis=0).astype(jnp.bfloat16)
    summed_mlp = lax.psum_scatter(mlp_weight_grads, "dp", scatter_dimension=1, tiled=True)
    for piece in pieces_fwd:
        d_normed_two_h = mp_allreduce(piece["dn_two_partial"], n_mp)
        d_mid_norm_h, gain_h, shift_h = piece["back_two"](d_normed_two_h)
        piece["ln2_gain"] = gain_h
        piece["ln2_bias"] = shift_h
        piece["d_middle"] = upstream[piece["rows"]] + d_mid_norm_h
        d_middle_low_h = piece["d_middle"].astype(jnp.bfloat16)
        piece["d_middle_low"] = d_middle_low_h
        piece["d_attended"] = jnp.einsum(
            "td,cd->tc", d_middle_low_h, w_out, preferred_element_type=jnp.float32
        ).astype(jnp.bfloat16)
    grad_ln2_gain = sum(p["ln2_gain"] for p in pieces_fwd)
    grad_ln2_bias = sum(p["ln2_bias"] for p in pieces_fwd)
    d_middle = jnp.concatenate([p["d_middle"] for p in pieces_fwd], axis=0)
    grad_b_out = jnp.sum(d_middle, axis=0)
    d_middle_low = jnp.concatenate([p["d_middle_low"] for p in pieces_fwd], axis=0)
    attended = jnp.concatenate([p["attended"] for p in pieces_fwd], axis=0)
    grad_w_out = jnp.einsum("tc,td->cd", attended, d_middle_low, preferred_element_type=jnp.float32)
    d_attended = jnp.concatenate([p["d_attended"] for p in pieces_fwd], axis=0)
    out_f32 = jnp.concatenate([p["out32_t"] for p in pieces_fwd], axis=2)
    log_norms = jnp.concatenate([p["lse"] for p in pieces_fwd], axis=2)
    d_att_heads = to_heads(d_attended)
    partials = lax.optimization_barrier(tuple(p["mlp_partial"] for p in pieces_fwd) + (d_att_heads,))
    d_att_heads = partials[-1]
    outputs = []
    for h, piece in enumerate(pieces_fwd):
        mlp_sum_h = mp_allreduce(partials[h], n_mp)
        outputs.append((piece["middle"] + mlp_sum_h + b_fc2).astype(jnp.bfloat16))
    output = jnp.concatenate(outputs, axis=0)
    d_q_heads, d_k_heads, d_v_heads = flash_backward(
        query_heads, key_heads, value_heads, d_att_heads, out_f32, log_norms,
        segments, lo_blocks, hi_blocks,
    )
    summed_mlp, d_q_heads = lax.optimization_barrier((summed_mlp, d_q_heads))
    d_queries = d_q_heads.transpose(2, 0, 1).reshape(row_count, local_cols)
    d_keys = from_heads(d_k_heads)
    d_values = from_heads(d_v_heads)
    grad_b_qv = jnp.stack([jnp.sum(d_queries, axis=0), jnp.sum(d_values, axis=0)])
    stacked = jnp.stack([d_queries, d_keys, d_values]).astype(jnp.bfloat16)
    grad_w_qkv_t = jnp.einsum(
        "stc,td->scd", stacked, normed_one, preferred_element_type=jnp.float32
    )
    d_normed_one = mp_allreduce(
        jnp.einsum("stc,sdc->td", stacked, w_qkv, preferred_element_type=jnp.float32).astype(
            jnp.bfloat16
        ),
        n_mp,
    )
    d_input_norm, grad_ln1_gain, grad_ln1_bias = norm_one_back(d_normed_one)
    grad_tokens = d_middle + d_input_norm

    def scatter(grad, dim):
        return lax.psum_scatter(grad.astype(jnp.bfloat16), "dp", scatter_dimension=dim, tiled=True).astype(jnp.float32)

    tail_grads = jnp.concatenate(
        [grad_w_qkv_t.reshape(3 * local_cols, -1), grad_w_out], axis=0
    )
    summed_tail = scatter(tail_grads, 1)
    share = summed_tail.shape[1]
    summed_qkv = summed_tail[: 3 * local_cols].reshape(3, local_cols, share).transpose(0, 2, 1)
    summed_out = summed_tail[3 * local_cols :]
    summed_mlp = summed_mlp.astype(jnp.float32)
    units = grad_w_fc2.shape[0]
    summed_fc2 = summed_mlp[:units]
    summed_fc1 = summed_mlp[units:].T
    early = dp_allreduce(
        jnp.concatenate([grad_ln2_gain, grad_ln2_bias, grad_b_out, grad_b_fc2, grad_b_fc1]), n_dp
    )
    late = dp_allreduce(jnp.concatenate([grad_ln1_gain, grad_ln1_bias, grad_b_qv.reshape(-1)]), n_dp)
    width = grad_ln1_gain.shape[0]
    pieces = [late[0:width], late[width : 2 * width]] + [
        early[k * width : (k + 1) * width] for k in range(4)
    ]
    summed_b_qv = late[2 * width :].reshape(grad_b_qv.shape)
    summed_b_fc1 = early[4 * width :]
    return (
        output,
        grad_tokens,
        summed_qkv,
        summed_b_qv,
        summed_out,
        pieces[4],
        summed_fc1,
        summed_b_fc1,
        summed_fc2,
        pieces[5],
        pieces[0],
        pieces[1],
        pieces[2],
        pieces[3],
    )


def solution(mesh):
    in_specs = (
        P("dp", None),
        P("dp", None),
        P("dp", None),
        P(None, None, "mp"),
        P(None, "mp"),
        P("mp", None),
        P(),
        P(None, "mp"),
        P("mp"),
        P("mp", None),
        P(),
        P(),
        P(),
        P(),
        P(),
    )
    out_specs = (
        P("dp", None),
        P("dp", None),
        P(None, "dp", "mp"),
        P(None, "mp"),
        P("mp", "dp"),
        P(),
        P("dp", "mp"),
        P("mp"),
        P("mp", "dp"),
        P(),
        P(),
        P(),
        P(),
        P(),
    )

    def body(*args):
        return per_device(mesh.shape["mp"], mesh.shape["dp"], *args)

    return jax.shard_map(
        body, mesh=mesh, in_specs=in_specs, out_specs=out_specs, check_vma=False
    )
```

```python
import jax
import jax.numpy as jnp
from jax import lax
from jax.experimental import pallas as pl
from jax.experimental.pallas import tpu as pltpu
from jax.sharding import PartitionSpec as P


HEAD = 64
TQ = 256
TK = 256
NEG = -1e30


HPS = 4


def _fwd_kernel(lo_ref, hi_ref, segc_ref, segr_ref, qt_ref, k_ref, vt_ref, ot_ref, o32t_ref, lse_ref):
    rows = qt_ref.shape[2]
    scale = HEAD ** (-0.5)

    def q_body(i, carry):
        r0 = pl.multiple_of(i * TQ, TQ)
        qts = [qt_ref[hh, :, pl.ds(r0, TQ)] for hh in range(HPS)]
        sq = segr_ref[:, pl.ds(r0, TQ)]

        def kv_body(j, state):
            c0 = pl.multiple_of(j * TK, TK)
            same = segc_ref[pl.ds(c0, TK), :] == sq
            new_state = []
            for hh in range(HPS):
                m, l, acc = state[hh]
                s = jnp.dot(k_ref[hh, pl.ds(c0, TK), :], qts[hh], preferred_element_type=jnp.float32) * scale
                s = jnp.where(same, s, NEG)
                m_new = jnp.maximum(m, jnp.max(s, axis=0, keepdims=True))
                p = jnp.exp(s - m_new)
                alpha = jnp.exp(m - m_new)
                l = alpha * l + jnp.sum(p, axis=0, keepdims=True)
                pv = jnp.dot(vt_ref[hh, :, pl.ds(c0, TK)], p.astype(jnp.bfloat16),
                             preferred_element_type=jnp.float32)
                new_state.append((m_new, l, alpha * acc + pv))
            return tuple(new_state)

        init = tuple(
            (jnp.full((1, TQ), NEG, jnp.float32), jnp.zeros((1, TQ), jnp.float32),
             jnp.zeros((HEAD, TQ), jnp.float32))
            for _ in range(HPS)
        )
        final = lax.fori_loop(lo_ref[i], hi_ref[i], kv_body, init)
        for hh in range(HPS):
            m, l, acc = final[hh]
            out = acc / l
            ot_ref[hh, :, pl.ds(r0, TQ)] = out.astype(ot_ref.dtype)
            o32t_ref[hh, :, pl.ds(r0, TQ)] = out
            lse_ref[hh, :, pl.ds(r0, TQ)] = m + jnp.log(l)
        return carry

    lax.fori_loop(0, rows // TQ, q_body, 0)


def _bwd_kernel(lo_ref, hi_ref, segc_ref, segr_ref, q_ref, qt_ref, k_ref, kt_ref, v_ref, do_ref, dot_ref,
                o32t_ref, lse_ref, dqt_ref, dk_ref, dv_ref, dvec_ref):
    rows = q_ref.shape[1]
    scale = HEAD ** (-0.5)
    dqt_ref[...] = jnp.zeros_like(dqt_ref)

    def d_body(i, carry):
        r0 = pl.multiple_of(i * TQ, TQ)
        for hh in range(HPS):
            prod = dot_ref[hh, :, pl.ds(r0, TQ)].astype(jnp.float32) * o32t_ref[hh, :, pl.ds(r0, TQ)]
            dvec_ref[hh, :, pl.ds(r0, TQ)] = jnp.sum(prod, axis=0, keepdims=True)
        return carry

    lax.fori_loop(0, rows // TQ, d_body, 0)

    def kv_body(j, carry):
        c0 = pl.multiple_of(j * TK, TK)
        ks = [k_ref[hh, pl.ds(c0, TK), :] for hh in range(HPS)]
        vs = [v_ref[hh, pl.ds(c0, TK), :] for hh in range(HPS)]
        kts = [kt_ref[hh, :, pl.ds(c0, TK)] for hh in range(HPS)]
        sk = segc_ref[pl.ds(c0, TK), :]

        def q_body(i, grads):
            r0 = pl.multiple_of(i * TQ, TQ)
            same = sk == segr_ref[:, pl.ds(r0, TQ)]
            new_grads = []
            for hh in range(HPS):
                dk, dv = grads[hh]
                s = jnp.dot(ks[hh], qt_ref[hh, :, pl.ds(r0, TQ)], preferred_element_type=jnp.float32) * scale
                s = jnp.where(same, s, NEG)
                p = jnp.exp(s - lse_ref[hh, :, pl.ds(r0, TQ)])
                dp = jnp.dot(vs[hh], dot_ref[hh, :, pl.ds(r0, TQ)], preferred_element_type=jnp.float32)
                ds = (p * (dp - dvec_ref[hh, :, pl.ds(r0, TQ)])).astype(jnp.bfloat16)
                dv = dv + jnp.dot(p.astype(jnp.bfloat16), do_ref[hh, pl.ds(r0, TQ), :],
                                  preferred_element_type=jnp.float32)
                dk = dk + jnp.dot(ds, q_ref[hh, pl.ds(r0, TQ), :], preferred_element_type=jnp.float32)
                dqt_ref[hh, :, pl.ds(r0, TQ)] += jnp.dot(kts[hh], ds, preferred_element_type=jnp.float32)
                new_grads.append((dk, dv))
            return tuple(new_grads)

        zeros = jnp.zeros((TK, HEAD), jnp.float32)
        final = lax.fori_loop(lo_ref[j], hi_ref[j], q_body, tuple((zeros, zeros) for _ in range(HPS)))
        for hh in range(HPS):
            dk, dv = final[hh]
            dk_ref[pl.ds(c0, TK), pl.ds(hh * HEAD, HEAD)] = dk * scale
            dv_ref[pl.ds(c0, TK), pl.ds(hh * HEAD, HEAD)] = dv
        return carry

    lax.fori_loop(0, rows // TK, kv_body, 0)
    dqt_ref[...] = dqt_ref[...] * scale


def block_ranges(segments, item_lengths_row):
    rows = segments.shape[0]
    ends = jnp.cumsum(item_lengths_row.astype(jnp.int32))
    starts = ends - item_lengths_row.astype(jnp.int32)
    first = segments[0::TQ]
    last = segments[TQ - 1::TQ]
    n_items = item_lengths_row.shape[0]
    key_lo = jnp.take(starts, jnp.clip(first, 0, n_items - 1))
    key_hi = jnp.take(ends, jnp.clip(last, 0, n_items - 1))
    lo = jnp.clip(key_lo // TK, 0, rows // TK)
    hi = jnp.clip((key_hi + TK - 1) // TK, 0, rows // TK)
    return lo.astype(jnp.int32), hi.astype(jnp.int32)


def _head_specs(rows):
    plain = pl.BlockSpec((HPS, rows, HEAD), lambda h, lo, hi: (h, 0, 0))
    flipped = pl.BlockSpec((HPS, HEAD, rows), lambda h, lo, hi: (h, 0, 0))
    stat = pl.BlockSpec((HPS, 1, rows), lambda h, lo, hi: (h, 0, 0))
    col = pl.BlockSpec((rows, 1), lambda h, lo, hi: (0, 0))
    row = pl.BlockSpec((1, rows), lambda h, lo, hi: (0, 0))
    return plain, flipped, stat, col, row


def flash_forward(qt, k, vt, seg_q, seg_k, lo, hi):
    heads, _, rows_q = qt.shape
    rows_k = k.shape[1]
    flipped_q = pl.BlockSpec((HPS, HEAD, rows_q), lambda h, lo, hi: (h, 0, 0))
    flipped_k = pl.BlockSpec((HPS, HEAD, rows_k), lambda h, lo, hi: (h, 0, 0))
    plain_k = pl.BlockSpec((HPS, rows_k, HEAD), lambda h, lo, hi: (h, 0, 0))
    stat = pl.BlockSpec((HPS, 1, rows_q), lambda h, lo, hi: (h, 0, 0))
    col = pl.BlockSpec((rows_k, 1), lambda h, lo, hi: (0, 0))
    row = pl.BlockSpec((1, rows_q), lambda h, lo, hi: (0, 0))
    flops = int(heads * rows_q * rows_k * HEAD * 2 * 2 * 0.6)
    return pl.pallas_call(
        _fwd_kernel,
        out_shape=(
            jax.ShapeDtypeStruct((heads, HEAD, rows_q), jnp.bfloat16),
            jax.ShapeDtypeStruct((heads, HEAD, rows_q), jnp.float32),
            jax.ShapeDtypeStruct((heads, 1, rows_q), jnp.float32),
        ),
        grid_spec=pltpu.PrefetchScalarGridSpec(
            num_scalar_prefetch=2,
            grid=(heads // HPS,),
            in_specs=[col, row, flipped_q, plain_k, flipped_k],
            out_specs=[flipped_q, flipped_q, stat],
        ),
        compiler_params=pltpu.CompilerParams(
            dimension_semantics=("arbitrary",), vmem_limit_bytes=48 * 1024 * 1024),
        cost_estimate=pl.CostEstimate(
            flops=flops, transcendentals=int(heads * rows_q * rows_k * 0.6),
            bytes_accessed=int(heads * HEAD * (rows_q * 8 + rows_k * 4))),
        name="segment_flash_fwd",
    )(lo, hi, seg_k.reshape(rows_k, 1), seg_q.reshape(1, rows_q), qt, k, vt)


def flash_backward(q, k, v, do, o32t, lse, segments, lo, hi):
    heads, rows, _ = q.shape
    plain, flipped, stat, col, row = _head_specs(rows)
    wide = pl.BlockSpec((rows, HPS * HEAD), lambda h, lo, hi: (0, h))
    flops = int(heads * rows * rows * HEAD * 2 * 4 * 0.6)
    return pl.pallas_call(
        _bwd_kernel,
        out_shape=(
            jax.ShapeDtypeStruct((heads, HEAD, rows), jnp.float32),
            jax.ShapeDtypeStruct((rows, heads * HEAD), jnp.float32),
            jax.ShapeDtypeStruct((rows, heads * HEAD), jnp.float32),
        ),
        grid_spec=pltpu.PrefetchScalarGridSpec(
            num_scalar_prefetch=2,
            grid=(heads // HPS,),
            in_specs=[col, row, plain, flipped, plain, flipped, plain, plain, flipped, flipped, stat],
            out_specs=[flipped, wide, wide],
            scratch_shapes=[pltpu.VMEM((HPS, 1, rows), jnp.float32)],
        ),
        compiler_params=pltpu.CompilerParams(
            dimension_semantics=("arbitrary",), vmem_limit_bytes=48 * 1024 * 1024),
        cost_estimate=pl.CostEstimate(
            flops=flops, transcendentals=int(heads * rows * rows * 0.6),
            bytes_accessed=int(heads * rows * HEAD * (2 * 7 + 4 * 4) + heads * rows * 4)),
        name="segment_flash_bwd",
    )(lo, hi, segments.reshape(rows, 1), segments.reshape(1, rows),
      q, q.transpose(0, 2, 1), k, k.transpose(0, 2, 1), v, do, do.transpose(0, 2, 1), o32t, lse)


def normalize(values, gain, shift):
    center = jnp.mean(values, axis=-1, keepdims=True)
    centered = values - center
    spread = jnp.mean(centered * centered, axis=-1, keepdims=True)
    return centered * lax.rsqrt(spread + 1e-06) * gain + shift


def exact_gelu(values):
    return jax.nn.gelu(values, approximate=False)


def segment_ids(lengths_row, row_count):
    ends = jnp.cumsum(lengths_row)
    positions = jnp.arange(row_count, dtype=jnp.int32)
    return jnp.sum((positions[:, None] >= ends[None, :]).astype(jnp.int32), axis=1)


def mp_allreduce(partial, n_mp):
    if n_mp != 4:
        return lax.psum(partial, "mp").astype(jnp.float32)
    idx = lax.axis_index("mp")
    low_bit = idx % 2
    half = partial.shape[0] // 2
    mine = lax.dynamic_slice_in_dim(partial, low_bit * half, half, 0)
    other = lax.dynamic_slice_in_dim(partial, (1 - low_bit) * half, half, 0)
    got = lax.ppermute(other, "mp", [(k, k ^ 1) for k in range(4)])
    first = (mine.astype(jnp.float32) + got.astype(jnp.float32)).astype(jnp.bfloat16)
    got_far = lax.ppermute(first, "mp", [(k, k ^ 2) for k in range(4)])
    second = (first.astype(jnp.float32) + got_far.astype(jnp.float32)).astype(jnp.bfloat16)
    got_back = lax.ppermute(second, "mp", [(k, k ^ 1) for k in range(4)])
    top = jnp.where(low_bit == 0, second, got_back)
    bottom = jnp.where(low_bit == 0, got_back, second)
    return jnp.concatenate([top, bottom], axis=0).astype(jnp.float32)


def dp_allreduce(values, n_dp):
    if n_dp & (n_dp - 1):
        return lax.psum(values, "dp")
    total = values
    step = 1
    while step < n_dp:
        total = total + lax.ppermute(total, "dp", [(k, k ^ step) for k in range(n_dp)])
        step *= 2
    return total


def per_device(n_mp, n_dp,
    tokens,
    cotangent,
    item_lengths,
    w_qkv,
    b_qv,
    w_out,
    b_out,
    w_fc1,
    b_fc1,
    w_fc2,
    b_fc2,
    ln1_gain,
    ln1_bias,
    ln2_gain,
    ln2_bias,
):
    row_count = tokens.shape[0]
    local_cols = w_qkv.shape[2]
    heads_here = local_cols // HEAD
    segments = segment_ids(item_lengths[0], row_count)
    inputs = tokens.astype(jnp.float32)
    norm_one, norm_one_back = jax.vjp(normalize, inputs, ln1_gain, ln1_bias)
    normed_one = norm_one.astype(jnp.bfloat16)
    queries = (jnp.dot(normed_one, w_qkv[0], preferred_element_type=jnp.float32) + b_qv[0]).astype(
        jnp.bfloat16
    )
    key_rows = jnp.dot(normed_one, w_qkv[1], preferred_element_type=jnp.float32).astype(
        jnp.bfloat16
    )
    value_rows = (
        jnp.dot(normed_one, w_qkv[2], preferred_element_type=jnp.float32) + b_qv[1]
    ).astype(jnp.bfloat16)

    def to_heads(values):
        return values.reshape(values.shape[0], heads_here, HEAD).transpose(1, 0, 2)

    lo_blocks, hi_blocks = block_ranges(segments, item_lengths[0])
    query_heads = to_heads(queries)
    key_heads = to_heads(key_rows)
    value_heads = to_heads(value_rows)
    query_t = queries.reshape(row_count, heads_here, HEAD).transpose(1, 2, 0)
    value_t = value_rows.reshape(row_count, heads_here, HEAD).transpose(1, 2, 0)
    upstream = cotangent.astype(jnp.float32)
    q_blocks = row_count // TQ
    first_blocks = (q_blocks * 3) // 8
    bounds = [(0, first_blocks), (first_blocks, q_blocks)]
    pieces_fwd = []
    for b0, b1 in bounds:
        rows = slice(b0 * TQ, b1 * TQ)
        out_t, out32_t, lse_h = flash_forward(
            query_t[:, :, rows], key_heads, value_t, segments[rows], segments,
            lo_blocks[b0:b1], hi_blocks[b0:b1],
        )
        attended_h = out_t.transpose(2, 0, 1).reshape((b1 - b0) * TQ, local_cols)
        att_sum_h = mp_allreduce(
            jnp.dot(attended_h, w_out, preferred_element_type=jnp.float32).astype(jnp.bfloat16), n_mp
        )
        middle_h = inputs[rows] + att_sum_h + b_out
        norm_two_h, back_two_h = jax.vjp(normalize, middle_h, ln2_gain, ln2_bias)
        normed_two_h = norm_two_h.astype(jnp.bfloat16)
        hidden_pre_h = jnp.dot(normed_two_h, w_fc1, preferred_element_type=jnp.float32) + b_fc1
        act_h, gelu_back_h = jax.vjp(exact_gelu, hidden_pre_h)
        activated_h = act_h.astype(jnp.bfloat16)
        mlp_partial_h = jnp.dot(
            activated_h, w_fc2, preferred_element_type=jnp.float32
        ).astype(jnp.bfloat16)
        pieces_fwd.append(dict(
            rows=rows, out32_t=out32_t, lse=lse_h, attended=attended_h, middle=middle_h,
            back_two=back_two_h, normed_two=normed_two_h, gelu_back=gelu_back_h,
            activated=activated_h, mlp_partial=mlp_partial_h,
        ))
    grad_b_fc2 = jnp.sum(upstream, axis=0)
    for piece in pieces_fwd:
        d_act_h = jnp.einsum(
            "td,fd->tf", cotangent[piece["rows"]], w_fc2, preferred_element_type=jnp.float32
        )
        d_pre_h = piece["gelu_back"](d_act_h)[0]
        piece["b_fc1"] = jnp.sum(d_pre_h, axis=0)
        piece["d_pre_low"] = d_pre_h.astype(jnp.bfloat16)
        piece["dn_two_partial"] = jnp.einsum(
            "tf,df->td", piece["d_pre_low"], w_fc1, preferred_element_type=jnp.float32
        ).astype(jnp.bfloat16)
    activated = jnp.concatenate([p["activated"] for p in pieces_fwd], axis=0)
    normed_two = jnp.concatenate([p["normed_two"] for p in pieces_fwd], axis=0)
    d_pre_low = jnp.concatenate([p["d_pre_low"] for p in pieces_fwd], axis=0)
    grad_b_fc1 = sum(p["b_fc1"] for p in pieces_fwd)
    grad_w_fc2 = jnp.einsum("tf,td->fd", activated, cotangent, preferred_element_type=jnp.float32)
    grad_w_fc1_t = jnp.einsum(
        "tf,td->fd", d_pre_low, normed_two, preferred_element_type=jnp.float32
    )
    mlp_weight_grads = jnp.concatenate([grad_w_fc2, grad_w_fc1_t], axis=0).astype(jnp.bfloat16)
    summed_mlp = lax.psum_scatter(mlp_weight_grads, "dp", scatter_dimension=1, tiled=True)
    for piece in pieces_fwd:
        d_normed_two_h = mp_allreduce(piece["dn_two_partial"], n_mp)
        d_mid_norm_h, gain_h, shift_h = piece["back_two"](d_normed_two_h)
        piece["ln2_gain"] = gain_h
        piece["ln2_bias"] = shift_h
        piece["d_middle"] = upstream[piece["rows"]] + d_mid_norm_h
        d_middle_low_h = piece["d_middle"].astype(jnp.bfloat16)
        piece["d_middle_low"] = d_middle_low_h
        piece["d_attended"] = jnp.einsum(
            "td,cd->tc", d_middle_low_h, w_out, preferred_element_type=jnp.float32
        ).astype(jnp.bfloat16)
    grad_ln2_gain = sum(p["ln2_gain"] for p in pieces_fwd)
    grad_ln2_bias = sum(p["ln2_bias"] for p in pieces_fwd)
    d_middle = jnp.concatenate([p["d_middle"] for p in pieces_fwd], axis=0)
    grad_b_out = jnp.sum(d_middle, axis=0)
    d_middle_low = jnp.concatenate([p["d_middle_low"] for p in pieces_fwd], axis=0)
    attended = jnp.concatenate([p["attended"] for p in pieces_fwd], axis=0)
    grad_w_out = jnp.einsum(
        "tc,td->cd", attended, d_middle_low, preferred_element_type=jnp.float32
    )
    d_attended = jnp.concatenate([p["d_attended"] for p in pieces_fwd], axis=0)
    out_f32 = jnp.concatenate([p["out32_t"] for p in pieces_fwd], axis=2)
    log_norms = jnp.concatenate([p["lse"] for p in pieces_fwd], axis=2)
    d_att_heads = to_heads(d_attended)
    partials = lax.optimization_barrier(tuple(p["mlp_partial"] for p in pieces_fwd) + (d_att_heads,))
    d_att_heads = partials[-1]
    outputs = []
    for h, piece in enumerate(pieces_fwd):
        mlp_sum_h = mp_allreduce(partials[h], n_mp)
        outputs.append((piece["middle"] + mlp_sum_h + b_fc2).astype(jnp.bfloat16))
    output = jnp.concatenate(outputs, axis=0)
    d_q_heads, d_k_heads, d_v_heads = flash_backward(
        query_heads, key_heads, value_heads, d_att_heads, out_f32, log_norms,
        segments, lo_blocks, hi_blocks,
    )
    summed_mlp, d_q_heads = lax.optimization_barrier((summed_mlp, d_q_heads))
    d_queries = d_q_heads.transpose(2, 0, 1).reshape(row_count, local_cols)
    d_keys = d_k_heads
    d_values = d_v_heads
    grad_b_qv = jnp.stack([jnp.sum(d_queries, axis=0), jnp.sum(d_values, axis=0)])
    stacked = jnp.stack([d_queries, d_keys, d_values]).astype(jnp.bfloat16)
    grad_w_qkv_t = jnp.einsum("stc,td->scd", stacked, normed_one, preferred_element_type=jnp.float32)
    d_normed_one = mp_allreduce(
        jnp.einsum("stc,sdc->td", stacked, w_qkv, preferred_element_type=jnp.float32).astype(
            jnp.bfloat16
        ),
        n_mp,
    )
    d_input_norm, grad_ln1_gain, grad_ln1_bias = norm_one_back(d_normed_one)
    grad_tokens = d_middle + d_input_norm

    def scatter(grad, dim):
        return lax.psum_scatter(grad.astype(jnp.bfloat16), "dp", scatter_dimension=dim, tiled=True).astype(jnp.float32)

    tail_grads = jnp.concatenate(
        [grad_w_qkv_t.reshape(3 * local_cols, -1), grad_w_out], axis=0
    )
    summed_tail = scatter(tail_grads, 1)
    share = summed_tail.shape[1]
    summed_qkv = summed_tail[: 3 * local_cols].reshape(3, local_cols, share).transpose(0, 2, 1)
    summed_out = summed_tail[3 * local_cols :]
    summed_mlp = summed_mlp.astype(jnp.float32)
    units = grad_w_fc2.shape[0]
    summed_fc2 = summed_mlp[:units]
    summed_fc1 = summed_mlp[units:].T
    early = dp_allreduce(
        jnp.concatenate([grad_ln2_gain, grad_ln2_bias, grad_b_out, grad_b_fc2, grad_b_fc1]), n_dp
    )
    late = dp_allreduce(jnp.concatenate([grad_ln1_gain, grad_ln1_bias, grad_b_qv.reshape(-1)]), n_dp)
    width = grad_ln1_gain.shape[0]
    pieces = [late[0:width], late[width : 2 * width]] + [
        early[k * width : (k + 1) * width] for k in range(4)
    ]
    summed_b_qv = late[2 * width :].reshape(grad_b_qv.shape)
    summed_b_fc1 = early[4 * width :]
    return (
        output,
        grad_tokens,
        summed_qkv,
        summed_b_qv,
        summed_out,
        pieces[4],
        summed_fc1,
        summed_b_fc1,
        summed_fc2,
        pieces[5],
        pieces[0],
        pieces[1],
        pieces[2],
        pieces[3],
    )


def solution(mesh):
    in_specs = (
        P("dp", None),
        P("dp", None),
        P("dp", None),
        P(None, None, "mp"),
        P(None, "mp"),
        P("mp", None),
        P(),
        P(None, "mp"),
        P("mp"),
        P("mp", None),
        P(),
        P(),
        P(),
        P(),
        P(),
    )
    out_specs = (
        P("dp", None),
        P("dp", None),
        P(None, "dp", "mp"),
        P(None, "mp"),
        P("mp", "dp"),
        P(),
        P("dp", "mp"),
        P("mp"),
        P("mp", "dp"),
        P(),
        P(),
        P(),
        P(),
        P(),
    )

    def body(*args):
        return per_device(mesh.shape["mp"], mesh.shape["dp"], *args)

    return jax.shard_map(
        body, mesh=mesh, in_specs=in_specs, out_specs=out_specs, check_vma=False
    )
```

```python
import jax
import jax.numpy as jnp
from jax import lax
from jax.experimental import pallas as pl
from jax.experimental.pallas import tpu as pltpu
from jax.sharding import PartitionSpec as P


HEAD = 64
TQ = 256
TK = 256
NEG = -1e30


HPS = 4


def _fwd_kernel(lo_ref, hi_ref, segc_ref, segr_ref, qt_ref, k_ref, vt_ref, ot_ref, o32t_ref, lse_ref):
    rows = qt_ref.shape[2]
    scale = HEAD ** (-0.5)

    def q_body(i, carry):
        r0 = pl.multiple_of(i * TQ, TQ)
        qts = [qt_ref[hh, :, pl.ds(r0, TQ)] for hh in range(HPS)]
        sq = segr_ref[:, pl.ds(r0, TQ)]

        def kv_body(j, state):
            c0 = pl.multiple_of(j * TK, TK)
            same = segc_ref[pl.ds(c0, TK), :] == sq
            new_state = []
            for hh in range(HPS):
                m, l, acc = state[hh]
                s = jnp.dot(k_ref[hh, pl.ds(c0, TK), :], qts[hh], preferred_element_type=jnp.float32) * scale
                s = jnp.where(same, s, NEG)
                m_new = jnp.maximum(m, jnp.max(s, axis=0, keepdims=True))
                p = jnp.exp(s - m_new)
                alpha = jnp.exp(m - m_new)
                l = alpha * l + jnp.sum(p, axis=0, keepdims=True)
                pv = jnp.dot(vt_ref[hh, :, pl.ds(c0, TK)], p.astype(jnp.bfloat16),
                             preferred_element_type=jnp.float32)
                new_state.append((m_new, l, alpha * acc + pv))
            return tuple(new_state)

        init = tuple(
            (jnp.full((1, TQ), NEG, jnp.float32), jnp.zeros((1, TQ), jnp.float32),
             jnp.zeros((HEAD, TQ), jnp.float32))
            for _ in range(HPS)
        )
        final = lax.fori_loop(lo_ref[i], hi_ref[i], kv_body, init)
        for hh in range(HPS):
            m, l, acc = final[hh]
            out = acc / l
            ot_ref[hh, :, pl.ds(r0, TQ)] = out.astype(ot_ref.dtype)
            o32t_ref[hh, :, pl.ds(r0, TQ)] = out
            lse_ref[hh, :, pl.ds(r0, TQ)] = m + jnp.log(l)
        return carry

    lax.fori_loop(0, rows // TQ, q_body, 0)


def _bwd_kernel(lo_ref, hi_ref, segc_ref, segr_ref, q_ref, qt_ref, k_ref, kt_ref, v_ref, do_ref, dot_ref,
                o32t_ref, lse_ref, dqt_ref, dk_ref, dv_ref, dvec_ref):
    rows = q_ref.shape[1]
    scale = HEAD ** (-0.5)
    dqt_ref[...] = jnp.zeros_like(dqt_ref)

    def d_body(i, carry):
        r0 = pl.multiple_of(i * TQ, TQ)
        for hh in range(HPS):
            prod = dot_ref[hh, :, pl.ds(r0, TQ)].astype(jnp.float32) * o32t_ref[hh, :, pl.ds(r0, TQ)]
            dvec_ref[hh, :, pl.ds(r0, TQ)] = jnp.sum(prod, axis=0, keepdims=True)
        return carry

    lax.fori_loop(0, rows // TQ, d_body, 0)

    def kv_body(j, carry):
        c0 = pl.multiple_of(j * TK, TK)
        ks = [k_ref[hh, pl.ds(c0, TK), :] for hh in range(HPS)]
        vs = [v_ref[hh, pl.ds(c0, TK), :] for hh in range(HPS)]
        kts = [kt_ref[hh, :, pl.ds(c0, TK)] for hh in range(HPS)]
        sk = segc_ref[pl.ds(c0, TK), :]

        def q_body(i, grads):
            r0 = pl.multiple_of(i * TQ, TQ)
            same = sk == segr_ref[:, pl.ds(r0, TQ)]
            new_grads = []
            for hh in range(HPS):
                dk, dv = grads[hh]
                s = jnp.dot(ks[hh], qt_ref[hh, :, pl.ds(r0, TQ)], preferred_element_type=jnp.float32) * scale
                s = jnp.where(same, s, NEG)
                p = jnp.exp(s - lse_ref[hh, :, pl.ds(r0, TQ)])
                dp = jnp.dot(vs[hh], dot_ref[hh, :, pl.ds(r0, TQ)], preferred_element_type=jnp.float32)
                ds = (p * (dp - dvec_ref[hh, :, pl.ds(r0, TQ)])).astype(jnp.bfloat16)
                dv = dv + jnp.dot(p.astype(jnp.bfloat16), do_ref[hh, pl.ds(r0, TQ), :],
                                  preferred_element_type=jnp.float32)
                dk = dk + jnp.dot(ds, q_ref[hh, pl.ds(r0, TQ), :], preferred_element_type=jnp.float32)
                dqt_ref[hh, :, pl.ds(r0, TQ)] += jnp.dot(kts[hh], ds, preferred_element_type=jnp.float32)
                new_grads.append((dk, dv))
            return tuple(new_grads)

        zeros = jnp.zeros((TK, HEAD), jnp.float32)
        final = lax.fori_loop(lo_ref[j], hi_ref[j], q_body, tuple((zeros, zeros) for _ in range(HPS)))
        for hh in range(HPS):
            dk, dv = final[hh]
            dk_ref[pl.ds(c0, TK), pl.ds(hh * HEAD, HEAD)] = dk * scale
            dv_ref[pl.ds(c0, TK), pl.ds(hh * HEAD, HEAD)] = dv
        return carry

    lax.fori_loop(0, rows // TK, kv_body, 0)
    dqt_ref[...] = dqt_ref[...] * scale


def block_ranges(segments, item_lengths_row):
    rows = segments.shape[0]
    ends = jnp.cumsum(item_lengths_row.astype(jnp.int32))
    starts = ends - item_lengths_row.astype(jnp.int32)
    first = segments[0::TQ]
    last = segments[TQ - 1::TQ]
    n_items = item_lengths_row.shape[0]
    key_lo = jnp.take(starts, jnp.clip(first, 0, n_items - 1))
    key_hi = jnp.take(ends, jnp.clip(last, 0, n_items - 1))
    lo = jnp.clip(key_lo // TK, 0, rows // TK)
    hi = jnp.clip((key_hi + TK - 1) // TK, 0, rows // TK)
    return lo.astype(jnp.int32), hi.astype(jnp.int32)


def _head_specs(rows):
    plain = pl.BlockSpec((HPS, rows, HEAD), lambda h, lo, hi: (h, 0, 0))
    flipped = pl.BlockSpec((HPS, HEAD, rows), lambda h, lo, hi: (h, 0, 0))
    stat = pl.BlockSpec((HPS, 1, rows), lambda h, lo, hi: (h, 0, 0))
    col = pl.BlockSpec((rows, 1), lambda h, lo, hi: (0, 0))
    row = pl.BlockSpec((1, rows), lambda h, lo, hi: (0, 0))
    return plain, flipped, stat, col, row


def flash_forward(qt, k, vt, seg_q, seg_k, lo, hi):
    heads, _, rows_q = qt.shape
    rows_k = k.shape[1]
    flipped_q = pl.BlockSpec((HPS, HEAD, rows_q), lambda h, lo, hi: (h, 0, 0))
    flipped_k = pl.BlockSpec((HPS, HEAD, rows_k), lambda h, lo, hi: (h, 0, 0))
    plain_k = pl.BlockSpec((HPS, rows_k, HEAD), lambda h, lo, hi: (h, 0, 0))
    stat = pl.BlockSpec((HPS, 1, rows_q), lambda h, lo, hi: (h, 0, 0))
    col = pl.BlockSpec((rows_k, 1), lambda h, lo, hi: (0, 0))
    row = pl.BlockSpec((1, rows_q), lambda h, lo, hi: (0, 0))
    flops = int(heads * rows_q * rows_k * HEAD * 2 * 2 * 0.6)
    return pl.pallas_call(
        _fwd_kernel,
        out_shape=(
            jax.ShapeDtypeStruct((heads, HEAD, rows_q), jnp.bfloat16),
            jax.ShapeDtypeStruct((heads, HEAD, rows_q), jnp.float32),
            jax.ShapeDtypeStruct((heads, 1, rows_q), jnp.float32),
        ),
        grid_spec=pltpu.PrefetchScalarGridSpec(
            num_scalar_prefetch=2,
            grid=(heads // HPS,),
            in_specs=[col, row, flipped_q, plain_k, flipped_k],
            out_specs=[flipped_q, flipped_q, stat],
        ),
        compiler_params=pltpu.CompilerParams(
            dimension_semantics=("arbitrary",), vmem_limit_bytes=48 * 1024 * 1024),
        cost_estimate=pl.CostEstimate(
            flops=flops, transcendentals=int(heads * rows_q * rows_k * 0.6),
            bytes_accessed=int(heads * HEAD * (rows_q * 8 + rows_k * 4))),
        name="segment_flash_fwd",
    )(lo, hi, seg_k.reshape(rows_k, 1), seg_q.reshape(1, rows_q), qt, k, vt)


def flash_backward(q, k, v, do, o32t, lse, segments, lo, hi):
    heads, rows, _ = q.shape
    plain, flipped, stat, col, row = _head_specs(rows)
    wide = pl.BlockSpec((rows, HPS * HEAD), lambda h, lo, hi: (0, h))
    flops = int(heads * rows * rows * HEAD * 2 * 4 * 0.6)
    return pl.pallas_call(
        _bwd_kernel,
        out_shape=(
            jax.ShapeDtypeStruct((heads, HEAD, rows), jnp.float32),
            jax.ShapeDtypeStruct((rows, heads * HEAD), jnp.float32),
            jax.ShapeDtypeStruct((rows, heads * HEAD), jnp.float32),
        ),
        grid_spec=pltpu.PrefetchScalarGridSpec(
            num_scalar_prefetch=2,
            grid=(heads // HPS,),
            in_specs=[col, row, plain, flipped, plain, flipped, plain, plain, flipped, flipped, stat],
            out_specs=[flipped, wide, wide],
            scratch_shapes=[pltpu.VMEM((HPS, 1, rows), jnp.float32)],
        ),
        compiler_params=pltpu.CompilerParams(
            dimension_semantics=("arbitrary",), vmem_limit_bytes=48 * 1024 * 1024),
        cost_estimate=pl.CostEstimate(
            flops=flops, transcendentals=int(heads * rows * rows * 0.6),
            bytes_accessed=int(heads * rows * HEAD * (2 * 7 + 4 * 4) + heads * rows * 4)),
        name="segment_flash_bwd",
    )(lo, hi, segments.reshape(rows, 1), segments.reshape(1, rows),
      q, q.transpose(0, 2, 1), k, k.transpose(0, 2, 1), v, do, do.transpose(0, 2, 1), o32t, lse)


def normalize(values, gain, shift):
    center = jnp.mean(values, axis=-1, keepdims=True)
    centered = values - center
    spread = jnp.mean(centered * centered, axis=-1, keepdims=True)
    return centered * lax.rsqrt(spread + 1e-06) * gain + shift


def exact_gelu(values):
    return jax.nn.gelu(values, approximate=False)


def segment_ids(lengths_row, row_count):
    ends = jnp.cumsum(lengths_row)
    positions = jnp.arange(row_count, dtype=jnp.int32)
    return jnp.sum((positions[:, None] >= ends[None, :]).astype(jnp.int32), axis=1)


def mp_allreduce(partial, n_mp):
    if n_mp != 4:
        return lax.psum(partial, "mp").astype(jnp.float32)
    idx = lax.axis_index("mp")
    low_bit = idx % 2
    half = partial.shape[0] // 2
    mine = lax.dynamic_slice_in_dim(partial, low_bit * half, half, 0)
    other = lax.dynamic_slice_in_dim(partial, (1 - low_bit) * half, half, 0)
    got = lax.ppermute(other, "mp", [(k, k ^ 1) for k in range(4)])
    first = (mine.astype(jnp.float32) + got.astype(jnp.float32)).astype(jnp.bfloat16)
    got_far = lax.ppermute(first, "mp", [(k, k ^ 2) for k in range(4)])
    second = (first.astype(jnp.float32) + got_far.astype(jnp.float32)).astype(jnp.bfloat16)
    got_back = lax.ppermute(second, "mp", [(k, k ^ 1) for k in range(4)])
    top = jnp.where(low_bit == 0, second, got_back)
    bottom = jnp.where(low_bit == 0, got_back, second)
    return jnp.concatenate([top, bottom], axis=0).astype(jnp.float32)


def dp_allreduce(values, n_dp):
    if n_dp & (n_dp - 1):
        return lax.psum(values, "dp")
    total = values
    step = 1
    while step < n_dp:
        total = total + lax.ppermute(total, "dp", [(k, k ^ step) for k in range(n_dp)])
        step *= 2
    return total


def per_device(n_mp, n_dp,
    tokens,
    cotangent,
    item_lengths,
    w_qkv,
    b_qv,
    w_out,
    b_out,
    w_fc1,
    b_fc1,
    w_fc2,
    b_fc2,
    ln1_gain,
    ln1_bias,
    ln2_gain,
    ln2_bias,
):
    row_count = tokens.shape[0]
    local_cols = w_qkv.shape[2]
    heads_here = local_cols // HEAD
    segments = segment_ids(item_lengths[0], row_count)
    inputs = tokens.astype(jnp.float32)
    norm_one, norm_one_back = jax.vjp(normalize, inputs, ln1_gain, ln1_bias)
    normed_one = norm_one.astype(jnp.bfloat16)
    queries = (jnp.dot(normed_one, w_qkv[0], preferred_element_type=jnp.float32) + b_qv[0]).astype(
        jnp.bfloat16
    )
    key_rows = jnp.dot(normed_one, w_qkv[1], preferred_element_type=jnp.float32).astype(
        jnp.bfloat16
    )
    value_rows = (
        jnp.dot(normed_one, w_qkv[2], preferred_element_type=jnp.float32) + b_qv[1]
    ).astype(jnp.bfloat16)

    def to_heads(values):
        return values.reshape(values.shape[0], heads_here, HEAD).transpose(1, 0, 2)

    lo_blocks, hi_blocks = block_ranges(segments, item_lengths[0])
    query_heads = to_heads(queries)
    key_heads = to_heads(key_rows)
    value_heads = to_heads(value_rows)
    query_t = queries.reshape(row_count, heads_here, HEAD).transpose(1, 2, 0)
    value_t = value_rows.reshape(row_count, heads_here, HEAD).transpose(1, 2, 0)
    upstream = cotangent.astype(jnp.float32)
    q_blocks = row_count // TQ
    first_blocks = (q_blocks * 3) // 8
    bounds = [(0, first_blocks), (first_blocks, q_blocks)]
    pieces_fwd = []
    for b0, b1 in bounds:
        rows = slice(b0 * TQ, b1 * TQ)
        out_t, out32_t, lse_h = flash_forward(
            query_t[:, :, rows], key_heads, value_t, segments[rows], segments,
            lo_blocks[b0:b1], hi_blocks[b0:b1],
        )
        attended_h = out_t.transpose(2, 0, 1).reshape((b1 - b0) * TQ, local_cols)
        att_sum_h = mp_allreduce(
            jnp.dot(attended_h, w_out, preferred_element_type=jnp.float32).astype(jnp.bfloat16), n_mp
        )
        middle_h = inputs[rows] + att_sum_h + b_out
        norm_two_h, back_two_h = jax.vjp(normalize, middle_h, ln2_gain, ln2_bias)
        normed_two_h = norm_two_h.astype(jnp.bfloat16)
        hidden_pre_h = jnp.dot(normed_two_h, w_fc1, preferred_element_type=jnp.float32) + b_fc1
        act_h, gelu_back_h = jax.vjp(exact_gelu, hidden_pre_h)
        activated_h = act_h.astype(jnp.bfloat16)
        mlp_partial_h = jnp.dot(
            activated_h, w_fc2, preferred_element_type=jnp.float32
        ).astype(jnp.bfloat16)
        pieces_fwd.append(dict(
            rows=rows, out32_t=out32_t, lse=lse_h, attended=attended_h, middle=middle_h,
            back_two=back_two_h, normed_two=normed_two_h, gelu_back=gelu_back_h,
            activated=activated_h, mlp_partial=mlp_partial_h,
        ))
    grad_b_fc2 = jnp.sum(upstream, axis=0)
    for piece in pieces_fwd:
        d_act_h = jnp.einsum(
            "td,fd->tf", cotangent[piece["rows"]], w_fc2, preferred_element_type=jnp.float32
        )
        d_pre_h = piece["gelu_back"](d_act_h)[0]
        piece["b_fc1"] = jnp.sum(d_pre_h, axis=0)
        piece["d_pre_low"] = d_pre_h.astype(jnp.bfloat16)
        piece["dn_two_partial"] = jnp.einsum(
            "tf,df->td", piece["d_pre_low"], w_fc1, preferred_element_type=jnp.float32
        ).astype(jnp.bfloat16)
    activated = jnp.concatenate([p["activated"] for p in pieces_fwd], axis=0)
    normed_two = jnp.concatenate([p["normed_two"] for p in pieces_fwd], axis=0)
    d_pre_low = jnp.concatenate([p["d_pre_low"] for p in pieces_fwd], axis=0)
    grad_b_fc1 = sum(p["b_fc1"] for p in pieces_fwd)
    grad_w_fc2 = jnp.einsum("tf,td->fd", activated, cotangent, preferred_element_type=jnp.float32)
    grad_w_fc1_t = jnp.einsum(
        "tf,td->fd", d_pre_low, normed_two, preferred_element_type=jnp.float32
    )
    mlp_weight_grads = jnp.concatenate([grad_w_fc2, grad_w_fc1_t], axis=0).astype(jnp.bfloat16)
    summed_mlp = lax.psum_scatter(mlp_weight_grads, "dp", scatter_dimension=1, tiled=True)
    for piece in pieces_fwd:
        d_normed_two_h = mp_allreduce(piece["dn_two_partial"], n_mp)
        d_mid_norm_h, gain_h, shift_h = piece["back_two"](d_normed_two_h)
        piece["ln2_gain"] = gain_h
        piece["ln2_bias"] = shift_h
        piece["d_middle"] = upstream[piece["rows"]] + d_mid_norm_h
        d_middle_low_h = piece["d_middle"].astype(jnp.bfloat16)
        piece["d_middle_low"] = d_middle_low_h
        piece["d_attended"] = jnp.einsum(
            "td,cd->tc", d_middle_low_h, w_out, preferred_element_type=jnp.float32
        ).astype(jnp.bfloat16)
    grad_ln2_gain = sum(p["ln2_gain"] for p in pieces_fwd)
    grad_ln2_bias = sum(p["ln2_bias"] for p in pieces_fwd)
    d_middle = jnp.concatenate([p["d_middle"] for p in pieces_fwd], axis=0)
    grad_b_out = jnp.sum(d_middle, axis=0)
    d_middle_low = jnp.concatenate([p["d_middle_low"] for p in pieces_fwd], axis=0)
    attended = jnp.concatenate([p["attended"] for p in pieces_fwd], axis=0)
    grad_w_out = jnp.einsum("tc,td->cd", attended, d_middle_low, preferred_element_type=jnp.float32)
    d_attended = jnp.concatenate([p["d_attended"] for p in pieces_fwd], axis=0)
    out_f32 = jnp.concatenate([p["out32_t"] for p in pieces_fwd], axis=2)
    log_norms = jnp.concatenate([p["lse"] for p in pieces_fwd], axis=2)
    d_att_heads = to_heads(d_attended)
    partials = lax.optimization_barrier(tuple(p["mlp_partial"] for p in pieces_fwd) + (d_att_heads,))
    d_att_heads = partials[-1]
    outputs = []
    for h, piece in enumerate(pieces_fwd):
        mlp_sum_h = mp_allreduce(partials[h], n_mp)
        outputs.append((piece["middle"] + mlp_sum_h + b_fc2).astype(jnp.bfloat16))
    output = jnp.concatenate(outputs, axis=0)
    d_q_heads, d_k_heads, d_v_heads = flash_backward(
        query_heads, key_heads, value_heads, d_att_heads, out_f32, log_norms,
        segments, lo_blocks, hi_blocks,
    )
    summed_mlp, d_q_heads = lax.optimization_barrier((summed_mlp, d_q_heads))
    d_queries = d_q_heads.transpose(2, 0, 1).reshape(row_count, local_cols)
    d_keys = d_k_heads
    d_values = d_v_heads
    grad_b_qv = jnp.stack([jnp.sum(d_queries, axis=0), jnp.sum(d_values, axis=0)])
    stacked = jnp.stack([d_queries, d_keys, d_values]).astype(jnp.bfloat16)
    grad_w_qkv_t = jnp.einsum("stc,td->scd", stacked, normed_one, preferred_element_type=jnp.float32)
    d_normed_one = mp_allreduce(
        jnp.einsum("stc,sdc->td", stacked, w_qkv, preferred_element_type=jnp.float32).astype(
            jnp.bfloat16
        ),
        n_mp,
    )
    d_input_norm, grad_ln1_gain, grad_ln1_bias = norm_one_back(d_normed_one)
    grad_tokens = d_middle + d_input_norm

    def scatter(grad, dim):
        return lax.psum_scatter(grad.astype(jnp.bfloat16), "dp", scatter_dimension=dim, tiled=True).astype(jnp.float32)

    tail_grads = jnp.concatenate(
        [grad_w_qkv_t.reshape(3 * local_cols, -1), grad_w_out], axis=0
    )
    summed_tail = scatter(tail_grads, 1)
    share = summed_tail.shape[1]
    summed_qkv = summed_tail[: 3 * local_cols].reshape(3, local_cols, share).transpose(0, 2, 1)
    summed_out = summed_tail[3 * local_cols :]
    summed_mlp = summed_mlp.astype(jnp.float32)
    units = grad_w_fc2.shape[0]
    summed_fc2 = summed_mlp[:units]
    summed_fc1 = summed_mlp[units:].T
    early_parts = [grad_ln2_gain, grad_ln2_bias, grad_b_out, grad_b_fc2, grad_b_fc1]
    late_parts = [grad_ln1_gain, grad_ln1_bias, grad_b_qv.reshape(-1)]
    summed_small = dp_allreduce(jnp.concatenate(early_parts + late_parts), n_dp)
    split_at = sum(part.shape[0] for part in early_parts)
    early = summed_small[:split_at]
    late = summed_small[split_at:]
    width = grad_ln1_gain.shape[0]
    pieces = [late[0:width], late[width : 2 * width]] + [
        early[k * width : (k + 1) * width] for k in range(4)
    ]
    summed_b_qv = late[2 * width :].reshape(grad_b_qv.shape)
    summed_b_fc1 = early[4 * width :]
    return (
        output,
        grad_tokens,
        summed_qkv,
        summed_b_qv,
        summed_out,
        pieces[4],
        summed_fc1,
        summed_b_fc1,
        summed_fc2,
        pieces[5],
        pieces[0],
        pieces[1],
        pieces[2],
        pieces[3],
    )


def solution(mesh):
    in_specs = (
        P("dp", None),
        P("dp", None),
        P("dp", None),
        P(None, None, "mp"),
        P(None, "mp"),
        P("mp", None),
        P(),
        P(None, "mp"),
        P("mp"),
        P("mp", None),
        P(),
        P(),
        P(),
        P(),
        P(),
    )
    out_specs = (
        P("dp", None),
        P("dp", None),
        P(None, "dp", "mp"),
        P(None, "mp"),
        P("mp", "dp"),
        P(),
        P("dp", "mp"),
        P("mp"),
        P("mp", "dp"),
        P(),
        P(),
        P(),
        P(),
        P(),
    )

    def body(*args):
        return per_device(mesh.shape["mp"], mesh.shape["dp"], *args)

    return jax.shard_map(
        body, mesh=mesh, in_specs=in_specs, out_specs=out_specs, check_vma=False
    )
```

```python
import jax
import jax.numpy as jnp
from jax import lax
from jax.experimental import pallas as pl
from jax.experimental.pallas import tpu as pltpu
from jax.sharding import PartitionSpec as P


HEAD = 64
TQ = 256
TK = 256
NEG = -1e30


HPS = 4
HPS_B = 2


def _fwd_kernel(lo_ref, hi_ref, segc_ref, segr_ref, qt_ref, k_ref, vt_ref, ot_ref, o32t_ref, lse_ref):
    rows = qt_ref.shape[2]
    scale = HEAD ** (-0.5)

    def q_body(i, carry):
        r0 = pl.multiple_of(i * TQ, TQ)
        qts = [qt_ref[hh, :, pl.ds(r0, TQ)] for hh in range(HPS)]
        sq = segr_ref[:, pl.ds(r0, TQ)]

        def kv_body(j, state):
            c0 = pl.multiple_of(j * TK, TK)
            same = segc_ref[pl.ds(c0, TK), :] == sq
            new_state = []
            for hh in range(HPS):
                m, l, acc = state[hh]
                s = jnp.dot(k_ref[hh, pl.ds(c0, TK), :], qts[hh], preferred_element_type=jnp.float32) * scale
                s = jnp.where(same, s, NEG)
                m_new = jnp.maximum(m, jnp.max(s, axis=0, keepdims=True))
                p = jnp.exp(s - m_new)
                alpha = jnp.exp(m - m_new)
                l = alpha * l + jnp.sum(p, axis=0, keepdims=True)
                pv = jnp.dot(vt_ref[hh, :, pl.ds(c0, TK)], p.astype(jnp.bfloat16),
                             preferred_element_type=jnp.float32)
                new_state.append((m_new, l, alpha * acc + pv))
            return tuple(new_state)

        init = tuple(
            (jnp.full((1, TQ), NEG, jnp.float32), jnp.zeros((1, TQ), jnp.float32),
             jnp.zeros((HEAD, TQ), jnp.float32))
            for _ in range(HPS)
        )
        final = lax.fori_loop(lo_ref[i], hi_ref[i], kv_body, init)
        for hh in range(HPS):
            m, l, acc = final[hh]
            out = acc / l
            ot_ref[hh, :, pl.ds(r0, TQ)] = out.astype(ot_ref.dtype)
            o32t_ref[hh, :, pl.ds(r0, TQ)] = out
            lse_ref[hh, :, pl.ds(r0, TQ)] = m + jnp.log(l)
        return carry

    lax.fori_loop(0, rows // TQ, q_body, 0)


def _bwd_kernel(lo_ref, hi_ref, segc_ref, segr_ref, q_ref, qt_ref, k_ref, kt_ref, v_ref, do_ref, dot_ref,
                o32t_ref, lse_ref, dqt_ref, dk_ref, dv_ref, dvec_ref):
    rows = q_ref.shape[1]
    scale = HEAD ** (-0.5)
    dqt_ref[...] = jnp.zeros_like(dqt_ref)

    def d_body(i, carry):
        r0 = pl.multiple_of(i * TQ, TQ)
        for hh in range(HPS_B):
            prod = dot_ref[hh, :, pl.ds(r0, TQ)].astype(jnp.float32) * o32t_ref[hh, :, pl.ds(r0, TQ)]
            dvec_ref[hh, :, pl.ds(r0, TQ)] = jnp.sum(prod, axis=0, keepdims=True)
        return carry

    lax.fori_loop(0, rows // TQ, d_body, 0)

    def kv_body(j, carry):
        c0 = pl.multiple_of(j * TK, TK)
        ks = [k_ref[hh, pl.ds(c0, TK), :] for hh in range(HPS_B)]
        vs = [v_ref[hh, pl.ds(c0, TK), :] for hh in range(HPS_B)]
        kts = [kt_ref[hh, :, pl.ds(c0, TK)] for hh in range(HPS_B)]
        sk = segc_ref[pl.ds(c0, TK), :]

        def q_body(i, grads):
            r0 = pl.multiple_of(i * TQ, TQ)
            same = sk == segr_ref[:, pl.ds(r0, TQ)]
            new_grads = []
            for hh in range(HPS_B):
                dk, dv = grads[hh]
                s = jnp.dot(ks[hh], qt_ref[hh, :, pl.ds(r0, TQ)], preferred_element_type=jnp.float32) * scale
                s = jnp.where(same, s, NEG)
                p = jnp.exp(s - lse_ref[hh, :, pl.ds(r0, TQ)])
                dp = jnp.dot(vs[hh], dot_ref[hh, :, pl.ds(r0, TQ)], preferred_element_type=jnp.float32)
                ds = (p * (dp - dvec_ref[hh, :, pl.ds(r0, TQ)])).astype(jnp.bfloat16)
                dv = dv + jnp.dot(p.astype(jnp.bfloat16), do_ref[hh, pl.ds(r0, TQ), :],
                                  preferred_element_type=jnp.float32)
                dk = dk + jnp.dot(ds, q_ref[hh, pl.ds(r0, TQ), :], preferred_element_type=jnp.float32)
                dqt_ref[hh, :, pl.ds(r0, TQ)] += jnp.dot(kts[hh], ds, preferred_element_type=jnp.float32)
                new_grads.append((dk, dv))
            return tuple(new_grads)

        zeros = jnp.zeros((TK, HEAD), jnp.float32)
        final = lax.fori_loop(lo_ref[j], hi_ref[j], q_body, tuple((zeros, zeros) for _ in range(HPS_B)))
        for hh in range(HPS_B):
            dk, dv = final[hh]
            dk_ref[pl.ds(c0, TK), pl.ds(hh * HEAD, HEAD)] = dk * scale
            dv_ref[pl.ds(c0, TK), pl.ds(hh * HEAD, HEAD)] = dv
        return carry

    lax.fori_loop(0, rows // TK, kv_body, 0)
    dqt_ref[...] = dqt_ref[...] * scale


def block_ranges(segments, item_lengths_row):
    rows = segments.shape[0]
    ends = jnp.cumsum(item_lengths_row.astype(jnp.int32))
    starts = ends - item_lengths_row.astype(jnp.int32)
    first = segments[0::TQ]
    last = segments[TQ - 1::TQ]
    n_items = item_lengths_row.shape[0]
    key_lo = jnp.take(starts, jnp.clip(first, 0, n_items - 1))
    key_hi = jnp.take(ends, jnp.clip(last, 0, n_items - 1))
    lo = jnp.clip(key_lo // TK, 0, rows // TK)
    hi = jnp.clip((key_hi + TK - 1) // TK, 0, rows // TK)
    return lo.astype(jnp.int32), hi.astype(jnp.int32)


def _head_specs(rows):
    plain = pl.BlockSpec((HPS_B, rows, HEAD), lambda h, lo, hi: (h, 0, 0))
    flipped = pl.BlockSpec((HPS_B, HEAD, rows), lambda h, lo, hi: (h, 0, 0))
    stat = pl.BlockSpec((HPS_B, 1, rows), lambda h, lo, hi: (h, 0, 0))
    col = pl.BlockSpec((rows, 1), lambda h, lo, hi: (0, 0))
    row = pl.BlockSpec((1, rows), lambda h, lo, hi: (0, 0))
    return plain, flipped, stat, col, row


def flash_forward(qt, k, vt, seg_q, seg_k, lo, hi):
    heads, _, rows_q = qt.shape
    rows_k = k.shape[1]
    flipped_q = pl.BlockSpec((HPS, HEAD, rows_q), lambda h, lo, hi: (h, 0, 0))
    flipped_k = pl.BlockSpec((HPS, HEAD, rows_k), lambda h, lo, hi: (h, 0, 0))
    plain_k = pl.BlockSpec((HPS, rows_k, HEAD), lambda h, lo, hi: (h, 0, 0))
    stat = pl.BlockSpec((HPS, 1, rows_q), lambda h, lo, hi: (h, 0, 0))
    col = pl.BlockSpec((rows_k, 1), lambda h, lo, hi: (0, 0))
    row = pl.BlockSpec((1, rows_q), lambda h, lo, hi: (0, 0))
    flops = int(heads * rows_q * rows_k * HEAD * 2 * 2 * 0.6)
    return pl.pallas_call(
        _fwd_kernel,
        out_shape=(
            jax.ShapeDtypeStruct((heads, HEAD, rows_q), jnp.bfloat16),
            jax.ShapeDtypeStruct((heads, HEAD, rows_q), jnp.float32),
            jax.ShapeDtypeStruct((heads, 1, rows_q), jnp.float32),
        ),
        grid_spec=pltpu.PrefetchScalarGridSpec(
            num_scalar_prefetch=2,
            grid=(heads // HPS,),
            in_specs=[col, row, flipped_q, plain_k, flipped_k],
            out_specs=[flipped_q, flipped_q, stat],
        ),
        compiler_params=pltpu.CompilerParams(
            dimension_semantics=("arbitrary",), vmem_limit_bytes=48 * 1024 * 1024),
        cost_estimate=pl.CostEstimate(
            flops=flops, transcendentals=int(heads * rows_q * rows_k * 0.6),
            bytes_accessed=int(heads * HEAD * (rows_q * 8 + rows_k * 4))),
        name="segment_flash_fwd",
    )(lo, hi, seg_k.reshape(rows_k, 1), seg_q.reshape(1, rows_q), qt, k, vt)


def flash_backward(q, k, v, do, o32t, lse, segments, lo, hi):
    heads, rows, _ = q.shape
    plain, flipped, stat, col, row = _head_specs(rows)
    wide = pl.BlockSpec((rows, HPS_B * HEAD), lambda h, lo, hi: (0, h))
    flops = int(heads * rows * rows * HEAD * 2 * 4 * 0.6)
    return pl.pallas_call(
        _bwd_kernel,
        out_shape=(
            jax.ShapeDtypeStruct((heads, HEAD, rows), jnp.float32),
            jax.ShapeDtypeStruct((rows, heads * HEAD), jnp.float32),
            jax.ShapeDtypeStruct((rows, heads * HEAD), jnp.float32),
        ),
        grid_spec=pltpu.PrefetchScalarGridSpec(
            num_scalar_prefetch=2,
            grid=(heads // HPS_B,),
            in_specs=[col, row, plain, flipped, plain, flipped, plain, plain, flipped, flipped, stat],
            out_specs=[flipped, wide, wide],
            scratch_shapes=[pltpu.VMEM((HPS_B, 1, rows), jnp.float32)],
        ),
        compiler_params=pltpu.CompilerParams(
            dimension_semantics=("arbitrary",), vmem_limit_bytes=48 * 1024 * 1024),
        cost_estimate=pl.CostEstimate(
            flops=flops, transcendentals=int(heads * rows * rows * 0.6),
            bytes_accessed=int(heads * rows * HEAD * (2 * 7 + 4 * 4) + heads * rows * 4)),
        name="segment_flash_bwd",
    )(lo, hi, segments.reshape(rows, 1), segments.reshape(1, rows),
      q, q.transpose(0, 2, 1), k, k.transpose(0, 2, 1), v, do, do.transpose(0, 2, 1), o32t, lse)


def normalize(values, gain, shift):
    center = jnp.mean(values, axis=-1, keepdims=True)
    centered = values - center
    spread = jnp.mean(centered * centered, axis=-1, keepdims=True)
    return centered * lax.rsqrt(spread + 1e-06) * gain + shift


def exact_gelu(values):
    return jax.nn.gelu(values, approximate=False)


def segment_ids(lengths_row, row_count):
    ends = jnp.cumsum(lengths_row)
    positions = jnp.arange(row_count, dtype=jnp.int32)
    return jnp.sum((positions[:, None] >= ends[None, :]).astype(jnp.int32), axis=1)


def mp_allreduce(partial, n_mp):
    if n_mp != 4:
        return lax.psum(partial, "mp").astype(jnp.float32)
    idx = lax.axis_index("mp")
    low_bit = idx % 2
    half = partial.shape[0] // 2
    mine = lax.dynamic_slice_in_dim(partial, low_bit * half, half, 0)
    other = lax.dynamic_slice_in_dim(partial, (1 - low_bit) * half, half, 0)
    got = lax.ppermute(other, "mp", [(k, k ^ 1) for k in range(4)])
    first = (mine.astype(jnp.float32) + got.astype(jnp.float32)).astype(jnp.bfloat16)
    got_far = lax.ppermute(first, "mp", [(k, k ^ 2) for k in range(4)])
    second = (first.astype(jnp.float32) + got_far.astype(jnp.float32)).astype(jnp.bfloat16)
    got_back = lax.ppermute(second, "mp", [(k, k ^ 1) for k in range(4)])
    top = jnp.where(low_bit == 0, second, got_back)
    bottom = jnp.where(low_bit == 0, got_back, second)
    return jnp.concatenate([top, bottom], axis=0).astype(jnp.float32)


def dp_allreduce(values, n_dp):
    if n_dp & (n_dp - 1):
        return lax.psum(values, "dp")
    total = values
    step = 1
    while step < n_dp:
        total = total + lax.ppermute(total, "dp", [(k, k ^ step) for k in range(n_dp)])
        step *= 2
    return total


def per_device(n_mp, n_dp,
    tokens,
    cotangent,
    item_lengths,
    w_qkv,
    b_qv,
    w_out,
    b_out,
    w_fc1,
    b_fc1,
    w_fc2,
    b_fc2,
    ln1_gain,
    ln1_bias,
    ln2_gain,
    ln2_bias,
):
    row_count = tokens.shape[0]
    local_cols = w_qkv.shape[2]
    heads_here = local_cols // HEAD
    segments = segment_ids(item_lengths[0], row_count)
    inputs = tokens.astype(jnp.float32)
    norm_one, norm_one_back = jax.vjp(normalize, inputs, ln1_gain, ln1_bias)
    normed_one = norm_one.astype(jnp.bfloat16)
    queries = (jnp.dot(normed_one, w_qkv[0], preferred_element_type=jnp.float32) + b_qv[0]).astype(
        jnp.bfloat16
    )
    key_rows = jnp.dot(normed_one, w_qkv[1], preferred_element_type=jnp.float32).astype(
        jnp.bfloat16
    )
    value_rows = (
        jnp.dot(normed_one, w_qkv[2], preferred_element_type=jnp.float32) + b_qv[1]
    ).astype(jnp.bfloat16)

    def to_heads(values):
        return values.reshape(values.shape[0], heads_here, HEAD).transpose(1, 0, 2)

    lo_blocks, hi_blocks = block_ranges(segments, item_lengths[0])
    query_heads = to_heads(queries)
    key_heads = to_heads(key_rows)
    value_heads = to_heads(value_rows)
    query_t = queries.reshape(row_count, heads_here, HEAD).transpose(1, 2, 0)
    value_t = value_rows.reshape(row_count, heads_here, HEAD).transpose(1, 2, 0)
    upstream = cotangent.astype(jnp.float32)
    q_blocks = row_count // TQ
    first_blocks = (q_blocks * 3) // 8
    bounds = [(0, first_blocks), (first_blocks, q_blocks)]
    pieces_fwd = []
    for b0, b1 in bounds:
        rows = slice(b0 * TQ, b1 * TQ)
        out_t, out32_t, lse_h = flash_forward(
            query_t[:, :, rows], key_heads, value_t, segments[rows], segments,
            lo_blocks[b0:b1], hi_blocks[b0:b1],
        )
        attended_h = out_t.transpose(2, 0, 1).reshape((b1 - b0) * TQ, local_cols)
        att_sum_h = mp_allreduce(
            jnp.dot(attended_h, w_out, preferred_element_type=jnp.float32).astype(jnp.bfloat16), n_mp
        )
        middle_h = inputs[rows] + att_sum_h + b_out
        norm_two_h, back_two_h = jax.vjp(normalize, middle_h, ln2_gain, ln2_bias)
        normed_two_h = norm_two_h.astype(jnp.bfloat16)
        hidden_pre_h = jnp.dot(normed_two_h, w_fc1, preferred_element_type=jnp.float32) + b_fc1
        act_h, gelu_back_h = jax.vjp(exact_gelu, hidden_pre_h)
        activated_h = act_h.astype(jnp.bfloat16)
        mlp_partial_h = jnp.dot(
            activated_h, w_fc2, preferred_element_type=jnp.float32
        ).astype(jnp.bfloat16)
        pieces_fwd.append(dict(
            rows=rows, out32_t=out32_t, lse=lse_h, attended=attended_h, middle=middle_h,
            back_two=back_two_h, normed_two=normed_two_h, gelu_back=gelu_back_h,
            activated=activated_h, mlp_partial=mlp_partial_h,
        ))
    grad_b_fc2 = jnp.sum(upstream, axis=0)
    for piece in pieces_fwd:
        d_act_h = jnp.einsum(
            "td,fd->tf", cotangent[piece["rows"]], w_fc2, preferred_element_type=jnp.float32
        )
        d_pre_h = piece["gelu_back"](d_act_h)[0]
        piece["b_fc1"] = jnp.sum(d_pre_h, axis=0)
        piece["d_pre_low"] = d_pre_h.astype(jnp.bfloat16)
        piece["dn_two_partial"] = jnp.einsum(
            "tf,df->td", piece["d_pre_low"], w_fc1, preferred_element_type=jnp.float32
        ).astype(jnp.bfloat16)
    activated = jnp.concatenate([p["activated"] for p in pieces_fwd], axis=0)
    normed_two = jnp.concatenate([p["normed_two"] for p in pieces_fwd], axis=0)
    d_pre_low = jnp.concatenate([p["d_pre_low"] for p in pieces_fwd], axis=0)
    grad_b_fc1 = sum(p["b_fc1"] for p in pieces_fwd)
    grad_w_fc2 = jnp.einsum("tf,td->fd", activated, cotangent, preferred_element_type=jnp.float32)
    grad_w_fc1_t = jnp.einsum(
        "tf,td->fd", d_pre_low, normed_two, preferred_element_type=jnp.float32
    )
    mlp_weight_grads = jnp.concatenate([grad_w_fc2, grad_w_fc1_t], axis=0).astype(jnp.bfloat16)
    summed_mlp = lax.psum_scatter(mlp_weight_grads, "dp", scatter_dimension=1, tiled=True)
    for piece in pieces_fwd:
        d_normed_two_h = mp_allreduce(piece["dn_two_partial"], n_mp)
        d_mid_norm_h, gain_h, shift_h = piece["back_two"](d_normed_two_h)
        piece["ln2_gain"] = gain_h
        piece["ln2_bias"] = shift_h
        piece["d_middle"] = upstream[piece["rows"]] + d_mid_norm_h
        d_middle_low_h = piece["d_middle"].astype(jnp.bfloat16)
        piece["d_middle_low"] = d_middle_low_h
        piece["d_attended"] = jnp.einsum(
            "td,cd->tc", d_middle_low_h, w_out, preferred_element_type=jnp.float32
        ).astype(jnp.bfloat16)
    grad_ln2_gain = sum(p["ln2_gain"] for p in pieces_fwd)
    grad_ln2_bias = sum(p["ln2_bias"] for p in pieces_fwd)
    d_middle = jnp.concatenate([p["d_middle"] for p in pieces_fwd], axis=0)
    grad_b_out = jnp.sum(d_middle, axis=0)
    d_middle_low = jnp.concatenate([p["d_middle_low"] for p in pieces_fwd], axis=0)
    attended = jnp.concatenate([p["attended"] for p in pieces_fwd], axis=0)
    grad_w_out = jnp.einsum("tc,td->cd", attended, d_middle_low, preferred_element_type=jnp.float32)
    d_attended = jnp.concatenate([p["d_attended"] for p in pieces_fwd], axis=0)
    out_f32 = jnp.concatenate([p["out32_t"] for p in pieces_fwd], axis=2)
    log_norms = jnp.concatenate([p["lse"] for p in pieces_fwd], axis=2)
    d_att_heads = to_heads(d_attended)
    partials = lax.optimization_barrier(tuple(p["mlp_partial"] for p in pieces_fwd) + (d_att_heads,))
    d_att_heads = partials[-1]
    outputs = []
    for h, piece in enumerate(pieces_fwd):
        mlp_sum_h = mp_allreduce(partials[h], n_mp)
        outputs.append((piece["middle"] + mlp_sum_h + b_fc2).astype(jnp.bfloat16))
    output = jnp.concatenate(outputs, axis=0)
    d_q_heads, d_k_heads, d_v_heads = flash_backward(
        query_heads, key_heads, value_heads, d_att_heads, out_f32, log_norms,
        segments, lo_blocks, hi_blocks,
    )
    summed_mlp, d_q_heads = lax.optimization_barrier((summed_mlp, d_q_heads))
    d_queries = d_q_heads.transpose(2, 0, 1).reshape(row_count, local_cols)
    d_keys = d_k_heads
    d_values = d_v_heads
    grad_b_qv = jnp.stack([jnp.sum(d_queries, axis=0), jnp.sum(d_values, axis=0)])
    stacked = jnp.stack([d_queries, d_keys, d_values]).astype(jnp.bfloat16)
    grad_w_qkv_t = jnp.einsum("stc,td->scd", stacked, normed_one, preferred_element_type=jnp.float32)
    d_normed_one = mp_allreduce(
        jnp.einsum("stc,sdc->td", stacked, w_qkv, preferred_element_type=jnp.float32).astype(
            jnp.bfloat16
        ),
        n_mp,
    )
    d_input_norm, grad_ln1_gain, grad_ln1_bias = norm_one_back(d_normed_one)
    grad_tokens = d_middle + d_input_norm

    def scatter(grad, dim):
        return lax.psum_scatter(grad.astype(jnp.bfloat16), "dp", scatter_dimension=dim, tiled=True).astype(jnp.float32)

    tail_grads = jnp.concatenate(
        [grad_w_qkv_t.reshape(3 * local_cols, -1), grad_w_out], axis=0
    )
    summed_tail = scatter(tail_grads, 1)
    share = summed_tail.shape[1]
    summed_qkv = summed_tail[: 3 * local_cols].reshape(3, local_cols, share).transpose(0, 2, 1)
    summed_out = summed_tail[3 * local_cols :]
    summed_mlp = summed_mlp.astype(jnp.float32)
    units = grad_w_fc2.shape[0]
    summed_fc2 = summed_mlp[:units]
    summed_fc1 = summed_mlp[units:].T
    early_parts = [grad_ln2_gain, grad_ln2_bias, grad_b_out, grad_b_fc2, grad_b_fc1]
    late_parts = [grad_ln1_gain, grad_ln1_bias, grad_b_qv.reshape(-1)]
    summed_small = dp_allreduce(jnp.concatenate(early_parts + late_parts), n_dp)
    split_at = sum(part.shape[0] for part in early_parts)
    early = summed_small[:split_at]
    late = summed_small[split_at:]
    width = grad_ln1_gain.shape[0]
    pieces = [late[0:width], late[width : 2 * width]] + [
        early[k * width : (k + 1) * width] for k in range(4)
    ]
    summed_b_qv = late[2 * width :].reshape(grad_b_qv.shape)
    summed_b_fc1 = early[4 * width :]
    return (
        output,
        grad_tokens,
        summed_qkv,
        summed_b_qv,
        summed_out,
        pieces[4],
        summed_fc1,
        summed_b_fc1,
        summed_fc2,
        pieces[5],
        pieces[0],
        pieces[1],
        pieces[2],
        pieces[3],
    )


def solution(mesh):
    in_specs = (
        P("dp", None),
        P("dp", None),
        P("dp", None),
        P(None, None, "mp"),
        P(None, "mp"),
        P("mp", None),
        P(),
        P(None, "mp"),
        P("mp"),
        P("mp", None),
        P(),
        P(),
        P(),
        P(),
        P(),
    )
    out_specs = (
        P("dp", None),
        P("dp", None),
        P(None, "dp", "mp"),
        P(None, "mp"),
        P("mp", "dp"),
        P(),
        P("dp", "mp"),
        P("mp"),
        P("mp", "dp"),
        P(),
        P(),
        P(),
        P(),
        P(),
    )

    def body(*args):
        return per_device(mesh.shape["mp"], mesh.shape["dp"], *args)

    return jax.shard_map(
        body, mesh=mesh, in_specs=in_specs, out_specs=out_specs, check_vma=False
    )
```
